256 devices in a mesh: grp: 2 (over y), gx: 16 (over z), gy: 4 (over x), gz: 2 (over core).
Axes of the slice: x: 4, y: 2, z: 16, core: 2. Of those that a mesh axis runs over, the one named last changes fastest.
The devices are a block of a 4x16x16 slice.
Arguments:
- observed: float32 [16384, 4, 256], P(('grp', 'gx', 'gy', 'gz')), parts along dimension 0, may hold values from -12 to 12
- predicted: float32 [16384, 4, 256], P(('grp', 'gx', 'gy', 'gz')), parts along dimension 0, may hold values from -6 to 6
- coherence_mask: int32 [16384, 256], P(('grp', 'gx', 'gy', 'gz')), parts along dimension 0, may hold values 0 or 1
- block_count: int32 [16384], P(('grp', 'gx', 'gy', 'gz')), parts along dimension 0, may hold values from 64 to 256
- block_owner: int32 [16384, 1], P(('grp', 'gx', 'gy', 'gz')), parts along dimension 0, may hold values from 0 to 63; in each aligned block of 64 rows (0 to 63, 64 to 127, ...) at most 4 rows name the same one
- block_matrix_choice: int32 [16384], P(('grp', 'gx', 'gy', 'gz')), parts along dimension 0, may hold values from 0 to 31
- block_patch: int32 [16384], P(('grp', 'gx', 'gy', 'gz')), parts along dimension 0, may hold values from 0 to 31
- look_vector: float32 [4, 3], replicated, may hold values from -1 to 1
- interp_weights: bfloat16 [32, 256, 128], replicated, may hold values from -0.375 to 0.375
- depth_kernel: float32 [64], P(('grp', 'gz')), parts along dimension 0, may hold values from 0.2 to 1
- stiffness: float32 [64, 512, 512], P(('grp', 'gz'), 'gx', 'gy'), parts along dimension 0, may hold values from 0.25 to 4
Outputs:
- adjoint_field: float32 [3, 64, 512, 512], P(None, ('grp', 'gz'), 'gx', 'gy'), parts along dimension 1
- cg_residual: float32 [3, 64, 512, 512], P(None, ('grp', 'gz'), 'gx', 'gy'), parts along dimension 1
The draws below stay inside these ranges and needn't reach their ends.
There are 2 independent parts, one for each index of `grp`. The reference program is written for one: setup_inputs(seed, part) draws one part's arguments, and reference() takes and returns one part's arrays. A program takes and returns all parts, laid end to end along the dimension named above; an argument that names none is the same for every part. Nothing has to cross between parts.
Inputs may be any that keep to these rules, and one draw needn't show every extreme that they name: `block_owner`: the blocks of one device name no column tile more than 4 times; in some devices one tile is named exactly 4 times.
All inputs are finite; a program needn't handle non-finite values. No bound on the sum of `coherence_mask` on one device may be relied on, other than what follows from the above.
Results may differ from the reference program's by a relative error of at most 0.0029.
Values sent between devices are 32-bit elements; how exact they have to be, the bound alone decides.
No kernel may reach another device: no remote copies, remote signals or barrier semaphores. Data moves between devices by JAX's collectives and lax.ppermute only.
A program may use at most 64 MiB of HBM per device.

```python
import math
import jax
import jax.numpy as jnp
import numpy as np
from jax import lax

CX = 32
CY = 128
BLK_DEV = 64
NTAB = 32
EPOCHS = 4
BPIX = 256
PATCH_X = 8
PATCH_Y = 16
ITERS = 3
NX = 512
NY = 512
NZ = 32
NBLK = 8192
CAP = 4
NPOS = 32
N_GX = 16
N_GY = 4


def draw_observed(key, part):
    rows = jnp.arange(NBLK, dtype=jnp.float32)
    spread = 1.0 + 2.0 * rows / max(NBLK - 1, 1)
    base = jax.random.truncated_normal(key, -4.0, 4.0, (NBLK, EPOCHS, BPIX), jnp.float32)
    return base * spread[:, None, None]


def place_ends(values, own_key, smallest, largest):
    dims = values.shape
    place = [jax.random.randint(jax.random.fold_in(own_key, axis), (), 0, dims[axis]) for axis in range(len(dims))]
    values = values.at[tuple(place)].set(smallest)
    longest = dims.index(max(dims))
    place[longest] = (place[longest] + 1) % dims[longest]
    return values.at[tuple(place)].set(largest)


def level_of(key, dims, split, low, largest):
    def one(dim, blocks):
        steps = jax.random.uniform(jax.random.fold_in(jax.random.fold_in(key, 6), dim), (blocks,), jnp.float32, low / len(split), largest / len(split))
        return jnp.repeat(jnp.exp(steps), dims[dim] // blocks).reshape((-1,) + (1,) * (len(dims) - dim - 1))

    level = one(*split[0])
    for cut in split[1:]:
        level = level * one(*cut)
    return level


def routed_block(rng, own, number, rows, number_of, top, reach, lean):
    ranking = jax.random.permutation(rng, number_of)
    heavy_load, ordinary = load_shares(number_of, rows * top, reach, lean, True), load_shares(number_of, rows * top, reach, lean, False)
    places = jnp.arange(number_of)

    def named(sizes, offset_by):
        used = int((sizes > 0).sum())
        fixed = max(1, used // 4)
        moved = fixed + (places - fixed + offset_by * (used - fixed)) % max(1, number_of - fixed)
        return jnp.zeros((number_of,), jnp.int32).at[ranking[jnp.where(places < fixed, places, moved)]].set(jnp.asarray(sizes, jnp.int32))

    sizes = jnp.where(number % 4 == 0, named(heavy_load, number // 4), named(ordinary, number - number // 4 - 1))
    mixed = jax.random.permutation(jax.random.fold_in(own, 3), number_of)
    giver, receiver = mixed[0:number_of // 2 * 2:2], mixed[1:number_of // 2 * 2:2]
    room = jnp.minimum(sizes[giver] - 1, reach - sizes[receiver]) // 2
    room = jnp.where((giver == ranking[0]) | (receiver == ranking[0]) | (sizes[receiver] == 0), 0, jnp.maximum(room, 0))
    moved = jax.random.randint(jax.random.fold_in(own, 4), (number_of // 2,), 0, 1 << 20) % (room + 1)
    sizes = sizes.at[giver].add(-moved).at[receiver].add(moved)
    members = jnp.searchsorted(jnp.cumsum(sizes), jnp.arange(rows * top), side="right").astype(jnp.int32)
    table = members.reshape(top, rows).T
    table = table[jax.random.permutation(jax.random.fold_in(own, 1), rows)]
    offset_by = jax.random.randint(jax.random.fold_in(own, 2), (rows, 1), 0, top)
    return jnp.take_along_axis(table, (jnp.arange(top)[None, :] + offset_by) % top, axis=1)


def load_shares(amount, total, bound, lean, full):
    portions = [(1 << 20) // math.isqrt(grade ** lean) + 1 for grade in range(1, amount + 1)]
    largest = bound if full else min(bound, max(-(-total // amount), total * portions[0] // sum(portions)))
    least = 1 if total - largest >= amount - 1 else 0
    counts, surplus = [largest] + [least] * (amount - 1), total - largest - least * (amount - 1)
    while surplus > 0:
        movable = [i for i in range(1, amount) if counts[i] < largest] or [i for i in range(1, amount) if counts[i] < bound]
        pool, budget = sum([portions[i] for i in movable]), surplus
        for i in movable:
            extra = min(bound - counts[i], max(1, budget * portions[i] // pool), surplus)
            counts[i] = counts[i] + extra
            surplus = surplus - extra
    return np.array(counts)


def noise(key, dims, deviation, bound, split=(), kind=jnp.bfloat16):
    level = level_of(key, dims, split, -0.22, 0.18) if split else 1.0
    drawn = jax.random.normal(key, dims, jnp.float32) * deviation * level
    return jnp.minimum(jnp.maximum(drawn, -bound), bound).astype(kind)


def setup_inputs(seed: int = 0, part: int = 0) -> dict:
    splits = jax.random.split(jax.random.key(seed), 12)
    part_splits = jax.random.split(jax.random.fold_in(splits[11], part), 12)
    observed = draw_observed(jax.random.fold_in(jax.random.fold_in(splits[11], part), 71), part)
    predicted = noise(part_splits[1], (NBLK, EPOCHS, BPIX), 1.0, 6.0, ((0, 128),), jnp.float32)
    coherence_mask = place_ends((jax.random.randint(part_splits[2], (NBLK, BPIX), 0, 4) < 3).astype(jnp.int32), jax.random.fold_in(part_splits[2], 1), 0, 1)
    block_count = place_ends(jax.random.randint(part_splits[3], (NBLK,), BPIX // 4, BPIX + 1), jax.random.fold_in(part_splits[3], 1), BPIX // 4, BPIX).astype(jnp.int32)
    block_owner_keys = jax.random.split(jax.random.fold_in(part_splits[4], 1), NBLK // BLK_DEV)
    block_owner_turns = jax.random.permutation(jax.random.fold_in(part_splits[4], 3), NBLK // BLK_DEV)
    block_owner = jax.vmap(lambda own, number: routed_block(jax.random.fold_in(part_splits[4], 2), own, number, BLK_DEV, N_GX * N_GY, 1, CAP, 2))(block_owner_keys, block_owner_turns).reshape((NBLK, 1))
    block_matrix_choice = place_ends(jax.random.randint(part_splits[5], (NBLK,), 0, NTAB), jax.random.fold_in(part_splits[5], 1), 0, NTAB - 1).astype(jnp.int32)
    block_patch = place_ends(jax.random.randint(part_splits[6], (NBLK,), 0, NPOS), jax.random.fold_in(part_splits[6], 1), 0, NPOS - 1).astype(jnp.int32)
    look_vector = jnp.clip(jax.random.uniform(splits[7], (EPOCHS, 3), jnp.float32, -1.0, 1.0), -1.0, 1.0)
    interp_weights = noise(splits[8], (NTAB, BPIX, PATCH_X * PATCH_Y), BPIX ** -0.5, 0.375)
    depth_kernel = jnp.clip(jnp.exp(math.log(1.0) - 1.609438 * jax.random.uniform(part_splits[9], (NZ,), jnp.float32) ** level_of(part_splits[9], (NZ,), ((0, 2),), -0.2, 0.2)), 0.2, 1.0)
    stiffness = jnp.clip(jnp.exp(math.log(4.0) - 2.7725887 * jax.random.uniform(part_splits[10], (NZ, NX, NY), jnp.float32) ** level_of(part_splits[10], (NZ, NX, NY), ((0, 2), (1, 16), (2, 4)), -0.2, 0.2)), 0.25, 4.0)
    return dict(observed=observed, predicted=predicted, coherence_mask=coherence_mask, block_count=block_count, block_owner=block_owner, block_matrix_choice=block_matrix_choice, block_patch=block_patch, look_vector=look_vector, interp_weights=interp_weights, depth_kernel=depth_kernel, stiffness=stiffness)


KAPPA = 0.5
EPS = 1e-06
SPATIAL = (1, 2, 0)

def beside_all(padded):
    total = padded[2:, 1:-1, 1:-1] + padded[:-2, 1:-1, 1:-1]
    total = total + padded[1:-1, 2:, 1:-1] + padded[1:-1, :-2, 1:-1]
    return total + padded[1:-1, 1:-1, 2:] + padded[1:-1, 1:-1, :-2]

def central(padded, axis):
    if axis == 0:
        return 0.5 * (padded[2:, 1:-1, 1:-1] - padded[:-2, 1:-1, 1:-1])
    if axis == 1:
        return 0.5 * (padded[1:-1, 2:, 1:-1] - padded[1:-1, :-2, 1:-1])
    return 0.5 * (padded[1:-1, 1:-1, 2:] - padded[1:-1, 1:-1, :-2])

def operate(field, stiffness):
    padded = jnp.pad(field, ((0, 0), (1, 1), (1, 1), (1, 1)))
    spread = central(padded[0], SPATIAL[0]) + central(padded[1], SPATIAL[1]) + central(padded[2], SPATIAL[2])
    spread_pad = jnp.pad(spread, 1)
    parts = [(6.0 + stiffness) * field[member] - beside_all(padded[member]) - KAPPA * central(spread_pad, SPATIAL[member]) for member in range(3)]
    return jnp.stack(parts)

def project(resid, look_vector):
    return jnp.einsum('ec,nep->ncp', look_vector, resid, precision=lax.Precision.HIGHEST).astype(jnp.bfloat16)

def contribute(coeffs, tables, weights):
    total = coeffs.shape[0]
    group = math.gcd(total, 64)
    coefficient_sets = coeffs.reshape(total // group, group, 3, coeffs.shape[2])
    table_groups = tables.reshape(total // group, group)

    def per_group(both_parts):
        block_coefficient_values, block_tables = both_parts
        selected_entries = jnp.take(weights, block_tables, axis=0).astype(jnp.float32)
        return jnp.einsum('aow,awv->aov', block_coefficient_values.astype(jnp.float32), selected_entries, precision=lax.Precision.HIGHEST)
    result = lax.map(per_group, (coefficient_sets, table_groups))
    return result.reshape(total, 3, weights.shape[2])

def reference(observed, predicted, coherence_mask, block_count, block_owner, block_matrix_choice, block_patch, look_vector, interp_weights, depth_kernel, stiffness):
    column = jnp.arange(BPIX, dtype=jnp.int32)
    valid = coherence_mask.astype(jnp.float32) * (column[None, :] < block_count[:, None]).astype(jnp.float32)
    resid = (predicted - observed) * valid[:, None, :]
    scale = lax.rsqrt(jnp.sum(resid * resid) / (EPOCHS * jnp.sum(valid)) + EPS)
    coeffs = project(resid, look_vector)
    sums = contribute(coeffs, block_matrix_choice, interp_weights)
    owner = block_owner[:, 0]
    tile_y = CY // PATCH_Y
    grid_x = owner // N_GY * (CX // PATCH_X) + block_patch // tile_y
    northing_grid = owner % N_GY * tile_y + block_patch % tile_y
    across_x = NX // PATCH_X
    across_y = NY // PATCH_Y
    placed = jax.ops.segment_sum(sums, (grid_x * across_y + northing_grid).astype(jnp.int32), num_segments=across_x * across_y)
    surface = placed.reshape(across_x, across_y, 3, PATCH_X, PATCH_Y).transpose(2, 0, 3, 1, 4).reshape(3, NX, NY)
    source = scale * depth_kernel[None, :, None, None] * surface[:, None, :, :]
    adjoint_field = jnp.zeros_like(source)
    cg_residual = source
    direction = source
    norm_now = jnp.sum(cg_residual * cg_residual)
    for step in range(ITERS):
        image = operate(direction, stiffness)
        alpha = norm_now / jnp.sum(direction * image)
        adjoint_field = adjoint_field + alpha * direction
        cg_residual = cg_residual - alpha * image
        norm_next = jnp.sum(cg_residual * cg_residual)
        direction = cg_residual + norm_next / norm_now * direction
        norm_now = norm_next
    return (adjoint_field, cg_residual)
```

```python
import functools

import jax
import jax.numpy as jnp
from jax import lax
from jax.experimental import pallas as pl
from jax.experimental.pallas import tpu as pltpu
from jax.sharding import PartitionSpec as P

EPOCHS = 4
PATCH_X = 8
PATCH_Y = 16
CAP = 4
LANES = 128
EPS = 1e-06
SHIFT = 8.0
REACH = 4
EDGE = 8
F32 = jnp.float32
VMEM = pl.BlockSpec(memory_space=pltpu.VMEM)
SMEM = pl.BlockSpec(memory_space=pltpu.SMEM)


def block_sums_kernel(owner_ref, patch_ref, coeffs_ref, choice_ref, weights_ref, out_ref, sums_ref, used_ref):
    step = pl.program_id(0)
    blocks = owner_ref.shape[0]
    tables = weights_ref.shape[0]
    owners = out_ref.shape[1]
    choice = choice_ref[...]
    coeffs = coeffs_ref[...]

    @pl.when(step == 0)
    def _():
        sums_ref[...] = jnp.zeros_like(sums_ref)

    total = sums_ref[...]
    for t in range(tables):
        product = jnp.dot(coeffs, weights_ref[t], preferred_element_type=F32)
        total = jnp.where(choice == step * tables + t, product, total)
    sums_ref[...] = total

    @pl.when(step == pl.num_programs(0) - 1)
    def _():
        out_ref[...] = jnp.zeros_like(out_ref)
        lane = lax.broadcasted_iota(jnp.int32, (1, LANES), 1)

        def clear(o, carry):
            used_ref[o] = 0
            return carry

        lax.fori_loop(0, owners, clear, 0)

        def put(b, carry):
            o = owner_ref[b]
            r = used_ref[o]
            used_ref[o] = r + 1
            for c in range(3):
                out_ref[r * 3 + c, pl.ds(o, 1), :] = sums_ref[pl.ds(c * blocks + b, 1), :]
            ids = out_ref[3 * CAP, pl.ds(o, 1), :]
            out_ref[3 * CAP, pl.ds(o, 1), :] = jnp.where(lane == r, patch_ref[b].astype(F32), ids)
            return carry

        lax.fori_loop(0, blocks, put, 0)


def block_sums(owner, patch, coeffs, choice, weights, owners):
    tables, pixels, cells = weights.shape
    blocks = owner.shape[0]
    steps = 8
    per = tables // steps
    return pl.pallas_call(
        block_sums_kernel,
        grid=(steps,),
        out_shape=jax.ShapeDtypeStruct((3 * CAP + 1, owners, cells), F32),
        in_specs=[
            SMEM,
            SMEM,
            pl.BlockSpec((3 * blocks, pixels), lambda i: (0, 0)),
            pl.BlockSpec((3 * blocks, LANES), lambda i: (0, 0)),
            pl.BlockSpec((per, pixels, cells), lambda i: (i, 0, 0)),
        ],
        out_specs=pl.BlockSpec((3 * CAP + 1, owners, cells), lambda i: (0, 0, 0)),
        scratch_shapes=[pltpu.VMEM((3 * blocks, cells), F32), pltpu.SMEM((owners,), jnp.int32)],
        name="block_sums",
    )(owner, patch, coeffs, choice, weights)


def swap_granules(tile, size):
    count = tile.shape[0]
    lanes = tile.shape[1]
    row = lax.broadcasted_iota(jnp.int32, tile.shape, 0)
    granule = lax.broadcasted_iota(jnp.int32, tile.shape, 1) // size
    k = 1
    while k < count:
        low = (row & k) == 0
        same = low == ((granule & k) == 0)
        up = pltpu.roll(pltpu.roll(tile, count - k, 0), k * size, 1)
        down = pltpu.roll(pltpu.roll(tile, k, 0), lanes - k * size, 1)
        tile = jnp.where(same, tile, jnp.where(low, up, down))
        k *= 2
    return tile


def place_kernel(got_ref, out_ref):
    sources, cells = got_ref.shape[1:]
    local_x, local_y = out_ref.shape[1:]
    places_x, places_y = local_x // PATCH_X, local_y // PATCH_Y
    places = places_x * places_y
    place = lax.broadcasted_iota(jnp.int32, (sources, places), 1).astype(F32)
    ids = got_ref[3 * CAP]
    total = jnp.zeros((places, 3 * cells), F32)
    for r in range(CAP):
        hot = (ids[:, r : r + 1] == place).astype(F32)
        total += lax.dot_general(
            hot,
            jnp.concatenate([got_ref[3 * r + c] for c in range(3)], axis=1),
            (((0,), (0,)), ((), ())),
            precision=lax.Precision.HIGHEST,
            preferred_element_type=F32,
        )
    for c in range(3):
        for i in range(places_x):
            tile = total[i * places_y : (i + 1) * places_y, c * cells : (c + 1) * cells]
            out_ref[c, i * PATCH_X : (i + 1) * PATCH_X, :] = swap_granules(tile, PATCH_Y)


def place(got, local_x, local_y):
    return pl.pallas_call(
        place_kernel,
        out_shape=jax.ShapeDtypeStruct((3, local_x, local_y), F32),
        in_specs=[VMEM],
        out_specs=VMEM,
        name="place",
    )(got)


def lane_steps(own, side):
    lane = lax.broadcasted_iota(jnp.int32, own.shape, 1)
    last, first = lane == LANES - 1, lane == 0
    a0, a1 = pltpu.roll(own, LANES - 1, 1), pltpu.roll(side, LANES - 1, 1)
    b0, b1 = pltpu.roll(own, 1, 1), pltpu.roll(side, 1, 1)
    ahead = (jnp.where(last, a1, a0), jnp.where(last, a0, a1))
    behind = (jnp.where(first, b1, b0), jnp.where(first, b0, b1))
    return ahead, behind


def powers_kernel(
    at_ref, depth_ref, beyond_ref, own_ref, left_ref, right_ref, stiff_ref, stiff_side_ref, stiff_beyond_ref,
    tally_ref, one_ref, two_ref, three_ref, row_ref, flat, keep, diag, w1, w2, div,
):
    layers, rows = stiff_ref.shape[0], stiff_ref.shape[1]
    local_x = one_ref.shape[2]
    upper = at_ref[0] == 1
    sign = jnp.where(upper, -1.0, 1.0).astype(F32)
    tall = own_ref.shape[1]

    def layer_of(z):
        return jnp.where(upper, layers - 1 - z, z)

    def depth(z):
        inner = depth_ref[layer_of(jnp.clip(z, 0, layers - 1))]
        outer = beyond_ref[layer_of(jnp.clip(z - layers, 0, layers - 1))]
        return jnp.where(z < 0, 0.0, jnp.where(z < layers, inner, outer))

    lane = lax.broadcasted_iota(jnp.int32, (tall, LANES), 1)
    line = lax.broadcasted_iota(jnp.int32, (tall, LANES), 0)
    outside_x = ((line < EDGE) & (at_ref[1] == 1)) | ((line >= tall - EDGE) & (at_ref[2] == 1))
    half = lane < LANES // 2
    outside_y = (half & (at_ref[4] == 1)) | (jnp.logical_not(half) & (at_ref[3] == 1))
    in0 = jnp.where(outside_x, 0.0, 1.0)
    in1 = jnp.where(outside_x | outside_y, 0.0, 1.0)
    inside = (in0, in1)

    def tiles(c):
        return own_ref[c], jnp.where(half, right_ref[c], left_ref[c])

    def down(v):
        return pltpu.roll(v, tall - 1, 0)

    def up(v):
        return pltpu.roll(v, 1, 0)

    s = [tiles(0), tiles(1), tuple(sign * v for v in tiles(2))]
    moved = [lane_steps(*v) for v in s]
    grad = tuple(
        inside[t] * 0.5 * (down(s[0][t]) - up(s[0][t]) + moved[1][0][t] - moved[1][1][t]) for t in range(2)
    )
    grad_moved = lane_steps(*grad)
    for t in range(2):
        around = [down(s[c][t]) + up(s[c][t]) + moved[c][0][t] + moved[c][1][t] for c in range(3)]
        keep[t] = inside[t]
        for c in range(3):
            flat[t, c] = s[c][t]
        flat[t, 3] = inside[t] * (-around[0] - 0.25 * (down(grad[t]) - up(grad[t])))
        flat[t, 4] = inside[t] * (-around[1] - 0.25 * (grad_moved[0][t] - grad_moved[1][t]))
        flat[t, 5] = inside[t] * (-around[2])
        flat[t, 6] = inside[t] * (-0.25) * (down(s[2][t]) - up(s[2][t]))
        flat[t, 7] = inside[t] * (-0.25) * (moved[2][0][t] - moved[2][1][t])
        flat[t, 8] = inside[t] * (-0.5) * grad[t]

    first = EDGE - REACH
    body = pl.ds(EDGE, rows)
    ahead_x, behind_x = pl.ds(EDGE + 1, rows), pl.ds(EDGE - 1, rows)
    flat_rows = pl.ds(first, rows)

    def apply_first(z, carry):
        d = depth(z)
        before, after = depth(z - 1), depth(z + 1)
        slope = 0.5 * (after - before)
        slope_after = 0.5 * (depth(z + 2) - d)
        slope_before = jnp.where(z > 0, 0.5 * (d - depth(z - 2)), 0.0)
        bend = 0.5 * (slope_after - slope_before)
        sides = before + after
        z_in = layer_of(jnp.minimum(z, layers - 1))
        z_out = jnp.clip(jnp.where(upper, REACH - 1 - (z - layers), z - layers), 0, REACH - 1)
        for t in range(2):
            inner = (stiff_ref if t == 0 else stiff_side_ref)[z_in]
            stiff = jnp.where(z < layers, inner, stiff_beyond_ref[t, z_out])
            centre = stiff + (6.0 - SHIFT)
            diag[z, t] = centre
            for c in range(3):
                v = flat[t, c, flat_rows, :]
                rest = flat[t, 3 + c, flat_rows, :]
                cross = flat[t, 6 + c, flat_rows, :]
                own_part = sides if c < 2 else sides + 0.5 * bend
                w1[c, z + 1, t, body, :] = d * (centre * v + rest) - own_part * v + slope * cross
        return carry

    for c in range(3):
        for t in range(2):
            w1[c, 0, t] = jnp.zeros_like(w1[c, 0, t])
            w2[c, 0, t] = jnp.zeros_like(w2[c, 0, t])
    for t in range(2):
        div[0, t] = jnp.zeros_like(div[0, t])
    lax.fori_loop(0, layers + REACH, apply_first, 0)

    def spread(w, z):
        ahead, behind = lane_steps(w[1, z, 0, body, :], w[1, z, 1, body, :])
        for t in range(2):
            total = w[0, z, t, ahead_x, :] - w[0, z, t, behind_x, :] + ahead[t] - behind[t]
            total += w[2, z + 1, t, body, :] - w[2, z - 1, t, body, :]
            div[z, t, body, :] = keep[t, flat_rows, :] * total

    def spread_first(z, carry):
        spread(w1, z + 1)
        return carry

    lax.fori_loop(0, layers + REACH - 1, spread_first, 0)

    def apply_second(z, carry):
        ahead, behind = lane_steps(div[z + 1, 0, body, :], div[z + 1, 1, body, :])
        for c in range(3):
            yp, ym = lane_steps(w1[c, z + 1, 0, body, :], w1[c, z + 1, 1, body, :])
            for t in range(2):
                around = w1[c, z + 1, t, ahead_x, :] + w1[c, z + 1, t, behind_x, :] + yp[t] + ym[t]
                around += w1[c, z, t, body, :] + w1[c, z + 2, t, body, :]
                if c == 0:
                    slope = div[z + 1, t, ahead_x, :] - div[z + 1, t, behind_x, :]
                elif c == 1:
                    slope = ahead[t] - behind[t]
                else:
                    slope = div[z + 2, t, body, :] - div[z, t, body, :]
                value = diag[z, t] * w1[c, z + 1, t, body, :] - around - 0.125 * slope
                w2[c, z + 1, t, body, :] = keep[t, flat_rows, :] * value
        return carry

    lax.fori_loop(0, layers + REACH - 2, apply_second, 0)

    def spread_second(z, carry):
        spread(w2, z + 1)
        return carry

    lax.fori_loop(0, layers + REACH // 4, spread_second, 0)

    lo = EDGE + REACH
    mid = pl.ds(lo, local_x)
    mid_ahead, mid_behind = pl.ds(lo + 1, local_x), pl.ds(lo - 1, local_x)
    narrow = lax.broadcasted_iota(jnp.int32, (local_x, LANES), 1)
    at_last, at_first = narrow == LANES - 1, narrow == 0

    def sides_of(own, side):
        ahead = jnp.where(at_last, pltpu.roll(side, LANES - 1, 1), pltpu.roll(own, LANES - 1, 1))
        behind = jnp.where(at_first, pltpu.roll(side, 1, 1), pltpu.roll(own, 1, 1))
        return ahead, behind

    def fold(v):
        out = v[0:8]
        for k in range(8, local_x, 8):
            out += v[k : k + 8]
        return out

    def apply_third(z, sums):
        sums = list(sums)
        d = depth(z)
        z_out = layer_of(z)
        ahead, behind = sides_of(div[z + 1, 0, mid, :], div[z + 1, 1, mid, :])
        for c in range(3):
            centre = w2[c, z + 1, 0, mid, :]
            yp, ym = sides_of(centre, w2[c, z + 1, 1, mid, :])
            around = w2[c, z + 1, 0, mid_ahead, :] + w2[c, z + 1, 0, mid_behind, :] + yp + ym
            around += w2[c, z, 0, mid, :] + w2[c, z + 2, 0, mid, :]
            if c == 0:
                slope = div[z + 1, 0, mid_ahead, :] - div[z + 1, 0, mid_behind, :]
            elif c == 1:
                slope = ahead - behind
            else:
                slope = div[z + 2, 0, mid, :] - div[z, 0, mid, :]
            third = diag[z, 0, pl.ds(REACH, local_x), :] * centre - around - 0.125 * slope
            begin = d * flat[0, c, pl.ds(EDGE, local_x), :]
            once = w1[c, z + 1, 0, mid, :]
            factor = sign if c == 2 else None
            for ref, value in ((one_ref, once), (two_ref, centre), (three_ref, third)):
                ref[c, z_out] = value if factor is None else factor * value
            pairs = ((begin, begin), (begin, once), (once, once), (once, centre), (centre, centre), (centre, third))
            for k, (a, b) in enumerate(pairs):
                sums[k] = sums[k] + fold(a * b)
        return tuple(sums)

    zero = jnp.zeros((8, LANES), F32)
    sums = lax.fori_loop(0, layers, apply_third, (zero,) * 6)
    spot = lax.broadcasted_iota(jnp.int32, (1, row_ref.shape[1]), 1)
    row = jnp.zeros((1, row_ref.shape[1]), F32)
    for k in range(6):
        row = jnp.where(spot == k, jnp.sum(sums[k]), row)
    for k in range(2):
        row = jnp.where(spot == 6 + k, tally_ref[k], row)
    row_ref[...] = jnp.broadcast_to(row, row_ref.shape)


def powers(at, depth, beyond, own, left, right, stiff, stiff_side, stiff_beyond, tally, copies):
    layers, rows, lanes = stiff.shape
    tall = own.shape[1]
    local_x = tall - 2 * EDGE
    field = jax.ShapeDtypeStruct((3, layers, local_x, lanes), F32)
    deep = rows + 2 * EDGE
    return pl.pallas_call(
        powers_kernel,
        out_shape=(field, field, field, jax.ShapeDtypeStruct((copies, 16), F32)),
        in_specs=[SMEM] * 3 + [VMEM] * 6 + [SMEM],
        out_specs=(VMEM,) * 4,
        scratch_shapes=[
            pltpu.VMEM((2, 9, tall, lanes), F32),
            pltpu.VMEM((2, tall, lanes), F32),
            pltpu.VMEM((layers + REACH, 2, rows, lanes), F32),
            pltpu.VMEM((3, layers + REACH + 1, 2, deep, lanes), F32),
            pltpu.VMEM((3, layers + REACH - 1, 2, deep, lanes), F32),
            pltpu.VMEM((layers + REACH, 2, deep, lanes), F32),
        ],
        name="powers",
    )(at, depth, beyond, own, left, right, stiff, stiff_side, stiff_beyond, tally)


def step_factors(nu):
    def inner(a, b):
        total = None
        for i, u in enumerate(a):
            for j, v in enumerate(b):
                term = u * v * nu[i + j]
                total = term if total is None else total + term
        return total

    def applied(a):
        out = [SHIFT * u for u in a] + [jnp.zeros_like(nu[0])]
        for i, u in enumerate(a):
            out[i + 1] = out[i + 1] + u
        return out

    def plus(a, factor, b):
        size = max(len(a), len(b))
        out = []
        for i in range(size):
            if i >= len(b):
                out.append(a[i])
            elif i >= len(a):
                out.append(factor * b[i])
            else:
                out.append(a[i] + factor * b[i])
        return out

    one = jnp.ones_like(nu[0])
    resid, along = [one], [one]
    found = [jnp.zeros_like(one)]
    now = nu[0]
    for step in range(3):
        image = applied(along)
        alpha = now / inner(along, image)
        found = plus(found, alpha, along)
        resid = plus(resid, -alpha, image)
        if step < 2:
            new = inner(resid, resid)
            along = plus(resid, new / now, along)
            now = new
    return found, resid


def finish_kernel(depth_ref, got_ref, surface_ref, one_ref, two_ref, three_ref, field_ref, resid_ref):
    block = one_ref.shape[1]
    step = pl.program_id(0)
    totals = jnp.sum(got_ref[...], axis=0, keepdims=True)
    values = [totals[:, k : k + 1] for k in range(8)]
    found, resid = step_factors(values[:6])
    scale = lax.rsqrt(values[6] / (EPOCHS * values[7]) + EPS)
    found = [scale * v for v in found]
    resid = [scale * v for v in resid]
    for z in range(block):
        d = depth_ref[step * block + z]
        for c in range(3):
            begin = d * surface_ref[c]
            once, twice = one_ref[c, z], two_ref[c, z]
            field_ref[c, z] = found[0] * begin + found[1] * once + found[2] * twice
            resid_ref[c, z] = resid[0] * begin + resid[1] * once + resid[2] * twice + resid[3] * three_ref[c, z]


def finish(depth, got, surface, one, two, three):
    layers = one.shape[1]
    block = 4
    spec = pl.BlockSpec((3, block) + one.shape[2:], lambda i: (0, i, 0, 0))
    field = jax.ShapeDtypeStruct(one.shape, F32)
    return pl.pallas_call(
        finish_kernel,
        grid=(layers // block,),
        out_shape=(field, field),
        in_specs=[
            SMEM,
            pl.BlockSpec(got.shape, lambda i: (0, 0)),
            pl.BlockSpec(surface.shape, lambda i: (0, 0, 0)),
            spec,
            spec,
            spec,
        ],
        out_specs=(spec, spec),
        name="finish",
    )(depth, got, surface, one, two, three)


def from_below(value, axis):
    count = lax.axis_size(axis)
    return lax.ppermute(value, axis, [(i, i + 1) for i in range(count - 1)])


def from_above(value, axis):
    count = lax.axis_size(axis)
    return lax.ppermute(value, axis, [(i + 1, i) for i in range(count - 1)])


def from_partner(value, axis):
    return lax.ppermute(value, axis, [(0, 1), (1, 0)])


def beside(left, right):
    lane = lax.broadcasted_iota(jnp.int32, left.shape, left.ndim - 1)
    return jnp.where(lane < LANES // 2, right, left)


def per_device(
    observed,
    predicted,
    coherence_mask,
    block_count,
    block_owner,
    block_matrix_choice,
    block_patch,
    look_vector,
    interp_weights,
    depth_kernel,
    stiffness,
):
    blocks, _, pixels = observed.shape
    layers, local_x, local_y = stiffness.shape
    owners = lax.axis_size("gx") * lax.axis_size("gy")
    copies = owners * lax.axis_size("gz")
    gx, gy, gz = (lax.axis_index(a) for a in ("gx", "gy", "gz"))

    tall = jnp.concatenate(
        [
            from_below(stiffness[:, local_x - REACH :, :], "gx"),
            stiffness,
            from_above(stiffness[:, :REACH, :], "gx"),
        ],
        axis=1,
    )
    stiff_side = beside(from_below(tall, "gy"), from_above(tall, "gy"))
    start = jnp.where(gz == 0, layers - REACH, 0)
    stiff_beyond = from_partner(
        jnp.stack([lax.dynamic_slice_in_dim(v, start, REACH, axis=0) for v in (tall, stiff_side)]), "gz"
    )
    depth_beyond = from_partner(depth_kernel, "gz")

    column = lax.broadcasted_iota(jnp.int32, (blocks, pixels), 1)
    valid = coherence_mask.astype(F32) * (column < block_count[:, None]).astype(F32)
    resid = (predicted - observed) * valid[:, None, :]
    tally = jnp.stack([jnp.sum(resid * resid), jnp.sum(valid)])
    coeffs = jnp.stack(
        [sum(look_vector[e, c] * resid[:, e, :] for e in range(EPOCHS)) for c in range(3)]
    ).astype(jnp.bfloat16)
    choice = jnp.broadcast_to(block_matrix_choice[None, :, None], (3, blocks, LANES))
    sums = block_sums(
        block_owner[:, 0],
        block_patch,
        coeffs.reshape(3 * blocks, pixels),
        choice.reshape(3 * blocks, LANES),
        interp_weights,
        owners,
    )
    got = lax.all_to_all(sums, ("gx", "gy"), split_axis=1, concat_axis=1, tiled=True)
    part = place(got, local_x, local_y)
    surface = part + from_partner(part, "gz")
    own = jnp.concatenate(
        [
            from_below(surface[:, local_x - EDGE :, :], "gx"),
            surface,
            from_above(surface[:, :EDGE, :], "gx"),
        ],
        axis=1,
    )
    left, right = from_below(own, "gy"), from_above(own, "gy")
    at = jnp.stack(
        [
            gz,
            (gx == 0).astype(jnp.int32),
            (gx == lax.axis_size("gx") - 1).astype(jnp.int32),
            (gy == 0).astype(jnp.int32),
            (gy == lax.axis_size("gy") - 1).astype(jnp.int32),
        ]
    )
    one, two, three, rows = powers(
        at, depth_kernel, depth_beyond, own, left, right, tall, stiff_side, stiff_beyond, tally, copies
    )
    rows = lax.all_to_all(rows, ("gx", "gy", "gz"), split_axis=0, concat_axis=0, tiled=True)
    return finish(depth_kernel, rows, surface, one, two, three)


def solution(mesh):
    in_specs = (
        P(("grp", "gx", "gy", "gz"), None, None),
        P(("grp", "gx", "gy", "gz"), None, None),
        P(("grp", "gx", "gy", "gz"), None),
        P(("grp", "gx", "gy", "gz")),
        P(("grp", "gx", "gy", "gz"), None),
        P(("grp", "gx", "gy", "gz")),
        P(("grp", "gx", "gy", "gz")),
        P(),
        P(),
        P(("grp", "gz")),
        P(("grp", "gz"), "gx", "gy"),
    )
    out_specs = (P(None, ("grp", "gz"), "gx", "gy"), P(None, ("grp", "gz"), "gx", "gy"))
    return jax.shard_map(
        per_device, mesh=mesh, in_specs=in_specs, out_specs=out_specs, check_vma=False
    )
```

```python
import functools
import math

import jax
import jax.numpy as jnp
from jax import lax
from jax.experimental import pallas as pl
from jax.experimental.pallas import tpu as pltpu
from jax.sharding import PartitionSpec as P

EPOCHS = 4
PATCH_X = 8
PATCH_Y = 16
CAP = 4
LANES = 128
EPS = 1e-06
SHIFT = 8.0
REACH = 4
EDGE = 8
ROW = 16
PIECES = 4
F32 = jnp.float32
VMEM = pl.BlockSpec(memory_space=pltpu.VMEM)
SMEM = pl.BlockSpec(memory_space=pltpu.SMEM)


def column(ref, first, count, lanes):
    row = lax.broadcasted_iota(jnp.int32, (count, lanes), 0)
    out = jnp.full((count, lanes), ref[first], jnp.int32)
    for i in range(1, count):
        out = jnp.where(row == i, ref[first + i], out)
    return out


def project_kernel(count_ref, look_ref, observed_ref, predicted_ref, mask_ref, coeffs_ref, tally_ref):
    blocks, _, pixels = observed_ref.shape
    group = 16
    place = lax.broadcasted_iota(jnp.int32, (group, pixels), 1)
    squares = jnp.zeros((group, pixels), F32)
    weight = jnp.zeros((group, pixels), F32)
    for g in range(0, blocks, group):
        rows = slice(g, g + group)
        inside = place < column(count_ref, g, group, pixels)
        valid = jnp.where(inside, mask_ref[rows, :].astype(F32), 0.0)
        weight += valid
        resid = []
        for e in range(EPOCHS):
            r = (predicted_ref[rows, e, :] - observed_ref[rows, e, :]) * valid
            squares += r * r
            resid.append(r)
        for c in range(3):
            total = look_ref[0, c] * resid[0]
            for e in range(1, EPOCHS):
                total += look_ref[e, c] * resid[e]
            coeffs_ref[c * blocks + g : c * blocks + g + group, :] = total.astype(jnp.bfloat16)
    spot = lax.broadcasted_iota(jnp.int32, tally_ref.shape, 1)
    tally = jnp.where(spot == 6, jnp.sum(squares), 0.0)
    tally_ref[...] = jnp.where(spot == 7, jnp.sum(weight), tally)


def project(count, look, observed, predicted, mask):
    blocks, _, pixels = observed.shape
    return pl.pallas_call(
        project_kernel,
        out_shape=(
            jax.ShapeDtypeStruct((3 * blocks, pixels), jnp.bfloat16),
            jax.ShapeDtypeStruct((1, ROW), F32),
        ),
        in_specs=[SMEM, SMEM, VMEM, VMEM, VMEM],
        out_specs=(VMEM, VMEM),
        compiler_params=pltpu.CompilerParams(vmem_limit_bytes=8 << 20),
        cost_estimate=pl.CostEstimate(flops=8_000_000, bytes_accessed=1 << 20, transcendentals=0),
        name="project",
    )(count, look, observed, predicted, mask)


def block_sums_kernel(
    owner_ref, patch_ref, choice_ref, coeffs_ref, weights_ref, below_ref, own_ref, above_ref,
    out_ref, tall_ref, packed_ref, sums_ref, slots_ref, used_ref, ids_ref, rank_ref,
):
    blocks = owner_ref.shape[0]
    tables = weights_ref.shape[0]
    owners, lanes = slots_ref.shape[1:]

    layers, local_x = own_ref.shape[:2]
    lane = lax.broadcasted_iota(jnp.int32, (local_x + 2 * REACH, lanes), 1)
    packed = jnp.zeros((local_x + 2 * REACH, lanes), F32)
    for z in range(layers):
        tall_ref[z, 0:REACH, :] = below_ref[z]
        tall_ref[z, REACH : REACH + local_x, :] = own_ref[z]
        tall_ref[z, REACH + local_x :, :] = above_ref[z]
        moved = pltpu.roll(tall_ref[z], (2 * REACH * z + REACH) % lanes, 1)
        packed = jnp.where(lane // (2 * REACH) == z, moved, packed)
    packed_ref[...] = packed

    for o in range(owners):
        used_ref[o] = 0
        for r in range(CAP):
            ids_ref[o * CAP + r] = 0
    for b in range(blocks):
        o = owner_ref[b]
        r = used_ref[o]
        used_ref[o] = r + 1
        rank_ref[b] = r
        ids_ref[o * CAP + r] = patch_ref[b]

    choice = jnp.concatenate([column(choice_ref, g, 8, lanes) for g in range(0, blocks, 8)] * 3, axis=0)
    coeffs = coeffs_ref[...]
    total = jnp.zeros(sums_ref.shape, F32)
    for t in range(tables):
        product = jnp.dot(coeffs, weights_ref[t], preferred_element_type=F32)
        total = jnp.where(choice == t, product, total)
    sums_ref[...] = total

    slots_ref[...] = jnp.zeros_like(slots_ref)
    for b in range(blocks):
        o, r = owner_ref[b], rank_ref[b]
        for c in range(3):
            slots_ref[r * 3 + c, pl.ds(o, 1), :] = sums_ref[c * blocks + b : c * blocks + b + 1, :]
    for k in range(3 * CAP):
        out_ref[:, k * lanes : (k + 1) * lanes] = slots_ref[k]
    spot = lax.broadcasted_iota(jnp.int32, (8, lanes), 1)
    spot = jnp.where(spot < CAP, lax.broadcasted_iota(jnp.int32, (8, lanes), 0) * CAP + spot, -1)
    for g in range(0, owners, 8):
        ids = jnp.zeros((8, lanes), jnp.int32)
        for k in range(8 * CAP):
            ids = jnp.where(spot == k, ids_ref[g * CAP + k], ids)
        out_ref[g : g + 8, 3 * CAP * lanes :] = ids.astype(F32)


def block_sums(owner, patch, choice, coeffs, weights, below, own, above, owners):
    tables, pixels, cells = weights.shape
    blocks = owner.shape[0]
    layers, local_x, lanes = own.shape
    rows = local_x + 2 * REACH
    return pl.pallas_call(
        block_sums_kernel,
        out_shape=(
            jax.ShapeDtypeStruct((owners, (3 * CAP + 1) * cells), F32),
            jax.ShapeDtypeStruct((layers, rows, lanes), F32),
            jax.ShapeDtypeStruct((rows, lanes), F32),
        ),
        in_specs=[SMEM] * 3 + [VMEM] * 5,
        out_specs=(VMEM,) * 3,
        scratch_shapes=[
            pltpu.VMEM((3 * blocks, cells), F32),
            pltpu.VMEM((3 * CAP, owners, cells), F32),
            pltpu.SMEM((owners,), jnp.int32),
            pltpu.SMEM((owners * CAP,), jnp.int32),
            pltpu.SMEM((blocks,), jnp.int32),
        ],
        compiler_params=pltpu.CompilerParams(vmem_limit_bytes=8 << 20),
        cost_estimate=pl.CostEstimate(flops=400_000_000, bytes_accessed=4 << 20, transcendentals=0),
        name="block_sums",
    )(owner, patch, choice, coeffs, weights, below, own, above)


def swap_granules(tile, size):
    count = tile.shape[0]
    lanes = tile.shape[1]
    row = lax.broadcasted_iota(jnp.int32, tile.shape, 0)
    granule = lax.broadcasted_iota(jnp.int32, tile.shape, 1) // size
    k = 1
    while k < count:
        low = (row & k) == 0
        same = low == ((granule & k) == 0)
        up = pltpu.roll(pltpu.roll(tile, count - k, 0), k * size, 1)
        down = pltpu.roll(pltpu.roll(tile, k, 0), lanes - k * size, 1)
        tile = jnp.where(same, tile, jnp.where(low, up, down))
        k *= 2
    return tile


def place_kernel(got_ref, out_ref):
    sources = got_ref.shape[0]
    cells = PATCH_X * PATCH_Y
    local_x, local_y = out_ref.shape[1:]
    places_x, places_y = local_x // PATCH_X, local_y // PATCH_Y
    places = places_x * places_y
    place = lax.broadcasted_iota(jnp.int32, (sources, places), 1).astype(F32)
    ids = got_ref[:, 3 * CAP * cells :]
    total = jnp.zeros((places, 3 * cells), F32)
    for r in range(CAP):
        hot = (ids[:, r : r + 1] == place).astype(F32)
        total += lax.dot_general(
            hot,
            got_ref[:, r * 3 * cells : (r + 1) * 3 * cells],
            (((0,), (0,)), ((), ())),
            precision=lax.Precision.HIGHEST,
            preferred_element_type=F32,
        )
    for c in range(3):
        for i in range(places_x):
            tile = total[i * places_y : (i + 1) * places_y, c * cells : (c + 1) * cells]
            out_ref[c, i * PATCH_X : (i + 1) * PATCH_X, :] = swap_granules(tile, PATCH_Y)


def place(got, local_x, local_y):
    return pl.pallas_call(
        place_kernel,
        out_shape=jax.ShapeDtypeStruct((3, local_x, local_y), F32),
        in_specs=[VMEM],
        out_specs=VMEM,
        compiler_params=pltpu.CompilerParams(vmem_limit_bytes=8 << 20),
        cost_estimate=pl.CostEstimate(flops=40_000_000, bytes_accessed=1 << 19, transcendentals=0),
        name="place",
    )(got)


def lane_steps(own, side):
    lane = lax.broadcasted_iota(jnp.int32, own.shape, 1)
    last, first = lane == LANES - 1, lane == 0
    a0, a1 = pltpu.roll(own, LANES - 1, 1), pltpu.roll(side, LANES - 1, 1)
    b0, b1 = pltpu.roll(own, 1, 1), pltpu.roll(side, 1, 1)
    ahead = (jnp.where(last, a1, a0), jnp.where(last, a0, a1))
    behind = (jnp.where(first, b1, b0), jnp.where(first, b0, b1))
    return ahead, behind


def powers_kernel(
    sizes, at_ref, depth_ref, beyond_ref, own_ref, left_ref, right_ref, stiff_ref, side_ref, partner_ref,
    tally_ref, one_ref, two_ref, three_ref, row_ref, flat, keep, diag, w1, w2, div,
):
    layers, rows = stiff_ref.shape[0], stiff_ref.shape[1]
    local_x = one_ref.shape[2]
    size_x, size_y, size_z = sizes
    at = at_ref[0]
    at_z = lax.rem(at, size_z)
    at_y = lax.rem(lax.div(at, size_z), size_y)
    at_x = lax.div(at, size_z * size_y)
    upper = at_z == 1
    sign = jnp.where(upper, -1.0, 1.0).astype(F32)
    tall = own_ref.shape[1]

    def layer_of(z):
        return jnp.where(upper, layers - 1 - z, z)

    def depth(z):
        inner = depth_ref[layer_of(jnp.clip(z, 0, layers - 1))]
        outer = beyond_ref[layer_of(jnp.clip(z - layers, 0, layers - 1))]
        return jnp.where(z < 0, 0.0, jnp.where(z < layers, inner, outer))

    lane = lax.broadcasted_iota(jnp.int32, (tall, LANES), 1)
    line = lax.broadcasted_iota(jnp.int32, (tall, LANES), 0)
    outside_x = ((line < EDGE) & (at_x == 0)) | ((line >= tall - EDGE) & (at_x == size_x - 1))
    half = lane < LANES // 2
    outside_y = (half & (at_y == size_y - 1)) | (jnp.logical_not(half) & (at_y == 0))
    in0 = jnp.where(outside_x, 0.0, 1.0)
    in1 = jnp.where(outside_x | outside_y, 0.0, 1.0)
    inside = (in0, in1)

    def tiles(c):
        return own_ref[c], jnp.where(half, right_ref[c], left_ref[c])

    def down(v):
        return pltpu.roll(v, tall - 1, 0)

    def up(v):
        return pltpu.roll(v, 1, 0)

    s = [tiles(0), tiles(1), tuple(sign * v for v in tiles(2))]
    moved = [lane_steps(*v) for v in s]
    grad = tuple(
        inside[t] * 0.5 * (down(s[0][t]) - up(s[0][t]) + moved[1][0][t] - moved[1][1][t]) for t in range(2)
    )
    grad_moved = lane_steps(*grad)
    for t in range(2):
        around = [down(s[c][t]) + up(s[c][t]) + moved[c][0][t] + moved[c][1][t] for c in range(3)]
        keep[t] = inside[t]
        for c in range(3):
            flat[t, c] = s[c][t]
        flat[t, 3] = inside[t] * (-around[0] - 0.25 * (down(grad[t]) - up(grad[t])))
        flat[t, 4] = inside[t] * (-around[1] - 0.25 * (grad_moved[0][t] - grad_moved[1][t]))
        flat[t, 5] = inside[t] * (-around[2])
        flat[t, 6] = inside[t] * (-0.25) * (down(s[2][t]) - up(s[2][t]))
        flat[t, 7] = inside[t] * (-0.25) * (moved[2][0][t] - moved[2][1][t])
        flat[t, 8] = inside[t] * (-0.5) * grad[t]

    first = EDGE - REACH
    body = pl.ds(EDGE, rows)
    ahead_x, behind_x = pl.ds(EDGE + 1, rows), pl.ds(EDGE - 1, rows)
    flat_rows = pl.ds(first, rows)

    def apply_first(z, carry):
        d = depth(z)
        before, after = depth(z - 1), depth(z + 1)
        slope = 0.5 * (after - before)
        slope_after = 0.5 * (depth(z + 2) - d)
        slope_before = jnp.where(z > 0, 0.5 * (d - depth(z - 2)), 0.0)
        bend = 0.5 * (slope_after - slope_before)
        sides = before + after
        z_in = layer_of(jnp.minimum(z, layers - 1))
        z_out = jnp.clip(jnp.where(upper, REACH - 1 - (z - layers), z - layers), 0, REACH - 1)
        here = z < layers
        packed = jnp.where(here, side_ref[...], partner_ref[REACH])
        which = jnp.where(here, z_in, jnp.where(upper, layers - REACH, 0) + z_out)
        turn = LANES - REACH - 2 * REACH * which
        for t in range(2):
            if t == 0:
                stiff = jnp.where(here, stiff_ref[z_in], partner_ref[z_out])
            else:
                stiff = pltpu.roll(packed, turn, 1)
            centre = stiff + (6.0 - SHIFT)
            diag[z, t] = centre
            for c in range(3):
                v = flat[t, c, flat_rows, :]
                rest = flat[t, 3 + c, flat_rows, :]
                cross = flat[t, 6 + c, flat_rows, :]
                own_part = sides if c < 2 else sides + 0.5 * bend
                w1[c, z + 1, t, body, :] = d * (centre * v + rest) - own_part * v + slope * cross
        return carry

    for c in range(3):
        for t in range(2):
            w1[c, 0, t] = jnp.zeros_like(w1[c, 0, t])
            w2[c, 0, t] = jnp.zeros_like(w2[c, 0, t])
    for t in range(2):
        div[0, t] = jnp.zeros_like(div[0, t])
    lax.fori_loop(0, layers + REACH, apply_first, 0)

    def spread(w, z):
        ahead, behind = lane_steps(w[1, z, 0, body, :], w[1, z, 1, body, :])
        for t in range(2):
            total = w[0, z, t, ahead_x, :] - w[0, z, t, behind_x, :] + ahead[t] - behind[t]
            total += w[2, z + 1, t, body, :] - w[2, z - 1, t, body, :]
            div[z, t, body, :] = keep[t, flat_rows, :] * total

    def spread_first(z, carry):
        spread(w1, z + 1)
        return carry

    lax.fori_loop(0, layers + REACH - 1, spread_first, 0)

    def apply_second(z, carry):
        ahead, behind = lane_steps(div[z + 1, 0, body, :], div[z + 1, 1, body, :])
        for c in range(3):
            yp, ym = lane_steps(w1[c, z + 1, 0, body, :], w1[c, z + 1, 1, body, :])
            for t in range(2):
                around = w1[c, z + 1, t, ahead_x, :] + w1[c, z + 1, t, behind_x, :] + yp[t] + ym[t]
                around += w1[c, z, t, body, :] + w1[c, z + 2, t, body, :]
                if c == 0:
                    slope = div[z + 1, t, ahead_x, :] - div[z + 1, t, behind_x, :]
                elif c == 1:
                    slope = ahead[t] - behind[t]
                else:
                    slope = div[z + 2, t, body, :] - div[z, t, body, :]
                value = diag[z, t] * w1[c, z + 1, t, body, :] - around - 0.125 * slope
                w2[c, z + 1, t, body, :] = keep[t, flat_rows, :] * value
        return carry

    lax.fori_loop(0, layers + REACH - 2, apply_second, 0)

    def spread_second(z, carry):
        spread(w2, z + 1)
        return carry

    lax.fori_loop(0, layers + REACH // 4, spread_second, 0)

    lo = EDGE + REACH
    mid = pl.ds(lo, local_x)
    mid_ahead, mid_behind = pl.ds(lo + 1, local_x), pl.ds(lo - 1, local_x)
    narrow = lax.broadcasted_iota(jnp.int32, (local_x, LANES), 1)
    at_last, at_first = narrow == LANES - 1, narrow == 0

    def sides_of(own, side):
        ahead = jnp.where(at_last, pltpu.roll(side, LANES - 1, 1), pltpu.roll(own, LANES - 1, 1))
        behind = jnp.where(at_first, pltpu.roll(side, 1, 1), pltpu.roll(own, 1, 1))
        return ahead, behind

    def fold(v):
        out = v[0:8]
        for k in range(8, local_x, 8):
            out += v[k : k + 8]
        return out

    def apply_third(z, sums):
        sums = list(sums)
        d = depth(z)
        z_out = layer_of(z)
        ahead, behind = sides_of(div[z + 1, 0, mid, :], div[z + 1, 1, mid, :])
        for c in range(3):
            centre = w2[c, z + 1, 0, mid, :]
            yp, ym = sides_of(centre, w2[c, z + 1, 1, mid, :])
            around = w2[c, z + 1, 0, mid_ahead, :] + w2[c, z + 1, 0, mid_behind, :] + yp + ym
            around += w2[c, z, 0, mid, :] + w2[c, z + 2, 0, mid, :]
            if c == 0:
                slope = div[z + 1, 0, mid_ahead, :] - div[z + 1, 0, mid_behind, :]
            elif c == 1:
                slope = ahead - behind
            else:
                slope = div[z + 2, 0, mid, :] - div[z, 0, mid, :]
            third = diag[z, 0, pl.ds(REACH, local_x), :] * centre - around - 0.125 * slope
            begin = d * flat[0, c, pl.ds(EDGE, local_x), :]
            once = w1[c, z + 1, 0, mid, :]
            factor = sign if c == 2 else None
            for ref, value in ((one_ref, once), (two_ref, centre), (three_ref, third)):
                ref[c, z_out] = value if factor is None else factor * value
            pairs = ((begin, begin), (begin, once), (once, once), (once, centre), (centre, centre), (centre, third))
            for k, (a, b) in enumerate(pairs):
                sums[k] = sums[k] + fold(a * b)
        return tuple(sums)

    zero = jnp.zeros((8, LANES), F32)
    sums = lax.fori_loop(0, layers, apply_third, (zero,) * 6)
    spot = lax.broadcasted_iota(jnp.int32, (1, ROW), 1)
    row = tally_ref[...]
    for k in range(6):
        row = jnp.where(spot == k, jnp.sum(sums[k]), row)
    row_ref[...] = jnp.broadcast_to(row, row_ref.shape)


def powers(sizes, at, depth, beyond, own, left, right, stiff, side, partner, tally):
    layers, rows, lanes = stiff.shape
    tall = own.shape[1]
    local_x = tall - 2 * EDGE
    field = jax.ShapeDtypeStruct((3, layers, local_x, lanes), F32)
    deep = rows + 2 * EDGE
    return pl.pallas_call(
        functools.partial(powers_kernel, sizes),
        out_shape=(field, field, field, jax.ShapeDtypeStruct((math.prod(sizes), ROW), F32)),
        in_specs=[SMEM] * 3 + [VMEM] * 7,
        out_specs=(VMEM,) * 4,
        scratch_shapes=[
            pltpu.VMEM((2, 9, tall, lanes), F32),
            pltpu.VMEM((2, tall, lanes), F32),
            pltpu.VMEM((layers + REACH, 2, rows, lanes), F32),
            pltpu.VMEM((3, layers + REACH + 1, 2, deep, lanes), F32),
            pltpu.VMEM((3, layers + REACH - 1, 2, deep, lanes), F32),
            pltpu.VMEM((layers + REACH, 2, deep, lanes), F32),
        ],
        compiler_params=pltpu.CompilerParams(vmem_limit_bytes=20 << 20),
        cost_estimate=pl.CostEstimate(flops=100_000_000, bytes_accessed=4 << 20, transcendentals=0),
        name="powers",
    )(at, depth, beyond, own, left, right, stiff, side, partner, tally)


def step_factors(nu):
    def inner(a, b):
        total = None
        for i, u in enumerate(a):
            for j, v in enumerate(b):
                term = u * v * nu[i + j]
                total = term if total is None else total + term
        return total

    def applied(a):
        out = [SHIFT * u for u in a] + [jnp.zeros_like(nu[0])]
        for i, u in enumerate(a):
            out[i + 1] = out[i + 1] + u
        return out

    def plus(a, factor, b):
        size = max(len(a), len(b))
        out = []
        for i in range(size):
            if i >= len(b):
                out.append(a[i])
            elif i >= len(a):
                out.append(factor * b[i])
            else:
                out.append(a[i] + factor * b[i])
        return out

    one = jnp.ones_like(nu[0])
    resid, along = [one], [one]
    found = [jnp.zeros_like(one)]
    now = nu[0]
    for step in range(3):
        image = applied(along)
        alpha = now / inner(along, image)
        found = plus(found, alpha, along)
        resid = plus(resid, -alpha, image)
        if step < 2:
            new = inner(resid, resid)
            along = plus(resid, new / now, along)
            now = new
    return found, resid


def finish_kernel(
    depth_ref, got_ref, surface_ref, one_ref, two_ref, three_ref, field_out, resid_out, field_ref, resid_ref, sems
):
    layers = one_ref.shape[1]
    totals = jnp.sum(got_ref[...], axis=0, keepdims=True)
    values = [totals[:, k : k + 1] for k in range(8)]
    found, resid = step_factors(values[:6])
    scale = lax.rsqrt(values[6] / (EPOCHS * values[7]) + EPS)
    shape = surface_ref.shape[1:]
    found = [jnp.broadcast_to(scale * v, shape) for v in found]
    resid = [jnp.broadcast_to(scale * v, shape) for v in resid]
    chunk = layers // PIECES
    copies = []
    for piece in range(PIECES):
        first = piece * chunk

        def one_layer(k, carry, first=first):
            z = first + k
            d = depth_ref[z]
            for c in range(3):
                begin = d * surface_ref[c]
                once, twice = one_ref[c, z], two_ref[c, z]
                field_ref[c, z] = found[0] * begin + found[1] * once + found[2] * twice
                resid_ref[c, z] = resid[0] * begin + resid[1] * once + resid[2] * twice + resid[3] * three_ref[c, z]
            return carry

        lax.fori_loop(0, chunk, one_layer, 0)
        for k, (src, dst) in enumerate(((field_ref, field_out), (resid_ref, resid_out))):
            part = pl.ds(first, chunk)
            copy = pltpu.make_async_copy(src.at[:, part], dst.at[:, part], sems.at[k, piece])
            copy.start()
            copies.append(copy)
    for copy in copies:
        copy.wait()


def finish(depth, got, surface, one, two, three):
    field = jax.ShapeDtypeStruct(one.shape, F32)
    return pl.pallas_call(
        finish_kernel,
        out_shape=(field, field),
        in_specs=[SMEM] + [VMEM] * 5,
        out_specs=(pl.BlockSpec(memory_space=pl.ANY),) * 2,
        scratch_shapes=[
            pltpu.VMEM(one.shape, F32),
            pltpu.VMEM(one.shape, F32),
            pltpu.SemaphoreType.DMA((2, PIECES)),
        ],
        compiler_params=pltpu.CompilerParams(vmem_limit_bytes=12 << 20),
        cost_estimate=pl.CostEstimate(flops=20_000_000, bytes_accessed=4 << 20, transcendentals=0),
        name="finish",
    )(depth, got, surface, one, two, three)


def from_below(value, axis):
    count = lax.axis_size(axis)
    return lax.ppermute(value, axis, [(i, i + 1) for i in range(count - 1)])


def from_above(value, axis):
    count = lax.axis_size(axis)
    return lax.ppermute(value, axis, [(i + 1, i) for i in range(count - 1)])


def from_partner(value, axis):
    return lax.ppermute(value, axis, [(0, 1), (1, 0)])


def per_device(
    observed,
    predicted,
    coherence_mask,
    block_count,
    block_owner,
    block_matrix_choice,
    block_patch,
    look_vector,
    interp_weights,
    depth_kernel,
    stiffness,
):
    layers, local_x, local_y = stiffness.shape
    sizes = tuple(lax.axis_size(a) for a in ("gx", "gy", "gz"))
    owners = sizes[0] * sizes[1]
    at = lax.axis_index(("gx", "gy", "gz")).astype(jnp.int32).reshape(1)
    upper = lax.axis_index("gz") == 1

    below = from_below(stiffness[:, local_x - REACH :, :], "gx")
    above = from_above(stiffness[:, :REACH, :], "gx")
    coeffs, tally = project(block_count, look_vector, observed, predicted, coherence_mask)
    sums, tall, packed = block_sums(
        block_owner[:, 0], block_patch, block_matrix_choice, coeffs, interp_weights, below, stiffness, above, owners
    )
    packed_left, packed_right = from_below(packed, "gy"), from_above(packed, "gy")
    got = lax.all_to_all(sums, ("gx", "gy"), split_axis=0, concat_axis=0, tiled=True)

    lane = lax.broadcasted_iota(jnp.int32, packed.shape, 1)
    side = jnp.where(lane % (2 * REACH) >= REACH, packed_right, packed_left)
    near = jnp.where(upper, tall[:REACH], tall[layers - REACH :])
    partner = from_partner(jnp.concatenate([near, side[None]]), "gz")
    depth_beyond = from_partner(depth_kernel, "gz")

    part = place(got, local_x, local_y)
    surface = part + from_partner(part, "gz")
    own = jnp.concatenate(
        [
            from_below(surface[:, local_x - EDGE :, :], "gx"),
            surface,
            from_above(surface[:, :EDGE, :], "gx"),
        ],
        axis=1,
    )
    left, right = from_below(own, "gy"), from_above(own, "gy")
    one, two, three, rows = powers(
        sizes, at, depth_kernel, depth_beyond, own, left, right, tall, side, partner, tally
    )
    rows = lax.all_to_all(rows, ("gx", "gy", "gz"), split_axis=0, concat_axis=0, tiled=True)
    return finish(depth_kernel, rows, surface, one, two, three)


def solution(mesh):
    in_specs = (
        P(("grp", "gx", "gy", "gz"), None, None),
        P(("grp", "gx", "gy", "gz"), None, None),
        P(("grp", "gx", "gy", "gz"), None),
        P(("grp", "gx", "gy", "gz")),
        P(("grp", "gx", "gy", "gz"), None),
        P(("grp", "gx", "gy", "gz")),
        P(("grp", "gx", "gy", "gz")),
        P(),
        P(),
        P(("grp", "gz")),
        P(("grp", "gz"), "gx", "gy"),
    )
    out_specs = (P(None, ("grp", "gz"), "gx", "gy"), P(None, ("grp", "gz"), "gx", "gy"))
    return jax.shard_map(
        per_device, mesh=mesh, in_specs=in_specs, out_specs=out_specs, check_vma=False
    )
```

```python
import functools
import math

import jax
import jax.numpy as jnp
from jax import lax
from jax.experimental import pallas as pl
from jax.experimental.pallas import tpu as pltpu
from jax.sharding import PartitionSpec as P


EPOCHS = 4
PATCH_X = 8
PATCH_Y = 16
CAP = 4
LANES = 128
EPS = 1e-06
SHIFT = 8.0
REACH = 4
EDGE = 8
ROW = 16
PIECES = 4
F32 = jnp.float32
VMEM = pl.BlockSpec(memory_space=pltpu.VMEM)
SMEM = pl.BlockSpec(memory_space=pltpu.SMEM)
ANY = pl.BlockSpec(memory_space=pl.ANY)


def column(ref, first, count, lanes):
    row = lax.broadcasted_iota(jnp.int32, (count, lanes), 0)
    out = jnp.full((count, lanes), ref[first], jnp.int32)
    for i in range(1, count):
        out = jnp.where(row == i, ref[first + i], out)
    return out


def front_kernel(
    count_ref, look_ref, owner_ref, patch_ref, choice_ref, observed_hbm, predicted_hbm, mask_hbm, weights_hbm,
    out_ref, tally_ref,
    observed_ref, predicted_ref, mask_ref, weights_ref, coeffs_ref, sums_ref, used_ref, ids_ref, rank_ref, sems,
):
    blocks, _, pixels = observed_ref.shape
    tables, _, lanes = weights_ref.shape
    owners = out_ref.shape[0]

    first = [
        pltpu.make_async_copy(src, dst, sems.at[k])
        for k, (src, dst) in enumerate(
            ((observed_hbm, observed_ref), (predicted_hbm, predicted_ref), (mask_hbm, mask_ref))
        )
    ]
    chunk = tables // PIECES
    second = []
    for piece in range(PIECES):
        part = pl.ds(piece * chunk, chunk)
        second.append(pltpu.make_async_copy(weights_hbm.at[part], weights_ref.at[part], sems.at[len(first) + piece]))
    for copy in first + second:
        copy.start()

    for o in range(owners):
        used_ref[o] = 0
        for r in range(CAP):
            ids_ref[o * CAP + r] = 0
    for b in range(blocks):
        o = owner_ref[b]
        r = used_ref[o]
        used_ref[o] = r + 1
        rank_ref[b] = r
        ids_ref[o * CAP + r] = patch_ref[b]
    out_ref[...] = jnp.zeros_like(out_ref)
    spot = lax.broadcasted_iota(jnp.int32, (1, lanes), 1)
    for o in range(owners):
        ids = jnp.zeros((1, lanes), jnp.int32)
        for r in range(CAP):
            ids = jnp.where(spot == r, ids_ref[o * CAP + r], ids)
        out_ref[o, :, 3 * CAP * lanes :] = ids.astype(F32)
    choice = jnp.concatenate([column(choice_ref, g, 8, lanes) for g in range(0, blocks, 8)] * 3, axis=0)

    for copy in first:
        copy.wait()
    group = 16
    place = lax.broadcasted_iota(jnp.int32, (group, pixels), 1)
    squares = jnp.zeros((group, pixels), F32)
    weight = jnp.zeros((group, pixels), F32)
    for g in range(0, blocks, group):
        rows = slice(g, g + group)
        inside = place < column(count_ref, g, group, pixels)
        valid = jnp.where(inside, mask_ref[rows, :].astype(F32), 0.0)
        weight += valid
        resid = []
        for e in range(EPOCHS):
            r = (predicted_ref[rows, e, :] - observed_ref[rows, e, :]) * valid
            squares += r * r
            resid.append(r)
        for c in range(3):
            total = look_ref[0, c] * resid[0]
            for e in range(1, EPOCHS):
                total += look_ref[e, c] * resid[e]
            coeffs_ref[c * blocks + g : c * blocks + g + group, :] = total.astype(jnp.bfloat16)
    spot = lax.broadcasted_iota(jnp.int32, tally_ref.shape, 1)
    tally = jnp.where(spot == 6, jnp.sum(squares), 0.0)
    tally_ref[...] = jnp.where(spot == 7, jnp.sum(weight), tally)

    coeffs = coeffs_ref[...]
    total = jnp.zeros(sums_ref.shape, F32)
    for piece in range(PIECES):
        second[piece].wait()
        for t in range(piece * chunk, (piece + 1) * chunk):
            product = jnp.dot(coeffs, weights_ref[t], preferred_element_type=F32)
            total = jnp.where(choice == t, product, total)
    sums_ref[...] = total
    for b in range(blocks):
        o, r = owner_ref[b], rank_ref[b]
        for c in range(3):
            at = pl.multiple_of((r * 3 + c) * lanes, lanes)
            out_ref[o, :, pl.ds(at, lanes)] = sums_ref[c * blocks + b : c * blocks + b + 1, :]


def front(count, look, owner, patch, choice, observed, predicted, mask, weights, owners):
    _, pixels, cells = weights.shape
    blocks = owner.shape[0]
    return pl.pallas_call(
        front_kernel,
        out_shape=(
            jax.ShapeDtypeStruct((owners, 1, (3 * CAP + 1) * cells), F32),
            jax.ShapeDtypeStruct((1, ROW), F32),
        ),
        in_specs=[SMEM] * 5 + [ANY] * 4,
        out_specs=(VMEM,) * 2,
        scratch_shapes=[
            pltpu.VMEM(observed.shape, F32),
            pltpu.VMEM(observed.shape, F32),
            pltpu.VMEM(mask.shape, jnp.int32),
            pltpu.VMEM(weights.shape, weights.dtype),
            pltpu.VMEM((3 * blocks, pixels), jnp.bfloat16),
            pltpu.VMEM((3 * blocks, cells), F32),
            pltpu.SMEM((owners,), jnp.int32),
            pltpu.SMEM((owners * CAP,), jnp.int32),
            pltpu.SMEM((blocks,), jnp.int32),
            pltpu.SemaphoreType.DMA((3 + PIECES,)),
        ],
        cost_estimate=pl.CostEstimate(flops=400_000_000, bytes_accessed=4 << 20, transcendentals=0),
        name="front",
    )(count, look, owner, patch, choice, observed, predicted, mask, weights)


def pack_kernel(own_ref, far_ref, out_ref):
    lane = lax.broadcasted_iota(jnp.int32, out_ref.shape[1:], 1)
    for k, ref in enumerate((own_ref, far_ref)):
        packed = jnp.zeros(out_ref.shape[1:], F32)
        for z in range(ref.shape[0]):
            moved = pltpu.roll(ref[z], (2 * REACH * z + REACH) % LANES, 1)
            packed = jnp.where(lane // (2 * REACH) == z, moved, packed)
        out_ref[k] = packed


def pack(own, far):
    return pl.pallas_call(
        pack_kernel,
        out_shape=jax.ShapeDtypeStruct((2,) + own.shape[1:], F32),
        in_specs=[VMEM] * 2,
        out_specs=VMEM,
        compiler_params=pltpu.CompilerParams(vmem_limit_bytes=4 << 20),
        cost_estimate=pl.CostEstimate(flops=1_000_000, bytes_accessed=1 << 18, transcendentals=0),
        name="pack",
    )(own, far)


def swap_granules(tile, size):
    count = tile.shape[0]
    lanes = tile.shape[1]
    row = lax.broadcasted_iota(jnp.int32, tile.shape, 0)
    granule = lax.broadcasted_iota(jnp.int32, tile.shape, 1) // size
    k = 1
    while k < count:
        low = (row & k) == 0
        same = low == ((granule & k) == 0)
        up = pltpu.roll(pltpu.roll(tile, count - k, 0), k * size, 1)
        down = pltpu.roll(pltpu.roll(tile, k, 0), lanes - k * size, 1)
        tile = jnp.where(same, tile, jnp.where(low, up, down))
        k *= 2
    return tile


def place_kernel(got_ref, out_ref):
    sources = got_ref.shape[0]
    cells = PATCH_X * PATCH_Y
    local_x, local_y = out_ref.shape[1:]
    places_x, places_y = local_x // PATCH_X, local_y // PATCH_Y
    places = places_x * places_y
    place = lax.broadcasted_iota(jnp.int32, (sources, places), 1).astype(F32)
    ids = got_ref[:, 3 * CAP * cells :]
    total = jnp.zeros((places, 3 * cells), F32)
    for r in range(CAP):
        hot = (ids[:, r : r + 1] == place).astype(F32)
        total += lax.dot_general(
            hot,
            got_ref[:, r * 3 * cells : (r + 1) * 3 * cells],
            (((0,), (0,)), ((), ())),
            precision=lax.Precision.HIGHEST,
            preferred_element_type=F32,
        )
    for c in range(3):
        for i in range(places_x):
            tile = total[i * places_y : (i + 1) * places_y, c * cells : (c + 1) * cells]
            out_ref[c, i * PATCH_X : (i + 1) * PATCH_X, :] = swap_granules(tile, PATCH_Y)


def place(got, local_x, local_y):
    return pl.pallas_call(
        place_kernel,
        out_shape=jax.ShapeDtypeStruct((3, local_x, local_y), F32),
        in_specs=[VMEM],
        out_specs=VMEM,
        compiler_params=pltpu.CompilerParams(vmem_limit_bytes=8 << 20),
        cost_estimate=pl.CostEstimate(flops=40_000_000, bytes_accessed=1 << 19, transcendentals=0),
        name="place",
    )(got)


def lane_steps(own, side):
    lane = lax.broadcasted_iota(jnp.int32, own.shape, 1)
    last, first = lane == LANES - 1, lane == 0
    a0, a1 = pltpu.roll(own, LANES - 1, 1), pltpu.roll(side, LANES - 1, 1)
    b0, b1 = pltpu.roll(own, 1, 1), pltpu.roll(side, 1, 1)
    ahead = (jnp.where(last, a1, a0), jnp.where(last, a0, a1))
    behind = (jnp.where(first, b1, b0), jnp.where(first, b0, b1))
    return ahead, behind


def powers_kernel(
    sizes, layers, at_ref, depth_ref, beyond_ref, own_ref, left_ref, right_ref, stiff_ref,
    tally_ref, one_ref, two_ref, three_ref, row_ref, flat, keep, diag, w1, w2, div1, div2,
):
    rows, local_x = stiff_ref.shape[1], one_ref.shape[2]
    size_x, size_y, size_z = sizes
    at = at_ref[0]
    at_z = lax.rem(at, size_z)
    at_y = lax.rem(lax.div(at, size_z), size_y)
    at_x = lax.div(at, size_z * size_y)
    upper = at_z == 1
    sign = jnp.where(upper, -1.0, 1.0).astype(F32)
    tall = own_ref.shape[1]

    def layer_of(z):
        return jnp.where(upper, layers - 1 - z, z)

    depths = [depth_ref[layer_of(z)] for z in range(layers)]
    depths += [beyond_ref[layer_of(z)] for z in range(REACH + 2)]

    def depth(z):
        return depths[z] if z >= 0 else jnp.zeros((), F32)

    lane = lax.broadcasted_iota(jnp.int32, (tall, LANES), 1)
    line = lax.broadcasted_iota(jnp.int32, (tall, LANES), 0)
    outside_x = ((line < EDGE) & (at_x == 0)) | ((line >= tall - EDGE) & (at_x == size_x - 1))
    half = lane < LANES // 2
    outside_y = (half & (at_y == size_y - 1)) | (jnp.logical_not(half) & (at_y == 0))
    in0 = jnp.where(outside_x, 0.0, 1.0)
    in1 = jnp.where(outside_x | outside_y, 0.0, 1.0)
    inside = (in0, in1)

    def tiles(c):
        return own_ref[c], jnp.where(half, right_ref[c], left_ref[c])

    def down(v):
        return pltpu.roll(v, tall - 1, 0)

    def up(v):
        return pltpu.roll(v, 1, 0)

    s = [tiles(0), tiles(1), tuple(sign * v for v in tiles(2))]
    moved = [lane_steps(*v) for v in s]
    grad = tuple(
        inside[t] * 0.5 * (down(s[0][t]) - up(s[0][t]) + moved[1][0][t] - moved[1][1][t]) for t in range(2)
    )
    grad_moved = lane_steps(*grad)
    for t in range(2):
        around = [down(s[c][t]) + up(s[c][t]) + moved[c][0][t] + moved[c][1][t] for c in range(3)]
        keep[t] = inside[t]
        for c in range(3):
            flat[t, c] = s[c][t]
        flat[t, 3] = inside[t] * (-around[0] - 0.25 * (down(grad[t]) - up(grad[t])))
        flat[t, 4] = inside[t] * (-around[1] - 0.25 * (grad_moved[0][t] - grad_moved[1][t]))
        flat[t, 5] = inside[t] * (-around[2])
        flat[t, 6] = inside[t] * (-0.25) * (down(s[2][t]) - up(s[2][t]))
        flat[t, 7] = inside[t] * (-0.25) * (moved[2][0][t] - moved[2][1][t])
        flat[t, 8] = inside[t] * (-0.5) * grad[t]

    first = EDGE - REACH
    body = pl.ds(EDGE, rows)
    ahead_x, behind_x = pl.ds(EDGE + 1, rows), pl.ds(EDGE - 1, rows)
    flat_rows = pl.ds(first, rows)

    def apply_first(z):
        d = depth(z)
        before, after = depth(z - 1), depth(z + 1)
        slope = 0.5 * (after - before)
        slope_after = 0.5 * (depth(z + 2) - d)
        slope_before = 0.5 * (d - depth(z - 2)) if z > 0 else 0.0
        bend = 0.5 * (slope_after - slope_before)
        sides = before + after
        if z < layers:
            place = layer_of(z)
            stiff, packed, group = stiff_ref[place], stiff_ref[layers + REACH], place
        else:
            group = jnp.where(upper, REACH - 1 - (z - layers), z - layers)
            stiff, packed = stiff_ref[layers + group], stiff_ref[layers + REACH + 1]
        turned = pltpu.roll(packed, LANES - REACH - 2 * REACH * group, 1)
        for t in range(2):
            centre = (stiff if t == 0 else turned) + (6.0 - SHIFT)
            diag[z, t] = centre
            for c in range(3):
                v = flat[t, c, flat_rows, :]
                rest = flat[t, 3 + c, flat_rows, :]
                cross = flat[t, 6 + c, flat_rows, :]
                own_part = sides if c < 2 else sides + 0.5 * bend
                w1[c, z + 1, t, body, :] = d * (centre * v + rest) - own_part * v + slope * cross

    for c in range(3):
        for t in range(2):
            w1[c, 0, t] = jnp.zeros_like(w1[c, 0, t])
            w2[c, 0, t] = jnp.zeros_like(w2[c, 0, t])
    for t in range(2):
        div1[0, t] = jnp.zeros_like(div1[0, t])
        div2[0, t] = jnp.zeros_like(div2[0, t])

    def spread(w, div, z):
        ahead, behind = lane_steps(w[1, z, 0, body, :], w[1, z, 1, body, :])
        for t in range(2):
            total = w[0, z, t, ahead_x, :] - w[0, z, t, behind_x, :] + ahead[t] - behind[t]
            total += w[2, z + 1, t, body, :] - w[2, z - 1, t, body, :]
            div[z, t, body, :] = keep[t, flat_rows, :] * total

    def apply_second(z):
        ahead, behind = lane_steps(div1[z + 1, 0, body, :], div1[z + 1, 1, body, :])
        for c in range(3):
            yp, ym = lane_steps(w1[c, z + 1, 0, body, :], w1[c, z + 1, 1, body, :])
            for t in range(2):
                around = w1[c, z + 1, t, ahead_x, :] + w1[c, z + 1, t, behind_x, :] + yp[t] + ym[t]
                around += w1[c, z, t, body, :] + w1[c, z + 2, t, body, :]
                if c == 0:
                    slope = div1[z + 1, t, ahead_x, :] - div1[z + 1, t, behind_x, :]
                elif c == 1:
                    slope = ahead[t] - behind[t]
                else:
                    slope = div1[z + 2, t, body, :] - div1[z, t, body, :]
                value = diag[z, t] * w1[c, z + 1, t, body, :] - around - 0.125 * slope
                w2[c, z + 1, t, body, :] = keep[t, flat_rows, :] * value

    lo = EDGE + REACH
    mid = pl.ds(lo, local_x)
    mid_ahead, mid_behind = pl.ds(lo + 1, local_x), pl.ds(lo - 1, local_x)
    narrow = lax.broadcasted_iota(jnp.int32, (local_x, LANES), 1)
    at_last, at_first = narrow == LANES - 1, narrow == 0

    def sides_of(own, side):
        ahead = jnp.where(at_last, pltpu.roll(side, LANES - 1, 1), pltpu.roll(own, LANES - 1, 1))
        behind = jnp.where(at_first, pltpu.roll(side, 1, 1), pltpu.roll(own, 1, 1))
        return ahead, behind

    def fold(v):
        out = v[0:8]
        for k in range(8, local_x, 8):
            out += v[k : k + 8]
        return out

    def apply_third(z, sums):
        d = depth(z)
        z_out = layer_of(z)
        ahead, behind = sides_of(div2[z + 1, 0, mid, :], div2[z + 1, 1, mid, :])
        for c in range(3):
            centre = w2[c, z + 1, 0, mid, :]
            yp, ym = sides_of(centre, w2[c, z + 1, 1, mid, :])
            around = w2[c, z + 1, 0, mid_ahead, :] + w2[c, z + 1, 0, mid_behind, :] + yp + ym
            around += w2[c, z, 0, mid, :] + w2[c, z + 2, 0, mid, :]
            if c == 0:
                slope = div2[z + 1, 0, mid_ahead, :] - div2[z + 1, 0, mid_behind, :]
            elif c == 1:
                slope = ahead - behind
            else:
                slope = div2[z + 2, 0, mid, :] - div2[z, 0, mid, :]
            third = diag[z, 0, pl.ds(REACH, local_x), :] * centre - around - 0.125 * slope
            begin = d * flat[0, c, pl.ds(EDGE, local_x), :]
            once = w1[c, z + 1, 0, mid, :]
            factor = sign if c == 2 else None
            for ref, value in ((one_ref, once), (two_ref, centre), (three_ref, third)):
                ref[c, z_out] = value if factor is None else factor * value
            pairs = ((begin, begin), (begin, once), (once, once), (once, centre), (centre, centre), (centre, third))
            for k, (a, b) in enumerate(pairs):
                sums[k] = sums[k] + fold(a * b)

    zero = jnp.zeros((8, LANES), F32)
    sums = [zero] * 6
    for step in range(layers + REACH + 4):
        for stage, (count, lag) in enumerate(((REACH, 0), (REACH - 1, 1), (REACH - 2, 2), (1, 3), (0, 4))):
            z = step - lag
            if not 0 <= z < layers + count:
                continue
            if stage == 0:
                apply_first(z)
            elif stage == 1:
                spread(w1, div1, z + 1)
            elif stage == 2:
                apply_second(z)
            elif stage == 3:
                spread(w2, div2, z + 1)
            else:
                apply_third(z, sums)
    spot = lax.broadcasted_iota(jnp.int32, (1, ROW), 1)
    row = tally_ref[...]
    for k in range(6):
        row = jnp.where(spot == k, jnp.sum(sums[k]), row)
    row_ref[...] = jnp.broadcast_to(row, row_ref.shape)


def powers(sizes, at, depth, beyond, own, left, right, stiff, tally):
    layers = depth.shape[0]
    _, rows, lanes = stiff.shape
    tall = own.shape[1]
    local_x = tall - 2 * EDGE
    field = jax.ShapeDtypeStruct((3, layers, local_x, lanes), F32)
    deep = rows + 2 * EDGE
    return pl.pallas_call(
        functools.partial(powers_kernel, sizes, layers),
        out_shape=(field, field, field, jax.ShapeDtypeStruct((math.prod(sizes), ROW), F32)),
        in_specs=[SMEM] * 3 + [VMEM] * 5,
        out_specs=(VMEM,) * 4,
        scratch_shapes=[
            pltpu.VMEM((2, 9, tall, lanes), F32),
            pltpu.VMEM((2, tall, lanes), F32),
            pltpu.VMEM((layers + REACH, 2, rows, lanes), F32),
            pltpu.VMEM((3, layers + REACH + 1, 2, deep, lanes), F32),
            pltpu.VMEM((3, layers + REACH - 1, 2, deep, lanes), F32),
            pltpu.VMEM((layers + REACH, 2, deep, lanes), F32),
            pltpu.VMEM((layers + REACH // 2, 2, deep, lanes), F32),
        ],
        compiler_params=pltpu.CompilerParams(vmem_limit_bytes=20 << 20),
        cost_estimate=pl.CostEstimate(flops=100_000_000, bytes_accessed=4 << 20, transcendentals=0),
        name="powers",
    )(at, depth, beyond, own, left, right, stiff, tally)


def step_factors(nu):
    def inner(a, b):
        total = None
        for i, u in enumerate(a):
            for j, v in enumerate(b):
                term = u * v * nu[i + j]
                total = term if total is None else total + term
        return total

    def applied(a):
        out = [SHIFT * u for u in a] + [jnp.zeros_like(nu[0])]
        for i, u in enumerate(a):
            out[i + 1] = out[i + 1] + u
        return out

    def plus(a, factor, b):
        size = max(len(a), len(b))
        out = []
        for i in range(size):
            if i >= len(b):
                out.append(a[i])
            elif i >= len(a):
                out.append(factor * b[i])
            else:
                out.append(a[i] + factor * b[i])
        return out

    one = jnp.ones_like(nu[0])
    resid, along = [one], [one]
    found = [jnp.zeros_like(one)]
    now = nu[0]
    for step in range(3):
        image = applied(along)
        alpha = now / inner(along, image)
        found = plus(found, alpha, along)
        resid = plus(resid, -alpha, image)
        if step < 2:
            new = inner(resid, resid)
            along = plus(resid, new / now, along)
            now = new
    return found, resid


def finish_kernel(
    depth_ref, got_ref, surface_ref, one_ref, two_ref, three_ref, field_out, resid_out, field_ref, resid_ref, sems
):
    layers = one_ref.shape[1]
    totals = jnp.sum(got_ref[...], axis=0, keepdims=True)
    values = [totals[:, k : k + 1] for k in range(8)]
    found, resid = step_factors(values[:6])
    scale = lax.rsqrt(values[6] / (EPOCHS * values[7]) + EPS)
    shape = surface_ref.shape[1:]
    found = [jnp.broadcast_to(scale * v, shape) for v in found]
    resid = [jnp.broadcast_to(scale * v, shape) for v in resid]
    chunk = layers // PIECES
    copies = []
    for piece in range(PIECES):
        first = piece * chunk

        def one_layer(k, carry, first=first):
            z = first + k
            d = depth_ref[z]
            for c in range(3):
                begin = d * surface_ref[c]
                once, twice = one_ref[c, z], two_ref[c, z]
                field_ref[c, z] = found[0] * begin + found[1] * once + found[2] * twice
                resid_ref[c, z] = resid[0] * begin + resid[1] * once + resid[2] * twice + resid[3] * three_ref[c, z]
            return carry

        lax.fori_loop(0, chunk, one_layer, 0)
        for k, (src, dst) in enumerate(((field_ref, field_out), (resid_ref, resid_out))):
            part = pl.ds(first, chunk)
            copy = pltpu.make_async_copy(src.at[:, part], dst.at[:, part], sems.at[k, piece])
            copy.start()
            copies.append(copy)
    for copy in copies:
        copy.wait()


def finish(depth, got, surface, one, two, three):
    field = jax.ShapeDtypeStruct(one.shape, F32)
    return pl.pallas_call(
        finish_kernel,
        out_shape=(field, field),
        in_specs=[SMEM] + [VMEM] * 5,
        out_specs=(ANY,) * 2,
        scratch_shapes=[
            pltpu.VMEM(one.shape, F32),
            pltpu.VMEM(one.shape, F32),
            pltpu.SemaphoreType.DMA((2, PIECES)),
        ],
        compiler_params=pltpu.CompilerParams(vmem_limit_bytes=12 << 20),
        cost_estimate=pl.CostEstimate(flops=20_000_000, bytes_accessed=4 << 20, transcendentals=0),
        name="finish",
    )(depth, got, surface, one, two, three)


def from_below(value, axis):
    count = lax.axis_size(axis)
    return lax.ppermute(value, axis, [(i, i + 1) for i in range(count - 1)])


def from_above(value, axis):
    count = lax.axis_size(axis)
    return lax.ppermute(value, axis, [(i + 1, i) for i in range(count - 1)])


def from_partner(value, axis):
    return lax.ppermute(value, axis, [(0, 1), (1, 0)])


def per_device(
    observed,
    predicted,
    coherence_mask,
    block_count,
    block_owner,
    block_matrix_choice,
    block_patch,
    look_vector,
    interp_weights,
    depth_kernel,
    stiffness,
):
    layers, local_x, local_y = stiffness.shape
    sizes = tuple(lax.axis_size(a) for a in ("gx", "gy", "gz"))
    owners = sizes[0] * sizes[1]
    at = lax.axis_index(("gx", "gy", "gz")).astype(jnp.int32).reshape(1)
    upper = lax.axis_index("gz") == 1

    sums, tally = front(
        block_count, look_vector, block_owner[:, 0], block_patch, block_matrix_choice,
        observed, predicted, coherence_mask, interp_weights, owners,
    )
    sums, stiffness, depth_kernel = lax.optimization_barrier((sums, stiffness, depth_kernel))
    got = lax.all_to_all(sums, ("gx", "gy"), split_axis=0, concat_axis=0, tiled=True)
    depth_beyond = from_partner(depth_kernel, "gz")
    far = from_partner(jnp.where(upper, stiffness[:REACH], stiffness[layers - REACH :]), "gz")
    packed = pack(stiffness, far)
    lane = lax.broadcasted_iota(jnp.int32, packed.shape, 2)
    side = jnp.where(lane % (2 * REACH) >= REACH, from_above(packed, "gy"), from_below(packed, "gy"))
    stiff = jnp.concatenate([stiffness, far, side])
    low, high = stiff[:, :REACH, :], stiff[:, local_x - REACH :, :]
    below = from_below(high, "gx")
    above = from_above(low, "gx")
    stiff = jnp.concatenate([below, stiff, above], axis=1)

    part = place(got[:, 0], local_x, local_y)
    surface = part + from_partner(part, "gz")
    own = jnp.concatenate(
        [
            from_below(surface[:, local_x - EDGE :, :], "gx"),
            surface,
            from_above(surface[:, :EDGE, :], "gx"),
        ],
        axis=1,
    )
    left, right = from_below(own, "gy"), from_above(own, "gy")
    one, two, three, rows = powers(
        sizes, at, depth_kernel, depth_beyond, own, left, right, stiff, tally
    )
    rows = lax.all_to_all(rows, ("gx", "gy", "gz"), split_axis=0, concat_axis=0, tiled=True)
    return finish(depth_kernel, rows, surface, one, two, three)


def solution(mesh):
    in_specs = (
        P(("grp", "gx", "gy", "gz"), None, None),
        P(("grp", "gx", "gy", "gz"), None, None),
        P(("grp", "gx", "gy", "gz"), None),
        P(("grp", "gx", "gy", "gz")),
        P(("grp", "gx", "gy", "gz"), None),
        P(("grp", "gx", "gy", "gz")),
        P(("grp", "gx", "gy", "gz")),
        P(),
        P(),
        P(("grp", "gz")),
        P(("grp", "gz"), "gx", "gy"),
    )
    out_specs = (P(None, ("grp", "gz"), "gx", "gy"), P(None, ("grp", "gz"), "gx", "gy"))
    return jax.shard_map(per_device, mesh=mesh, in_specs=in_specs, out_specs=out_specs, check_vma=False)
```

```python
import functools

import jax
import jax.numpy as jnp
from jax import lax
from jax.experimental import pallas as pl
from jax.experimental.pallas import tpu as pltpu
from jax.sharding import PartitionSpec as P


EPOCHS = 4
PATCH_X = 8
PATCH_Y = 16
CAP = 4
LANES = 128
EPS = 1e-06
SHIFT = 8.0
REACH = 4
EDGE = 8
ROW = 16
PIECES = 4
F32 = jnp.float32
VMEM = pl.BlockSpec(memory_space=pltpu.VMEM)
SMEM = pl.BlockSpec(memory_space=pltpu.SMEM)
ANY = pl.BlockSpec(memory_space=pl.ANY)


def column(ref, first, count, lanes):
    row = lax.broadcasted_iota(jnp.int32, (count, lanes), 0)
    out = jnp.full((count, lanes), ref[first], jnp.int32)
    for i in range(1, count):
        out = jnp.where(row == i, ref[first + i], out)
    return out


def front_kernel(
    count_ref, look_ref, owner_ref, patch_ref, choice_ref, observed_hbm, predicted_hbm, mask_hbm, weights_hbm,
    out_ref, tally_ref,
    observed_ref, predicted_ref, mask_ref, weights_ref, coeffs_ref, sums_ref, used_ref, ids_ref, rank_ref, sems,
):
    blocks, _, pixels = observed_ref.shape
    tables, _, lanes = weights_ref.shape
    owners = out_ref.shape[0]

    first = [
        pltpu.make_async_copy(src, dst, sems.at[k])
        for k, (src, dst) in enumerate(
            ((observed_hbm, observed_ref), (predicted_hbm, predicted_ref), (mask_hbm, mask_ref))
        )
    ]
    chunk = tables // PIECES
    second = []
    for piece in range(PIECES):
        part = pl.ds(piece * chunk, chunk)
        second.append(pltpu.make_async_copy(weights_hbm.at[part], weights_ref.at[part], sems.at[len(first) + piece]))
    for copy in first + second:
        copy.start()

    for o in range(owners):
        used_ref[o] = 0
        for r in range(CAP):
            ids_ref[o * CAP + r] = 0
    for b in range(blocks):
        o = owner_ref[b]
        r = used_ref[o]
        used_ref[o] = r + 1
        rank_ref[b] = r
        ids_ref[o * CAP + r] = patch_ref[b]
    out_ref[...] = jnp.zeros_like(out_ref)
    spot = lax.broadcasted_iota(jnp.int32, (1, lanes), 1)
    for o in range(owners):
        ids = jnp.zeros((1, lanes), jnp.int32)
        for r in range(CAP):
            ids = jnp.where(spot == r, ids_ref[o * CAP + r], ids)
        out_ref[o, :, 3 * CAP * lanes :] = ids.astype(F32)
    choice = jnp.concatenate([column(choice_ref, g, 8, lanes) for g in range(0, blocks, 8)] * 3, axis=0)

    for copy in first:
        copy.wait()
    group = 16
    place = lax.broadcasted_iota(jnp.int32, (group, pixels), 1)
    squares = jnp.zeros((group, pixels), F32)
    weight = jnp.zeros((group, pixels), F32)
    for g in range(0, blocks, group):
        rows = slice(g, g + group)
        inside = place < column(count_ref, g, group, pixels)
        valid = jnp.where(inside, mask_ref[rows, :].astype(F32), 0.0)
        weight += valid
        resid = []
        for e in range(EPOCHS):
            r = (predicted_ref[rows, e, :] - observed_ref[rows, e, :]) * valid
            squares += r * r
            resid.append(r)
        for c in range(3):
            total = look_ref[0, c] * resid[0]
            for e in range(1, EPOCHS):
                total += look_ref[e, c] * resid[e]
            coeffs_ref[c * blocks + g : c * blocks + g + group, :] = total.astype(jnp.bfloat16)
    spot = lax.broadcasted_iota(jnp.int32, tally_ref.shape, 1)
    tally = jnp.where(spot == 6, jnp.sum(squares), 0.0)
    tally_ref[...] = jnp.where(spot == 7, jnp.sum(weight), tally)

    coeffs = coeffs_ref[...]
    total = jnp.zeros(sums_ref.shape, F32)
    for piece in range(PIECES):
        second[piece].wait()
        for t in range(piece * chunk, (piece + 1) * chunk):
            product = jnp.dot(coeffs, weights_ref[t], preferred_element_type=F32)
            total = jnp.where(choice == t, product, total)
    sums_ref[...] = total
    for b in range(blocks):
        o, r = owner_ref[b], rank_ref[b]
        for c in range(3):
            at = pl.multiple_of((r * 3 + c) * lanes, lanes)
            out_ref[o, :, pl.ds(at, lanes)] = sums_ref[c * blocks + b : c * blocks + b + 1, :]


def front(count, look, owner, patch, choice, observed, predicted, mask, weights, owners):
    _, pixels, cells = weights.shape
    blocks = owner.shape[0]
    return pl.pallas_call(
        front_kernel,
        out_shape=(
            jax.ShapeDtypeStruct((owners, 1, (3 * CAP + 1) * cells), F32),
            jax.ShapeDtypeStruct((1, ROW), F32),
        ),
        in_specs=[SMEM] * 5 + [ANY] * 4,
        out_specs=(VMEM,) * 2,
        scratch_shapes=[
            pltpu.VMEM(observed.shape, F32),
            pltpu.VMEM(observed.shape, F32),
            pltpu.VMEM(mask.shape, jnp.int32),
            pltpu.VMEM(weights.shape, weights.dtype),
            pltpu.VMEM((3 * blocks, pixels), jnp.bfloat16),
            pltpu.VMEM((3 * blocks, cells), F32),
            pltpu.SMEM((owners,), jnp.int32),
            pltpu.SMEM((owners * CAP,), jnp.int32),
            pltpu.SMEM((blocks,), jnp.int32),
            pltpu.SemaphoreType.DMA((3 + PIECES,)),
        ],
        cost_estimate=pl.CostEstimate(flops=400_000_000, bytes_accessed=4 << 20, transcendentals=0),
        name="front",
    )(count, look, owner, patch, choice, observed, predicted, mask, weights)


def pack_kernel(own_ref, far_ref, out_ref):
    lane = lax.broadcasted_iota(jnp.int32, out_ref.shape[1:], 1)
    for k, ref in enumerate((own_ref, far_ref)):
        packed = jnp.zeros(out_ref.shape[1:], F32)
        for z in range(ref.shape[0]):
            moved = pltpu.roll(ref[z], (2 * REACH * z + REACH) % LANES, 1)
            packed = jnp.where(lane // (2 * REACH) == z, moved, packed)
        out_ref[k] = packed


def pack(own, far):
    return pl.pallas_call(
        pack_kernel,
        out_shape=jax.ShapeDtypeStruct((2,) + own.shape[1:], F32),
        in_specs=[VMEM] * 2,
        out_specs=VMEM,
        compiler_params=pltpu.CompilerParams(vmem_limit_bytes=4 << 20),
        cost_estimate=pl.CostEstimate(flops=1_000_000, bytes_accessed=1 << 18, transcendentals=0),
        name="pack",
    )(own, far)


def swap_granules(tile, size):
    count = tile.shape[0]
    lanes = tile.shape[1]
    row = lax.broadcasted_iota(jnp.int32, tile.shape, 0)
    granule = lax.broadcasted_iota(jnp.int32, tile.shape, 1) // size
    k = 1
    while k < count:
        low = (row & k) == 0
        same = low == ((granule & k) == 0)
        up = pltpu.roll(pltpu.roll(tile, count - k, 0), k * size, 1)
        down = pltpu.roll(pltpu.roll(tile, k, 0), lanes - k * size, 1)
        tile = jnp.where(same, tile, jnp.where(low, up, down))
        k *= 2
    return tile


def place_kernel(got_ref, out_ref, edge_ref):
    sources = got_ref.shape[0]
    cells = PATCH_X * PATCH_Y
    local_x, local_y = out_ref.shape[1:]
    places_x, places_y = local_x // PATCH_X, local_y // PATCH_Y
    places = places_x * places_y
    place = lax.broadcasted_iota(jnp.int32, (sources, places), 1).astype(F32)
    ids = got_ref[:, 3 * CAP * cells :]
    total = jnp.zeros((places, 3 * cells), F32)
    for r in range(CAP):
        hot = (ids[:, r : r + 1] == place).astype(F32)
        total += lax.dot_general(
            hot,
            got_ref[:, r * 3 * cells : (r + 1) * 3 * cells],
            (((0,), (0,)), ((), ())),
            precision=lax.Precision.HIGHEST,
            preferred_element_type=F32,
        )
    for c in range(3):
        for i in range(places_x):
            tile = total[i * places_y : (i + 1) * places_y, c * cells : (c + 1) * cells]
            out_ref[c, i * PATCH_X : (i + 1) * PATCH_X, :] = swap_granules(tile, PATCH_Y)
    lane = lax.broadcasted_iota(jnp.int32, edge_ref.shape, 1)
    packed = jnp.zeros(edge_ref.shape, F32)
    for c in range(3):
        moved = pltpu.roll(out_ref[c], 2 * EDGE * c + EDGE, 1)
        packed = jnp.where(lane // (2 * EDGE) == c, moved, packed)
    edge_ref[...] = packed


def place(got, local_x, local_y):
    return pl.pallas_call(
        place_kernel,
        out_shape=(
            jax.ShapeDtypeStruct((3, local_x, local_y), F32),
            jax.ShapeDtypeStruct((local_x, local_y), F32),
        ),
        in_specs=[VMEM],
        out_specs=(VMEM,) * 2,
        compiler_params=pltpu.CompilerParams(vmem_limit_bytes=8 << 20),
        cost_estimate=pl.CostEstimate(flops=40_000_000, bytes_accessed=1 << 19, transcendentals=0),
        name="place",
    )(got)


def lane_steps(own, side):
    lane = lax.broadcasted_iota(jnp.int32, own.shape, 1)
    last, first = lane == LANES - 1, lane == 0
    a0, a1 = pltpu.roll(own, LANES - 1, 1), pltpu.roll(side, LANES - 1, 1)
    b0, b1 = pltpu.roll(own, 1, 1), pltpu.roll(side, 1, 1)
    ahead = (jnp.where(last, a1, a0), jnp.where(last, a0, a1))
    behind = (jnp.where(first, b1, b0), jnp.where(first, b0, b1))
    return ahead, behind


def powers_kernel(
    sizes, layers, at_ref, depth_ref, beyond_ref, mine_ref, theirs_ref, stiff_ref,
    tally_ref, surface_ref, one_ref, two_ref, three_ref, row_ref, flat, keep, diag, w1, w2, div1, div2,
):
    rows, local_x = stiff_ref.shape[1], one_ref.shape[2]
    size_x, size_y, size_z = sizes
    at = at_ref[0]
    at_z = lax.rem(at, size_z)
    at_y = lax.rem(lax.div(at, size_z), size_y)
    at_x = lax.div(at, size_z * size_y)
    upper = at_z == 1
    sign = jnp.where(upper, -1.0, 1.0).astype(F32)
    tall = mine_ref.shape[1]

    def layer_of(z):
        return jnp.where(upper, layers - 1 - z, z)

    depths = [depth_ref[layer_of(z)] for z in range(layers)]
    depths += [beyond_ref[layer_of(z)] for z in range(REACH + 2)]

    def depth(z):
        return depths[z] if z >= 0 else jnp.zeros((), F32)

    lane = lax.broadcasted_iota(jnp.int32, (tall, LANES), 1)
    line = lax.broadcasted_iota(jnp.int32, (tall, LANES), 0)
    outside_x = ((line < EDGE) & (at_x == 0)) | ((line >= tall - EDGE) & (at_x == size_x - 1))
    half = lane < LANES // 2
    outside_y = (half & (at_y == size_y - 1)) | (jnp.logical_not(half) & (at_y == 0))
    in0 = jnp.where(outside_x, 0.0, 1.0)
    in1 = jnp.where(outside_x | outside_y, 0.0, 1.0)
    inside = (in0, in1)

    edges = mine_ref[3] + theirs_ref[3]

    def tiles(c):
        own = mine_ref[c] + theirs_ref[c]
        surface_ref[c] = own[EDGE : tall - EDGE]
        side = pltpu.roll(edges, LANES - EDGE - 2 * EDGE * c, 1)
        return jnp.where(outside_x, 0.0, own), jnp.where(outside_x | outside_y, 0.0, side)

    def down(v):
        return pltpu.roll(v, tall - 1, 0)

    def up(v):
        return pltpu.roll(v, 1, 0)

    s = [tiles(0), tiles(1), tuple(sign * v for v in tiles(2))]
    moved = [lane_steps(*v) for v in s]
    grad = tuple(
        inside[t] * 0.5 * (down(s[0][t]) - up(s[0][t]) + moved[1][0][t] - moved[1][1][t]) for t in range(2)
    )
    grad_moved = lane_steps(*grad)
    for t in range(2):
        around = [down(s[c][t]) + up(s[c][t]) + moved[c][0][t] + moved[c][1][t] for c in range(3)]
        keep[t] = inside[t]
        for c in range(3):
            flat[t, c] = s[c][t]
        flat[t, 3] = inside[t] * (-around[0] - 0.25 * (down(grad[t]) - up(grad[t])))
        flat[t, 4] = inside[t] * (-around[1] - 0.25 * (grad_moved[0][t] - grad_moved[1][t]))
        flat[t, 5] = inside[t] * (-around[2])
        flat[t, 6] = inside[t] * (-0.25) * (down(s[2][t]) - up(s[2][t]))
        flat[t, 7] = inside[t] * (-0.25) * (moved[2][0][t] - moved[2][1][t])
        flat[t, 8] = inside[t] * (-0.5) * grad[t]

    first = EDGE - REACH
    body = pl.ds(EDGE, rows)
    ahead_x, behind_x = pl.ds(EDGE + 1, rows), pl.ds(EDGE - 1, rows)
    flat_rows = pl.ds(first, rows)

    def apply_first(z):
        d = depth(z)
        before, after = depth(z - 1), depth(z + 1)
        slope = 0.5 * (after - before)
        slope_after = 0.5 * (depth(z + 2) - d)
        slope_before = 0.5 * (d - depth(z - 2)) if z > 0 else 0.0
        bend = 0.5 * (slope_after - slope_before)
        sides = before + after
        if z < layers:
            place = layer_of(z)
            stiff, packed, group = stiff_ref[place], stiff_ref[layers + REACH], place
        else:
            group = jnp.where(upper, REACH - 1 - (z - layers), z - layers)
            stiff, packed = stiff_ref[layers + group], stiff_ref[layers + REACH + 1]
        turned = pltpu.roll(packed, LANES - REACH - 2 * REACH * group, 1)
        for t in range(2):
            centre = (stiff if t == 0 else turned) + (6.0 - SHIFT)
            diag[z, t] = centre
            for c in range(3):
                v = flat[t, c, flat_rows, :]
                rest = flat[t, 3 + c, flat_rows, :]
                cross = flat[t, 6 + c, flat_rows, :]
                own_part = sides if c < 2 else sides + 0.5 * bend
                w1[c, z + 1, t, body, :] = d * (centre * v + rest) - own_part * v + slope * cross

    for c in range(3):
        for t in range(2):
            w1[c, 0, t] = jnp.zeros_like(w1[c, 0, t])
            w2[c, 0, t] = jnp.zeros_like(w2[c, 0, t])
    for t in range(2):
        div1[0, t] = jnp.zeros_like(div1[0, t])
        div2[0, t] = jnp.zeros_like(div2[0, t])

    def spread(w, div, z):
        ahead, behind = lane_steps(w[1, z, 0, body, :], w[1, z, 1, body, :])
        for t in range(2):
            total = w[0, z, t, ahead_x, :] - w[0, z, t, behind_x, :] + ahead[t] - behind[t]
            total += w[2, z + 1, t, body, :] - w[2, z - 1, t, body, :]
            div[z, t, body, :] = keep[t, flat_rows, :] * total

    def apply_second(z):
        ahead, behind = lane_steps(div1[z + 1, 0, body, :], div1[z + 1, 1, body, :])
        for c in range(3):
            yp, ym = lane_steps(w1[c, z + 1, 0, body, :], w1[c, z + 1, 1, body, :])
            for t in range(2):
                around = w1[c, z + 1, t, ahead_x, :] + w1[c, z + 1, t, behind_x, :] + yp[t] + ym[t]
                around += w1[c, z, t, body, :] + w1[c, z + 2, t, body, :]
                if c == 0:
                    slope = div1[z + 1, t, ahead_x, :] - div1[z + 1, t, behind_x, :]
                elif c == 1:
                    slope = ahead[t] - behind[t]
                else:
                    slope = div1[z + 2, t, body, :] - div1[z, t, body, :]
                value = diag[z, t] * w1[c, z + 1, t, body, :] - around - 0.125 * slope
                w2[c, z + 1, t, body, :] = keep[t, flat_rows, :] * value

    lo = EDGE + REACH
    mid = pl.ds(lo, local_x)
    mid_ahead, mid_behind = pl.ds(lo + 1, local_x), pl.ds(lo - 1, local_x)
    narrow = lax.broadcasted_iota(jnp.int32, (local_x, LANES), 1)
    at_last, at_first = narrow == LANES - 1, narrow == 0

    def sides_of(own, side):
        ahead = jnp.where(at_last, pltpu.roll(side, LANES - 1, 1), pltpu.roll(own, LANES - 1, 1))
        behind = jnp.where(at_first, pltpu.roll(side, 1, 1), pltpu.roll(own, 1, 1))
        return ahead, behind

    def fold(v):
        out = v[0:8]
        for k in range(8, local_x, 8):
            out += v[k : k + 8]
        return out

    def apply_third(z, sums):
        d = depth(z)
        z_out = layer_of(z)
        ahead, behind = sides_of(div2[z + 1, 0, mid, :], div2[z + 1, 1, mid, :])
        for c in range(3):
            centre = w2[c, z + 1, 0, mid, :]
            yp, ym = sides_of(centre, w2[c, z + 1, 1, mid, :])
            around = w2[c, z + 1, 0, mid_ahead, :] + w2[c, z + 1, 0, mid_behind, :] + yp + ym
            around += w2[c, z, 0, mid, :] + w2[c, z + 2, 0, mid, :]
            if c == 0:
                slope = div2[z + 1, 0, mid_ahead, :] - div2[z + 1, 0, mid_behind, :]
            elif c == 1:
                slope = ahead - behind
            else:
                slope = div2[z + 2, 0, mid, :] - div2[z, 0, mid, :]
            third = diag[z, 0, pl.ds(REACH, local_x), :] * centre - around - 0.125 * slope
            begin = d * flat[0, c, pl.ds(EDGE, local_x), :]
            once = w1[c, z + 1, 0, mid, :]
            factor = sign if c == 2 else None
            for ref, value in ((one_ref, once), (two_ref, centre), (three_ref, third)):
                ref[c, z_out] = value if factor is None else factor * value
            pairs = ((begin, begin), (begin, once), (once, once), (once, centre), (centre, centre), (centre, third))
            for k, (a, b) in enumerate(pairs):
                sums[k] = sums[k] + fold(a * b)

    zero = jnp.zeros((8, LANES), F32)
    sums = [zero] * 6
    for step in range(layers + REACH + 4):
        for stage, (count, lag) in enumerate(((REACH, 0), (REACH - 1, 1), (REACH - 2, 2), (1, 3), (0, 4))):
            z = step - lag
            if not 0 <= z < layers + count:
                continue
            if stage == 0:
                apply_first(z)
            elif stage == 1:
                spread(w1, div1, z + 1)
            elif stage == 2:
                apply_second(z)
            elif stage == 3:
                spread(w2, div2, z + 1)
            else:
                apply_third(z, sums)
    spot = lax.broadcasted_iota(jnp.int32, (1, ROW), 1)
    row = tally_ref[...]
    for k in range(6):
        row = jnp.where(spot == k, jnp.sum(sums[k]), row)
    row_ref[...] = row


def powers(sizes, at, depth, beyond, mine, theirs, stiff, tally):
    layers = depth.shape[0]
    _, rows, lanes = stiff.shape
    tall = mine.shape[1]
    local_x = tall - 2 * EDGE
    field = jax.ShapeDtypeStruct((3, layers, local_x, lanes), F32)
    deep = rows + 2 * EDGE
    return pl.pallas_call(
        functools.partial(powers_kernel, sizes, layers),
        out_shape=(
            jax.ShapeDtypeStruct((3, local_x, lanes), F32),
            field,
            field,
            field,
            jax.ShapeDtypeStruct((1, ROW), F32),
        ),
        in_specs=[SMEM] * 3 + [VMEM] * 4,
        out_specs=(VMEM,) * 5,
        scratch_shapes=[
            pltpu.VMEM((2, 9, tall, lanes), F32),
            pltpu.VMEM((2, tall, lanes), F32),
            pltpu.VMEM((layers + REACH, 2, rows, lanes), F32),
            pltpu.VMEM((3, layers + REACH + 1, 2, deep, lanes), F32),
            pltpu.VMEM((3, layers + REACH - 1, 2, deep, lanes), F32),
            pltpu.VMEM((layers + REACH, 2, deep, lanes), F32),
            pltpu.VMEM((layers + REACH // 2, 2, deep, lanes), F32),
        ],
        compiler_params=pltpu.CompilerParams(vmem_limit_bytes=20 << 20),
        cost_estimate=pl.CostEstimate(flops=100_000_000, bytes_accessed=4 << 20, transcendentals=0),
        name="powers",
    )(at, depth, beyond, mine, theirs, stiff, tally)


def step_factors(nu):
    def inner(a, b):
        total = None
        for i, u in enumerate(a):
            for j, v in enumerate(b):
                term = u * v * nu[i + j]
                total = term if total is None else total + term
        return total

    def applied(a):
        out = [SHIFT * u for u in a] + [jnp.zeros_like(nu[0])]
        for i, u in enumerate(a):
            out[i + 1] = out[i + 1] + u
        return out

    def plus(a, factor, b):
        size = max(len(a), len(b))
        out = []
        for i in range(size):
            if i >= len(b):
                out.append(a[i])
            elif i >= len(a):
                out.append(factor * b[i])
            else:
                out.append(a[i] + factor * b[i])
        return out

    one = jnp.ones_like(nu[0])
    resid, along = [one], [one]
    found = [jnp.zeros_like(one)]
    now = nu[0]
    for step in range(3):
        image = applied(along)
        alpha = now / inner(along, image)
        found = plus(found, alpha, along)
        resid = plus(resid, -alpha, image)
        if step < 2:
            new = inner(resid, resid)
            along = plus(resid, new / now, along)
            now = new
    return found, resid


def finish_kernel(
    depth_ref, got_ref, surface_ref, one_ref, two_ref, three_ref, field_out, resid_out, field_ref, resid_ref, sems
):
    layers = one_ref.shape[1]
    totals = jnp.sum(got_ref[...], axis=0, keepdims=True)
    values = [totals[:, k : k + 1] for k in range(8)]
    found, resid = step_factors(values[:6])
    scale = lax.rsqrt(values[6] / (EPOCHS * values[7]) + EPS)
    shape = surface_ref.shape[1:]
    found = [jnp.broadcast_to(scale * v, shape) for v in found]
    resid = [jnp.broadcast_to(scale * v, shape) for v in resid]
    chunk = layers // PIECES
    copies = []
    for piece in range(PIECES):
        first = piece * chunk

        def one_layer(k, carry, first=first):
            z = first + k
            d = depth_ref[z]
            for c in range(3):
                begin = d * surface_ref[c]
                once, twice = one_ref[c, z], two_ref[c, z]
                field_ref[c, z] = found[0] * begin + found[1] * once + found[2] * twice
                resid_ref[c, z] = resid[0] * begin + resid[1] * once + resid[2] * twice + resid[3] * three_ref[c, z]
            return carry

        lax.fori_loop(0, chunk, one_layer, 0)
        for k, (src, dst) in enumerate(((field_ref, field_out), (resid_ref, resid_out))):
            part = pl.ds(first, chunk)
            copy = pltpu.make_async_copy(src.at[:, part], dst.at[:, part], sems.at[k, piece])
            copy.start()
            copies.append(copy)
    for copy in copies:
        copy.wait()


def finish(depth, got, surface, one, two, three):
    field = jax.ShapeDtypeStruct(one.shape, F32)
    return pl.pallas_call(
        finish_kernel,
        out_shape=(field, field),
        in_specs=[SMEM] + [VMEM] * 5,
        out_specs=(ANY,) * 2,
        scratch_shapes=[
            pltpu.VMEM(one.shape, F32),
            pltpu.VMEM(one.shape, F32),
            pltpu.SemaphoreType.DMA((2, PIECES)),
        ],
        compiler_params=pltpu.CompilerParams(vmem_limit_bytes=12 << 20),
        cost_estimate=pl.CostEstimate(flops=20_000_000, bytes_accessed=4 << 20, transcendentals=0),
        name="finish",
    )(depth, got, surface, one, two, three)


def from_below(value, axis):
    count = lax.axis_size(axis)
    return lax.ppermute(value, axis, [(i, (i + 1) % count) for i in range(count)])


def from_above(value, axis):
    count = lax.axis_size(axis)
    return lax.ppermute(value, axis, [((i + 1) % count, i) for i in range(count)])


def from_partner(value, axis):
    return lax.ppermute(value, axis, [(0, 1), (1, 0)])


def beside(left, right, width):
    lane = lax.broadcasted_iota(jnp.int32, left.shape, left.ndim - 1)
    return jnp.where(lane % (2 * width) >= width, right, left)


def per_device(
    observed,
    predicted,
    coherence_mask,
    block_count,
    block_owner,
    block_matrix_choice,
    block_patch,
    look_vector,
    interp_weights,
    depth_kernel,
    stiffness,
):
    layers, local_x, local_y = stiffness.shape
    sizes = tuple(lax.axis_size(a) for a in ("gx", "gy", "gz"))
    owners = sizes[0] * sizes[1]
    at = lax.axis_index(("gx", "gy", "gz")).astype(jnp.int32).reshape(1)
    upper = lax.axis_index("gz") == 1

    sums, tally = front(
        block_count, look_vector, block_owner[:, 0], block_patch, block_matrix_choice,
        observed, predicted, coherence_mask, interp_weights, owners,
    )
    sums, stiffness, depth_kernel = lax.optimization_barrier((sums, stiffness, depth_kernel))
    got = lax.all_to_all(sums, ("gx", "gy"), split_axis=0, concat_axis=0, tiled=True)
    depth_beyond = from_partner(depth_kernel, "gz")
    far = from_partner(jnp.where(upper, stiffness[:REACH], stiffness[layers - REACH :]), "gz")
    packed = pack(stiffness, far)
    side = beside(from_below(packed, "gy"), from_above(packed, "gy"), REACH)
    stiff = jnp.concatenate([stiffness, far, side])
    low, high = stiff[:, :REACH, :], stiff[:, local_x - REACH :, :]
    below = from_below(high, "gx")
    above = from_above(low, "gx")
    stiff = jnp.concatenate([below, stiff, above], axis=1)

    part, edges = place(got[:, 0], local_x, local_y)
    side = beside(from_below(edges, "gy"), from_above(edges, "gy"), EDGE)
    mine = jnp.concatenate([part, side[None]])
    mine = jnp.concatenate(
        [from_below(mine[:, local_x - EDGE :, :], "gx"), mine, from_above(mine[:, :EDGE, :], "gx")], axis=1
    )
    surface, one, two, three, row = powers(
        sizes, at, depth_kernel, depth_beyond, mine, from_partner(mine, "gz"), stiff, tally
    )
    rows = jnp.broadcast_to(row + from_partner(row, "gz"), (owners, ROW))
    rows = lax.all_to_all(rows, ("gx", "gy"), split_axis=0, concat_axis=0, tiled=True)
    return finish(depth_kernel, rows, surface, one, two, three)


def solution(mesh):
    in_specs = (
        P(("grp", "gx", "gy", "gz"), None, None),
        P(("grp", "gx", "gy", "gz"), None, None),
        P(("grp", "gx", "gy", "gz"), None),
        P(("grp", "gx", "gy", "gz")),
        P(("grp", "gx", "gy", "gz"), None),
        P(("grp", "gx", "gy", "gz")),
        P(("grp", "gx", "gy", "gz")),
        P(),
        P(),
        P(("grp", "gz")),
        P(("grp", "gz"), "gx", "gy"),
    )
    out_specs = (P(None, ("grp", "gz"), "gx", "gy"), P(None, ("grp", "gz"), "gx", "gy"))
    return jax.shard_map(per_device, mesh=mesh, in_specs=in_specs, out_specs=out_specs, check_vma=False)
```

```python
import functools

import jax
import jax.numpy as jnp
from jax import lax
from jax.experimental import pallas as pl
from jax.experimental.pallas import tpu as pltpu
from jax.sharding import PartitionSpec as P


EPOCHS = 4
PATCH_X = 8
PATCH_Y = 16
CAP = 4
LANES = 128
EPS = 1e-06
SHIFT = 8.0
REACH = 4
EDGE = 8
ROW = 16
PIECES = 4
F32 = jnp.float32
VMEM = pl.BlockSpec(memory_space=pltpu.VMEM)
SMEM = pl.BlockSpec(memory_space=pltpu.SMEM)
ANY = pl.BlockSpec(memory_space=pl.ANY)


def column(ref, first, count, lanes):
    row = lax.broadcasted_iota(jnp.int32, (count, lanes), 0)
    out = jnp.full((count, lanes), ref[first], jnp.int32)
    for i in range(1, count):
        out = jnp.where(row == i, ref[first + i], out)
    return out


def front_kernel(
    count_hbm, look_hbm, owner_hbm, patch_hbm, choice_hbm, observed_hbm, predicted_hbm, mask_hbm, weights_hbm,
    out_ref, tally_ref,
    count_ref, look_ref, owner_ref, patch_ref, choice_ref,
    observed_ref, predicted_ref, mask_ref, weights_ref, coeffs_ref, sums_ref, used_ref, ids_ref, rank_ref, sems,
):
    blocks, _, pixels = observed_ref.shape
    tables, _, lanes = weights_ref.shape
    owners = out_ref.shape[0]

    first = [
        pltpu.make_async_copy(src, dst, sems.at[k])
        for k, (src, dst) in enumerate(
            (
                (owner_hbm, owner_ref),
                (patch_hbm, patch_ref),
                (choice_hbm, choice_ref),
                (count_hbm, count_ref),
                (look_hbm, look_ref),
                (observed_hbm, observed_ref),
                (predicted_hbm, predicted_ref),
                (mask_hbm, mask_ref),
            )
        )
    ]
    chunk = tables // PIECES
    second = []
    for piece in range(PIECES):
        part = pl.ds(piece * chunk, chunk)
        second.append(pltpu.make_async_copy(weights_hbm.at[part], weights_ref.at[part], sems.at[len(first) + piece]))
    for copy in first + second:
        copy.start()
    out_ref[...] = jnp.zeros_like(out_ref)
    for o in range(owners):
        used_ref[o] = 0
        for r in range(CAP):
            ids_ref[o * CAP + r] = 0
    for copy in first[:3]:
        copy.wait()

    for b in range(blocks):
        o = owner_ref[b]
        r = used_ref[o]
        used_ref[o] = r + 1
        rank_ref[b] = r
        ids_ref[o * CAP + r] = patch_ref[b]
    spot = lax.broadcasted_iota(jnp.int32, (1, lanes), 1)
    for o in range(owners):
        ids = jnp.zeros((1, lanes), jnp.int32)
        for r in range(CAP):
            ids = jnp.where(spot == r, ids_ref[o * CAP + r], ids)
        out_ref[o, :, 3 * CAP * lanes :] = ids.astype(F32)
    choice = jnp.concatenate([column(choice_ref, g, 8, lanes) for g in range(0, blocks, 8)] * 3, axis=0)

    for copy in first[3:]:
        copy.wait()
    group = 16
    place = lax.broadcasted_iota(jnp.int32, (group, pixels), 1)
    squares = jnp.zeros((group, pixels), F32)
    weight = jnp.zeros((group, pixels), F32)
    for g in range(0, blocks, group):
        rows = slice(g, g + group)
        inside = place < column(count_ref, g, group, pixels)
        valid = jnp.where(inside, mask_ref[rows, :].astype(F32), 0.0)
        weight += valid
        resid = []
        for e in range(EPOCHS):
            r = (predicted_ref[rows, e, :] - observed_ref[rows, e, :]) * valid
            squares += r * r
            resid.append(r)
        for c in range(3):
            total = look_ref[0, c] * resid[0]
            for e in range(1, EPOCHS):
                total += look_ref[e, c] * resid[e]
            coeffs_ref[c * blocks + g : c * blocks + g + group, :] = total.astype(jnp.bfloat16)
    spot = lax.broadcasted_iota(jnp.int32, tally_ref.shape, 1)
    tally = jnp.where(spot == 6, jnp.sum(squares), 0.0)
    tally_ref[...] = jnp.where(spot == 7, jnp.sum(weight), tally)

    coeffs = coeffs_ref[...]
    total = jnp.zeros(sums_ref.shape, F32)
    for piece in range(PIECES):
        second[piece].wait()
        for t in range(piece * chunk, (piece + 1) * chunk, 2):
            pair = jnp.concatenate([weights_ref[t], weights_ref[t + 1]], axis=1)
            product = jnp.dot(coeffs, pair, preferred_element_type=F32)
            total = jnp.where(choice == t, product[:, :lanes], total)
            total = jnp.where(choice == t + 1, product[:, lanes:], total)
    sums_ref[...] = total
    for b in range(blocks):
        o, r = owner_ref[b], rank_ref[b]
        for c in range(3):
            at = pl.multiple_of((r * 3 + c) * lanes, lanes)
            out_ref[o, :, pl.ds(at, lanes)] = sums_ref[c * blocks + b : c * blocks + b + 1, :]


def front(count, look, owner, patch, choice, observed, predicted, mask, weights, owners):
    _, pixels, cells = weights.shape
    blocks = owner.shape[0]
    return pl.pallas_call(
        front_kernel,
        out_shape=(
            jax.ShapeDtypeStruct((owners, 1, (3 * CAP + 1) * cells), F32),
            jax.ShapeDtypeStruct((1, ROW), F32),
        ),
        in_specs=[ANY] * 9,
        out_specs=(VMEM,) * 2,
        scratch_shapes=[
            pltpu.SMEM((blocks,), jnp.int32),
            pltpu.SMEM(look.shape, F32),
            pltpu.SMEM((blocks,), jnp.int32),
            pltpu.SMEM((blocks,), jnp.int32),
            pltpu.SMEM((blocks,), jnp.int32),
            pltpu.VMEM(observed.shape, F32),
            pltpu.VMEM(observed.shape, F32),
            pltpu.VMEM(mask.shape, jnp.int32),
            pltpu.VMEM(weights.shape, weights.dtype),
            pltpu.VMEM((3 * blocks, pixels), jnp.bfloat16),
            pltpu.VMEM((3 * blocks, cells), F32),
            pltpu.SMEM((owners,), jnp.int32),
            pltpu.SMEM((owners * CAP,), jnp.int32),
            pltpu.SMEM((blocks,), jnp.int32),
            pltpu.SemaphoreType.DMA((8 + PIECES,)),
        ],
        cost_estimate=pl.CostEstimate(flops=400_000_000, bytes_accessed=4 << 20, transcendentals=0),
        name="front",
    )(count, look, owner, patch, choice, observed, predicted, mask, weights)


def pack_kernel(own_ref, far_ref, out_ref):
    lane = lax.broadcasted_iota(jnp.int32, out_ref.shape[1:], 1)
    for k, ref in enumerate((own_ref, far_ref)):
        packed = jnp.zeros(out_ref.shape[1:], F32)
        for z in range(ref.shape[0]):
            moved = pltpu.roll(ref[z], (2 * REACH * z + REACH) % LANES, 1)
            packed = jnp.where(lane // (2 * REACH) == z, moved, packed)
        out_ref[k] = packed


def pack(own, far):
    return pl.pallas_call(
        pack_kernel,
        out_shape=jax.ShapeDtypeStruct((2,) + own.shape[1:], F32),
        in_specs=[VMEM] * 2,
        out_specs=VMEM,
        compiler_params=pltpu.CompilerParams(vmem_limit_bytes=4 << 20),
        cost_estimate=pl.CostEstimate(flops=1_000_000, bytes_accessed=1 << 18, transcendentals=0),
        name="pack",
    )(own, far)


def swap_granules(tile, size):
    count = tile.shape[0]
    lanes = tile.shape[1]
    row = lax.broadcasted_iota(jnp.int32, tile.shape, 0)
    granule = lax.broadcasted_iota(jnp.int32, tile.shape, 1) // size
    k = 1
    while k < count:
        low = (row & k) == 0
        same = low == ((granule & k) == 0)
        up = pltpu.roll(pltpu.roll(tile, count - k, 0), k * size, 1)
        down = pltpu.roll(pltpu.roll(tile, k, 0), lanes - k * size, 1)
        tile = jnp.where(same, tile, jnp.where(low, up, down))
        k *= 2
    return tile


def place_kernel(got_ref, out_ref, edge_ref):
    sources = got_ref.shape[0]
    cells = PATCH_X * PATCH_Y
    local_x, local_y = out_ref.shape[1:]
    places_x, places_y = local_x // PATCH_X, local_y // PATCH_Y
    places = places_x * places_y
    place = lax.broadcasted_iota(jnp.int32, (sources, places), 1).astype(F32)
    ids = got_ref[:, 3 * CAP * cells :]
    total = jnp.zeros((places, 3 * cells), F32)
    for r in range(CAP):
        hot = (ids[:, r : r + 1] == place).astype(F32)
        total += lax.dot_general(
            hot,
            got_ref[:, r * 3 * cells : (r + 1) * 3 * cells],
            (((0,), (0,)), ((), ())),
            precision=lax.Precision.HIGHEST,
            preferred_element_type=F32,
        )
    for c in range(3):
        for i in range(places_x):
            tile = total[i * places_y : (i + 1) * places_y, c * cells : (c + 1) * cells]
            out_ref[c, i * PATCH_X : (i + 1) * PATCH_X, :] = swap_granules(tile, PATCH_Y)
    lane = lax.broadcasted_iota(jnp.int32, edge_ref.shape, 1)
    packed = jnp.zeros(edge_ref.shape, F32)
    for c in range(3):
        moved = pltpu.roll(out_ref[c], 2 * EDGE * c + EDGE, 1)
        packed = jnp.where(lane // (2 * EDGE) == c, moved, packed)
    edge_ref[...] = packed


def place(got, local_x, local_y):
    return pl.pallas_call(
        place_kernel,
        out_shape=(
            jax.ShapeDtypeStruct((3, local_x, local_y), F32),
            jax.ShapeDtypeStruct((local_x, local_y), F32),
        ),
        in_specs=[VMEM],
        out_specs=(VMEM,) * 2,
        compiler_params=pltpu.CompilerParams(vmem_limit_bytes=8 << 20),
        cost_estimate=pl.CostEstimate(flops=40_000_000, bytes_accessed=1 << 19, transcendentals=0),
        name="place",
    )(got)


def lane_steps(own, side):
    lane = lax.broadcasted_iota(jnp.int32, own.shape, 1)
    last, first = lane == LANES - 1, lane == 0
    a0, a1 = pltpu.roll(own, LANES - 1, 1), pltpu.roll(side, LANES - 1, 1)
    b0, b1 = pltpu.roll(own, 1, 1), pltpu.roll(side, 1, 1)
    ahead = (jnp.where(last, a1, a0), jnp.where(last, a0, a1))
    behind = (jnp.where(first, b1, b0), jnp.where(first, b0, b1))
    return ahead, behind


def powers_kernel(
    sizes, layers, at_ref, depth_ref, beyond_ref, mine_ref, theirs_ref, stiff_ref,
    tally_ref, surface_ref, one_ref, two_ref, three_ref, row_ref, flat, keep, diag, w1, w2, div1, div2, across1, across2,
):
    rows, local_x = stiff_ref.shape[1], one_ref.shape[2]
    size_x, size_y, size_z = sizes
    at = at_ref[0]
    at_z = lax.rem(at, size_z)
    at_y = lax.rem(lax.div(at, size_z), size_y)
    at_x = lax.div(at, size_z * size_y)
    upper = at_z == 1
    sign = jnp.where(upper, -1.0, 1.0).astype(F32)
    tall = mine_ref.shape[1]

    def layer_of(z):
        return jnp.where(upper, layers - 1 - z, z)

    depths = [depth_ref[layer_of(z)] for z in range(layers)]
    depths += [beyond_ref[layer_of(z)] for z in range(REACH + 2)]

    def depth(z):
        return depths[z] if z >= 0 else jnp.zeros((), F32)

    lane = lax.broadcasted_iota(jnp.int32, (tall, LANES), 1)
    line = lax.broadcasted_iota(jnp.int32, (tall, LANES), 0)
    outside_x = ((line < EDGE) & (at_x == 0)) | ((line >= tall - EDGE) & (at_x == size_x - 1))
    half = lane < LANES // 2
    outside_y = (half & (at_y == size_y - 1)) | (jnp.logical_not(half) & (at_y == 0))
    in0 = jnp.where(outside_x, 0.0, 1.0)
    in1 = jnp.where(outside_x | outside_y, 0.0, 1.0)
    inside = (in0, in1)

    edges = mine_ref[3] + theirs_ref[3]

    def tiles(c):
        own = mine_ref[c] + theirs_ref[c]
        surface_ref[c] = own[EDGE : tall - EDGE]
        side = pltpu.roll(edges, LANES - EDGE - 2 * EDGE * c, 1)
        return jnp.where(outside_x, 0.0, own), jnp.where(outside_x | outside_y, 0.0, side)

    def down(v):
        return pltpu.roll(v, tall - 1, 0)

    def up(v):
        return pltpu.roll(v, 1, 0)

    s = [tiles(0), tiles(1), tuple(sign * v for v in tiles(2))]
    moved = [lane_steps(*v) for v in s]
    grad = tuple(
        inside[t] * 0.5 * (down(s[0][t]) - up(s[0][t]) + moved[1][0][t] - moved[1][1][t]) for t in range(2)
    )
    grad_moved = lane_steps(*grad)
    for t in range(2):
        around = [down(s[c][t]) + up(s[c][t]) + moved[c][0][t] + moved[c][1][t] for c in range(3)]
        keep[t] = inside[t]
        for c in range(3):
            flat[t, c] = s[c][t]
        flat[t, 3] = inside[t] * (-around[0] - 0.25 * (down(grad[t]) - up(grad[t])))
        flat[t, 4] = inside[t] * (-around[1] - 0.25 * (grad_moved[0][t] - grad_moved[1][t]))
        flat[t, 5] = inside[t] * (-around[2])
        flat[t, 6] = inside[t] * (-0.25) * (down(s[2][t]) - up(s[2][t]))
        flat[t, 7] = inside[t] * (-0.25) * (moved[2][0][t] - moved[2][1][t])
        flat[t, 8] = inside[t] * (-0.5) * grad[t]

    first = EDGE - REACH
    body = pl.ds(EDGE, rows)
    ahead_x, behind_x = pl.ds(EDGE + 1, rows), pl.ds(EDGE - 1, rows)
    flat_rows = pl.ds(first, rows)

    def apply_first(z):
        d = depth(z)
        before, after = depth(z - 1), depth(z + 1)
        slope = 0.5 * (after - before)
        slope_after = 0.5 * (depth(z + 2) - d)
        slope_before = 0.5 * (d - depth(z - 2)) if z > 0 else 0.0
        bend = 0.5 * (slope_after - slope_before)
        sides = before + after
        if z < layers:
            place = layer_of(z)
            stiff, packed, group = stiff_ref[place], stiff_ref[layers + REACH], place
        else:
            group = jnp.where(upper, REACH - 1 - (z - layers), z - layers)
            stiff, packed = stiff_ref[layers + group], stiff_ref[layers + REACH + 1]
        turned = pltpu.roll(packed, LANES - REACH - 2 * REACH * group, 1)
        for t in range(2):
            centre = (stiff if t == 0 else turned) + (6.0 - SHIFT)
            diag[z, t] = centre
            for c in range(3):
                v = flat[t, c, flat_rows, :]
                rest = flat[t, 3 + c, flat_rows, :]
                cross = flat[t, 6 + c, flat_rows, :]
                own_part = sides if c < 2 else sides + 0.5 * bend
                w1[c, z + 1, t, body, :] = d * (centre * v + rest) - own_part * v + slope * cross

    for c in range(3):
        for t in range(2):
            w1[c, 0, t] = jnp.zeros_like(w1[c, 0, t])
            w2[c, 0, t] = jnp.zeros_like(w2[c, 0, t])
    for t in range(2):
        div1[0, t] = jnp.zeros_like(div1[0, t])
        div2[0, t] = jnp.zeros_like(div2[0, t])

    def spread(w, div, across, z):
        ahead, behind = lane_steps(w[1, z, 0, body, :], w[1, z, 1, body, :])
        for t in range(2):
            across[z, t] = ahead[t] + behind[t]
            total = w[0, z, t, ahead_x, :] - w[0, z, t, behind_x, :] + ahead[t] - behind[t]
            total += w[2, z + 1, t, body, :] - w[2, z - 1, t, body, :]
            div[z, t, body, :] = keep[t, flat_rows, :] * total

    def apply_second(z):
        ahead, behind = lane_steps(div1[z + 1, 0, body, :], div1[z + 1, 1, body, :])
        for c in range(3):
            if c != 1:
                yp, ym = lane_steps(w1[c, z + 1, 0, body, :], w1[c, z + 1, 1, body, :])
            for t in range(2):
                around = w1[c, z + 1, t, ahead_x, :] + w1[c, z + 1, t, behind_x, :]
                around += across1[z + 1, t] if c == 1 else yp[t] + ym[t]
                around += w1[c, z, t, body, :] + w1[c, z + 2, t, body, :]
                if c == 0:
                    slope = div1[z + 1, t, ahead_x, :] - div1[z + 1, t, behind_x, :]
                elif c == 1:
                    slope = ahead[t] - behind[t]
                else:
                    slope = div1[z + 2, t, body, :] - div1[z, t, body, :]
                value = diag[z, t] * w1[c, z + 1, t, body, :] - around - 0.125 * slope
                w2[c, z + 1, t, body, :] = keep[t, flat_rows, :] * value

    lo = EDGE + REACH
    mid = pl.ds(lo, local_x)
    mid_ahead, mid_behind = pl.ds(lo + 1, local_x), pl.ds(lo - 1, local_x)
    narrow = lax.broadcasted_iota(jnp.int32, (local_x, LANES), 1)
    at_last, at_first = narrow == LANES - 1, narrow == 0

    def sides_of(own, side):
        ahead = pltpu.roll(jnp.where(at_first, side, own), LANES - 1, 1)
        behind = pltpu.roll(jnp.where(at_last, side, own), 1, 1)
        return ahead, behind

    def fold(v):
        out = v[0:8]
        for k in range(8, local_x, 8):
            out += v[k : k + 8]
        return out

    def apply_third(z, sums):
        d = depth(z)
        z_out = layer_of(z)
        ahead, behind = sides_of(div2[z + 1, 0, mid, :], div2[z + 1, 1, mid, :])
        for c in range(3):
            centre = w2[c, z + 1, 0, mid, :]
            around = w2[c, z + 1, 0, mid_ahead, :] + w2[c, z + 1, 0, mid_behind, :]
            if c == 1:
                around += across2[z + 1, 0, pl.ds(REACH, local_x), :]
            else:
                yp, ym = sides_of(centre, w2[c, z + 1, 1, mid, :])
                around += yp + ym
            around += w2[c, z, 0, mid, :] + w2[c, z + 2, 0, mid, :]
            if c == 0:
                slope = div2[z + 1, 0, mid_ahead, :] - div2[z + 1, 0, mid_behind, :]
            elif c == 1:
                slope = ahead - behind
            else:
                slope = div2[z + 2, 0, mid, :] - div2[z, 0, mid, :]
            third = diag[z, 0, pl.ds(REACH, local_x), :] * centre - around - 0.125 * slope
            begin = d * flat[0, c, pl.ds(EDGE, local_x), :]
            once = w1[c, z + 1, 0, mid, :]
            factor = sign if c == 2 else None
            for ref, value in ((one_ref, once), (two_ref, centre), (three_ref, third)):
                ref[c, z_out] = value if factor is None else factor * value
            pairs = ((begin, begin), (begin, once), (once, once), (once, centre), (centre, centre), (centre, third))
            for k, (a, b) in enumerate(pairs):
                sums[k] = sums[k] + fold(a * b)

    zero = jnp.zeros((8, LANES), F32)
    sums = [zero] * 6
    for step in range(layers + REACH + 8):
        for stage, (count, lag) in reversed(tuple(enumerate(((REACH, 0), (REACH - 1, 2), (REACH - 2, 4), (1, 6), (0, 8))))):
            z = step - lag
            if not 0 <= z < layers + count:
                continue
            if stage == 0:
                apply_first(z)
            elif stage == 1:
                spread(w1, div1, across1, z + 1)
            elif stage == 2:
                apply_second(z)
            elif stage == 3:
                spread(w2, div2, across2, z + 1)
            else:
                apply_third(z, sums)
    spot = lax.broadcasted_iota(jnp.int32, (1, ROW), 1)
    row = tally_ref[...]
    for k in range(6):
        row = jnp.where(spot == k, jnp.sum(sums[k]), row)
    row_ref[...] = row


def powers(sizes, at, depth, beyond, mine, theirs, stiff, tally):
    layers = depth.shape[0]
    _, rows, lanes = stiff.shape
    tall = mine.shape[1]
    local_x = tall - 2 * EDGE
    field = jax.ShapeDtypeStruct((3, layers, local_x, lanes), F32)
    deep = rows + 2 * EDGE
    return pl.pallas_call(
        functools.partial(powers_kernel, sizes, layers),
        out_shape=(
            jax.ShapeDtypeStruct((3, local_x, lanes), F32),
            field,
            field,
            field,
            jax.ShapeDtypeStruct((1, ROW), F32),
        ),
        in_specs=[SMEM] * 3 + [VMEM] * 4,
        out_specs=(VMEM,) * 5,
        scratch_shapes=[
            pltpu.VMEM((2, 9, tall, lanes), F32),
            pltpu.VMEM((2, tall, lanes), F32),
            pltpu.VMEM((layers + REACH, 2, rows, lanes), F32),
            pltpu.VMEM((3, layers + REACH + 1, 2, deep, lanes), F32),
            pltpu.VMEM((3, layers + REACH - 1, 2, deep, lanes), F32),
            pltpu.VMEM((layers + REACH, 2, deep, lanes), F32),
            pltpu.VMEM((layers + REACH // 2, 2, deep, lanes), F32),
            pltpu.VMEM((layers + REACH, 2, rows, lanes), F32),
            pltpu.VMEM((layers + REACH // 2, 2, rows, lanes), F32),
        ],
        compiler_params=pltpu.CompilerParams(vmem_limit_bytes=20 << 20),
        cost_estimate=pl.CostEstimate(flops=100_000_000, bytes_accessed=4 << 20, transcendentals=0),
        name="powers",
    )(at, depth, beyond, mine, theirs, stiff, tally)


def step_factors(nu):
    def inner(a, b):
        total = None
        for i, u in enumerate(a):
            for j, v in enumerate(b):
                term = u * v * nu[i + j]
                total = term if total is None else total + term
        return total

    def applied(a):
        out = [SHIFT * u for u in a] + [jnp.zeros_like(nu[0])]
        for i, u in enumerate(a):
            out[i + 1] = out[i + 1] + u
        return out

    def plus(a, factor, b):
        size = max(len(a), len(b))
        out = []
        for i in range(size):
            if i >= len(b):
                out.append(a[i])
            elif i >= len(a):
                out.append(factor * b[i])
            else:
                out.append(a[i] + factor * b[i])
        return out

    one = jnp.ones_like(nu[0])
    resid, along = [one], [one]
    found = [jnp.zeros_like(one)]
    now = nu[0]
    for step in range(3):
        image = applied(along)
        alpha = now / inner(along, image)
        found = plus(found, alpha, along)
        resid = plus(resid, -alpha, image)
        if step < 2:
            new = inner(resid, resid)
            along = plus(resid, new / now, along)
            now = new
    return found, resid


def finish_kernel(
    depth_ref, got_ref, surface_ref, one_ref, two_ref, three_ref, field_out, resid_out, field_ref, resid_ref, sems
):
    layers = one_ref.shape[1]
    totals = jnp.sum(got_ref[...], axis=0, keepdims=True)
    values = [totals[:, k : k + 1] for k in range(8)]
    found, resid = step_factors(values[:6])
    scale = lax.rsqrt(values[6] / (EPOCHS * values[7]) + EPS)
    shape = surface_ref.shape[1:]
    found = [jnp.broadcast_to(scale * v, shape) for v in found]
    resid = [jnp.broadcast_to(scale * v, shape) for v in resid]
    chunk = layers // 8
    copies = []
    for piece in range(8):
        first = piece * chunk

        def one_layer(k, carry, first=first):
            z = first + k
            d = depth_ref[z]
            for c in range(3):
                begin = d * surface_ref[c]
                once, twice = one_ref[c, z], two_ref[c, z]
                field_ref[c, z] = found[0] * begin + found[1] * once + found[2] * twice
                resid_ref[c, z] = resid[0] * begin + resid[1] * once + resid[2] * twice + resid[3] * three_ref[c, z]
            return carry

        lax.fori_loop(0, chunk, one_layer, 0)
        for k, (src, dst) in enumerate(((field_ref, field_out), (resid_ref, resid_out))):
            part = pl.ds(first, chunk)
            copy = pltpu.make_async_copy(src.at[:, part], dst.at[:, part], sems.at[k, piece])
            copy.start()
            copies.append(copy)
    for copy in copies:
        copy.wait()


def finish(depth, got, surface, one, two, three):
    field = jax.ShapeDtypeStruct(one.shape, F32)
    return pl.pallas_call(
        finish_kernel,
        out_shape=(field, field),
        in_specs=[SMEM] + [VMEM] * 5,
        out_specs=(ANY,) * 2,
        scratch_shapes=[
            pltpu.VMEM(one.shape, F32),
            pltpu.VMEM(one.shape, F32),
            pltpu.SemaphoreType.DMA((2, 8)),
        ],
        compiler_params=pltpu.CompilerParams(vmem_limit_bytes=12 << 20),
        cost_estimate=pl.CostEstimate(flops=20_000_000, bytes_accessed=4 << 20, transcendentals=0),
        name="finish",
    )(depth, got, surface, one, two, three)


def from_below(value, axis):
    count = lax.axis_size(axis)
    return lax.ppermute(value, axis, [(i, (i + 1) % count) for i in range(count)])


def from_above(value, axis):
    count = lax.axis_size(axis)
    return lax.ppermute(value, axis, [((i + 1) % count, i) for i in range(count)])


def from_partner(value, axis):
    return lax.ppermute(value, axis, [(0, 1), (1, 0)])


def beside(left, right, width):
    lane = lax.broadcasted_iota(jnp.int32, left.shape, left.ndim - 1)
    return jnp.where(lane % (2 * width) >= width, right, left)


def per_device(
    observed,
    predicted,
    coherence_mask,
    block_count,
    block_owner,
    block_matrix_choice,
    block_patch,
    look_vector,
    interp_weights,
    depth_kernel,
    stiffness,
):
    layers, local_x, local_y = stiffness.shape
    sizes = tuple(lax.axis_size(a) for a in ("gx", "gy", "gz"))
    owners = sizes[0] * sizes[1]
    at = lax.axis_index(("gx", "gy", "gz")).astype(jnp.int32).reshape(1)
    upper = lax.axis_index("gz") == 1

    sums, tally = front(
        block_count, look_vector, block_owner[:, 0], block_patch, block_matrix_choice,
        observed, predicted, coherence_mask, interp_weights, owners,
    )
    sums, stiffness, depth_kernel = lax.optimization_barrier((sums, stiffness, depth_kernel))
    got = lax.all_to_all(sums, ("gx", "gy"), split_axis=0, concat_axis=0, tiled=True)
    depth_beyond = from_partner(depth_kernel, "gz")
    far = from_partner(jnp.where(upper, stiffness[:REACH], stiffness[layers - REACH :]), "gz")
    packed = pack(stiffness, far)
    side = beside(from_below(packed, "gy"), from_above(packed, "gy"), REACH)
    stiff = jnp.concatenate([stiffness, far, side])
    low, high = stiff[:, :REACH, :], stiff[:, local_x - REACH :, :]
    below = from_below(high, "gx")
    above = from_above(low, "gx")
    stiff = jnp.concatenate([below, stiff, above], axis=1)

    part, edges = place(got[:, 0], local_x, local_y)
    side = beside(from_below(edges, "gy"), from_above(edges, "gy"), EDGE)
    mine = jnp.concatenate([part, side[None]])
    mine = jnp.concatenate(
        [from_below(mine[:, local_x - EDGE :, :], "gx"), mine, from_above(mine[:, :EDGE, :], "gx")], axis=1
    )
    surface, one, two, three, row = powers(
        sizes, at, depth_kernel, depth_beyond, mine, from_partner(mine, "gz"), stiff, tally
    )
    rows = jnp.broadcast_to(row + from_partner(row, "gz"), (owners, ROW))
    rows = lax.all_to_all(rows, ("gx", "gy"), split_axis=0, concat_axis=0, tiled=True)
    return finish(depth_kernel, rows, surface, one, two, three)


def solution(mesh):
    in_specs = (
        P(("grp", "gx", "gy", "gz"), None, None),
        P(("grp", "gx", "gy", "gz"), None, None),
        P(("grp", "gx", "gy", "gz"), None),
        P(("grp", "gx", "gy", "gz")),
        P(("grp", "gx", "gy", "gz"), None),
        P(("grp", "gx", "gy", "gz")),
        P(("grp", "gx", "gy", "gz")),
        P(),
        P(),
        P(("grp", "gz")),
        P(("grp", "gz"), "gx", "gy"),
    )
    out_specs = (P(None, ("grp", "gz"), "gx", "gy"), P(None, ("grp", "gz"), "gx", "gy"))
    return jax.shard_map(per_device, mesh=mesh, in_specs=in_specs, out_specs=out_specs, check_vma=False)
```

```python
import functools

import jax
import jax.numpy as jnp
from jax import lax
from jax.experimental import pallas as pl
from jax.experimental.pallas import tpu as pltpu
from jax.sharding import PartitionSpec as P


EPOCHS = 4
PATCH_X = 8
PATCH_Y = 16
CAP = 4
LANES = 128
EPS = 1e-06
SHIFT = 8.0
REACH = 4
EDGE = 8
ROW = 16
PIECES = 4
F32 = jnp.float32
VMEM = pl.BlockSpec(memory_space=pltpu.VMEM)
SMEM = pl.BlockSpec(memory_space=pltpu.SMEM)
ANY = pl.BlockSpec(memory_space=pl.ANY)


def column(ref, first, count, lanes):
    row = lax.broadcasted_iota(jnp.int32, (count, lanes), 0)
    out = jnp.full((count, lanes), ref[first], jnp.int32)
    for i in range(1, count):
        out = jnp.where(row == i, ref[first + i], out)
    return out


def front_kernel(
    size_y, count_hbm, look_hbm, owner_hbm, patch_hbm, choice_hbm, observed_hbm, predicted_hbm, mask_hbm, weights_hbm,
    out_ref, tally_ref,
    count_ref, look_ref, owner_ref, patch_ref, choice_ref,
    observed_ref, predicted_ref, mask_ref, weights_ref, coeffs_ref, sums_ref, used_ref, ids_ref, rank_ref, sems,
):
    blocks, _, pixels = observed_ref.shape
    tables, _, lanes = weights_ref.shape
    owners = out_ref.shape[0]

    first = [
        pltpu.make_async_copy(src, dst, sems.at[k])
        for k, (src, dst) in enumerate(
            (
                (owner_hbm, owner_ref),
                (patch_hbm, patch_ref),
                (choice_hbm, choice_ref),
                (count_hbm, count_ref),
                (look_hbm, look_ref),
                (observed_hbm, observed_ref),
                (predicted_hbm, predicted_ref),
                (mask_hbm, mask_ref),
            )
        )
    ]
    chunk = tables // PIECES
    second = []
    for piece in range(PIECES):
        part = pl.ds(piece * chunk, chunk)
        second.append(pltpu.make_async_copy(weights_hbm.at[part], weights_ref.at[part], sems.at[len(first) + piece]))
    for copy in first + second:
        copy.start()
    out_ref[...] = jnp.zeros_like(out_ref)
    for o in range(owners):
        used_ref[o] = 0
        for r in range(CAP):
            ids_ref[o * CAP + r] = 0
    for copy in first[:3]:
        copy.wait()

    def target(b):
        o = owner_ref[b]
        return lax.rem(o, size_y) * (owners // size_y) + lax.div(o, size_y)

    for b in range(blocks):
        o = target(b)
        r = used_ref[o]
        used_ref[o] = r + 1
        rank_ref[b] = r
        ids_ref[o * CAP + r] = patch_ref[b]
    spot = lax.broadcasted_iota(jnp.int32, (1, lanes), 1)
    for o in range(owners):
        ids = jnp.zeros((1, lanes), jnp.int32)
        for r in range(CAP):
            ids = jnp.where(spot == r, ids_ref[o * CAP + r], ids)
        out_ref[o, :, 3 * CAP * lanes :] = ids.astype(F32)
    choice = jnp.concatenate([column(choice_ref, g, 8, lanes) for g in range(0, blocks, 8)] * 3, axis=0)

    for copy in first[3:]:
        copy.wait()
    group = 16
    place = lax.broadcasted_iota(jnp.int32, (group, pixels), 1)
    squares = jnp.zeros((group, pixels), F32)
    weight = jnp.zeros((group, pixels), F32)
    for g in range(0, blocks, group):
        rows = slice(g, g + group)
        inside = place < column(count_ref, g, group, pixels)
        valid = jnp.where(inside, mask_ref[rows, :].astype(F32), 0.0)
        weight += valid
        resid = []
        for e in range(EPOCHS):
            r = (predicted_ref[rows, e, :] - observed_ref[rows, e, :]) * valid
            squares += r * r
            resid.append(r)
        for c in range(3):
            total = look_ref[0, c] * resid[0]
            for e in range(1, EPOCHS):
                total += look_ref[e, c] * resid[e]
            coeffs_ref[c * blocks + g : c * blocks + g + group, :] = total.astype(jnp.bfloat16)
    spot = lax.broadcasted_iota(jnp.int32, tally_ref.shape, 1)
    tally = jnp.where(spot == 6, jnp.sum(squares), 0.0)
    tally_ref[...] = jnp.where(spot == 7, jnp.sum(weight), tally)

    coeffs = coeffs_ref[...]
    total = jnp.zeros(sums_ref.shape, F32)
    for piece in range(PIECES):
        second[piece].wait()
        for t in range(piece * chunk, (piece + 1) * chunk, 2):
            pair = jnp.concatenate([weights_ref[t], weights_ref[t + 1]], axis=1)
            product = jnp.dot(coeffs, pair, preferred_element_type=F32)
            total = jnp.where(choice == t, product[:, :lanes], total)
            total = jnp.where(choice == t + 1, product[:, lanes:], total)
    sums_ref[...] = total
    for b in range(blocks):
        o, r = target(b), rank_ref[b]
        for c in range(3):
            at = pl.multiple_of((r * 3 + c) * lanes, lanes)
            out_ref[o, :, pl.ds(at, lanes)] = sums_ref[c * blocks + b : c * blocks + b + 1, :]


def front(count, look, owner, patch, choice, observed, predicted, mask, weights, owners, size_y):
    _, pixels, cells = weights.shape
    blocks = owner.shape[0]
    return pl.pallas_call(
        functools.partial(front_kernel, size_y),
        out_shape=(
            jax.ShapeDtypeStruct((owners, 1, (3 * CAP + 1) * cells), F32),
            jax.ShapeDtypeStruct((1, ROW), F32),
        ),
        in_specs=[ANY] * 9,
        out_specs=(VMEM,) * 2,
        scratch_shapes=[
            pltpu.SMEM((blocks,), jnp.int32),
            pltpu.SMEM(look.shape, F32),
            pltpu.SMEM((blocks,), jnp.int32),
            pltpu.SMEM((blocks,), jnp.int32),
            pltpu.SMEM((blocks,), jnp.int32),
            pltpu.VMEM(observed.shape, F32),
            pltpu.VMEM(observed.shape, F32),
            pltpu.VMEM(mask.shape, jnp.int32),
            pltpu.VMEM(weights.shape, weights.dtype),
            pltpu.VMEM((3 * blocks, pixels), jnp.bfloat16),
            pltpu.VMEM((3 * blocks, cells), F32),
            pltpu.SMEM((owners,), jnp.int32),
            pltpu.SMEM((owners * CAP,), jnp.int32),
            pltpu.SMEM((blocks,), jnp.int32),
            pltpu.SemaphoreType.DMA((8 + PIECES,)),
        ],
        cost_estimate=pl.CostEstimate(flops=400_000_000, bytes_accessed=4 << 20, transcendentals=0),
        name="front",
    )(count, look, owner, patch, choice, observed, predicted, mask, weights)


def pack_kernel(own_ref, far_ref, out_ref):
    lane = lax.broadcasted_iota(jnp.int32, out_ref.shape[1:], 1)
    for k, ref in enumerate((own_ref, far_ref)):
        packed = jnp.zeros(out_ref.shape[1:], F32)
        for z in range(ref.shape[0]):
            moved = pltpu.roll(ref[z], (2 * REACH * z + REACH) % LANES, 1)
            packed = jnp.where(lane // (2 * REACH) == z, moved, packed)
        out_ref[k] = packed


def pack(own, far):
    return pl.pallas_call(
        pack_kernel,
        out_shape=jax.ShapeDtypeStruct((2,) + own.shape[1:], F32),
        in_specs=[VMEM] * 2,
        out_specs=VMEM,
        compiler_params=pltpu.CompilerParams(vmem_limit_bytes=4 << 20),
        cost_estimate=pl.CostEstimate(flops=1_000_000, bytes_accessed=1 << 18, transcendentals=0),
        name="pack",
    )(own, far)


def swap_granules(tile, size):
    count = tile.shape[0]
    lanes = tile.shape[1]
    row = lax.broadcasted_iota(jnp.int32, tile.shape, 0)
    granule = lax.broadcasted_iota(jnp.int32, tile.shape, 1) // size
    k = 1
    while k < count:
        low = (row & k) == 0
        same = low == ((granule & k) == 0)
        up = pltpu.roll(pltpu.roll(tile, count - k, 0), k * size, 1)
        down = pltpu.roll(pltpu.roll(tile, k, 0), lanes - k * size, 1)
        tile = jnp.where(same, tile, jnp.where(low, up, down))
        k *= 2
    return tile


def place_kernel(got_ref, out_ref, edge_ref):
    sources = got_ref.shape[0]
    cells = PATCH_X * PATCH_Y
    local_x, local_y = out_ref.shape[1:]
    places_x, places_y = local_x // PATCH_X, local_y // PATCH_Y
    places = places_x * places_y
    place = lax.broadcasted_iota(jnp.int32, (sources, places), 1).astype(F32)
    ids = got_ref[:, 3 * CAP * cells :]
    total = jnp.zeros((places, 3 * cells), F32)
    for r in range(CAP):
        hot = (ids[:, r : r + 1] == place).astype(F32)
        total += lax.dot_general(
            hot,
            got_ref[:, r * 3 * cells : (r + 1) * 3 * cells],
            (((0,), (0,)), ((), ())),
            precision=lax.Precision.HIGHEST,
            preferred_element_type=F32,
        )
    for c in range(3):
        for i in range(places_x):
            tile = total[i * places_y : (i + 1) * places_y, c * cells : (c + 1) * cells]
            out_ref[c, i * PATCH_X : (i + 1) * PATCH_X, :] = swap_granules(tile, PATCH_Y)
    lane = lax.broadcasted_iota(jnp.int32, edge_ref.shape, 1)
    packed = jnp.zeros(edge_ref.shape, F32)
    for c in range(3):
        moved = pltpu.roll(out_ref[c], 2 * EDGE * c + EDGE, 1)
        packed = jnp.where(lane // (2 * EDGE) == c, moved, packed)
    edge_ref[...] = packed


def place(got, local_x, local_y):
    return pl.pallas_call(
        place_kernel,
        out_shape=(
            jax.ShapeDtypeStruct((3, local_x, local_y), F32),
            jax.ShapeDtypeStruct((local_x, local_y), F32),
        ),
        in_specs=[VMEM],
        out_specs=(VMEM,) * 2,
        compiler_params=pltpu.CompilerParams(vmem_limit_bytes=8 << 20),
        cost_estimate=pl.CostEstimate(flops=40_000_000, bytes_accessed=1 << 19, transcendentals=0),
        name="place",
    )(got)


def lane_steps(own, side):
    lane = lax.broadcasted_iota(jnp.int32, own.shape, 1)
    last, first = lane == LANES - 1, lane == 0
    a0, a1 = pltpu.roll(own, LANES - 1, 1), pltpu.roll(side, LANES - 1, 1)
    b0, b1 = pltpu.roll(own, 1, 1), pltpu.roll(side, 1, 1)
    ahead = (jnp.where(last, a1, a0), jnp.where(last, a0, a1))
    behind = (jnp.where(first, b1, b0), jnp.where(first, b0, b1))
    return ahead, behind


def powers_kernel(
    sizes, layers, at_ref, depth_ref, beyond_ref, mine_ref, theirs_ref, stiff_ref,
    tally_ref, zero_ref, one_ref, two_ref, three_ref, row_ref, flat, keep, diag, w1, w2, div1, div2, across1, across2,
):
    rows, local_x = stiff_ref.shape[1], one_ref.shape[2]
    size_x, size_y, size_z = sizes
    at = at_ref[0]
    at_z = lax.rem(at, size_z)
    at_y = lax.rem(lax.div(at, size_z), size_y)
    at_x = lax.div(at, size_z * size_y)
    upper = at_z == 1
    sign = jnp.where(upper, -1.0, 1.0).astype(F32)
    tall = mine_ref.shape[1]

    def layer_of(z):
        return jnp.where(upper, layers - 1 - z, z)

    depths = [depth_ref[layer_of(z)] for z in range(layers)]
    depths += [beyond_ref[layer_of(z)] for z in range(REACH + 2)]

    def depth(z):
        return depths[z] if z >= 0 else jnp.zeros((), F32)

    lane = lax.broadcasted_iota(jnp.int32, (tall, LANES), 1)
    line = lax.broadcasted_iota(jnp.int32, (tall, LANES), 0)
    outside_x = ((line < EDGE) & (at_x == 0)) | ((line >= tall - EDGE) & (at_x == size_x - 1))
    half = lane < LANES // 2
    outside_y = (half & (at_y == size_y - 1)) | (jnp.logical_not(half) & (at_y == 0))
    in0 = jnp.where(outside_x, 0.0, 1.0)
    in1 = jnp.where(outside_x | outside_y, 0.0, 1.0)
    inside = (in0, in1)

    edges = mine_ref[3] + theirs_ref[3]

    def tiles(c):
        own = mine_ref[c] + theirs_ref[c]
        side = pltpu.roll(edges, LANES - EDGE - 2 * EDGE * c, 1)
        return jnp.where(outside_x, 0.0, own), jnp.where(outside_x | outside_y, 0.0, side)

    def down(v):
        return pltpu.roll(v, tall - 1, 0)

    def up(v):
        return pltpu.roll(v, 1, 0)

    s = [tiles(0), tiles(1), tuple(sign * v for v in tiles(2))]
    moved = [lane_steps(*v) for v in s]
    grad = tuple(
        inside[t] * 0.5 * (down(s[0][t]) - up(s[0][t]) + moved[1][0][t] - moved[1][1][t]) for t in range(2)
    )
    grad_moved = lane_steps(*grad)
    for t in range(2):
        around = [down(s[c][t]) + up(s[c][t]) + moved[c][0][t] + moved[c][1][t] for c in range(3)]
        keep[t] = inside[t]
        for c in range(3):
            flat[t, c] = s[c][t]
        flat[t, 3] = inside[t] * (-around[0] - 0.25 * (down(grad[t]) - up(grad[t])))
        flat[t, 4] = inside[t] * (-around[1] - 0.25 * (grad_moved[0][t] - grad_moved[1][t]))
        flat[t, 5] = inside[t] * (-around[2])
        flat[t, 6] = inside[t] * (-0.25) * (down(s[2][t]) - up(s[2][t]))
        flat[t, 7] = inside[t] * (-0.25) * (moved[2][0][t] - moved[2][1][t])
        flat[t, 8] = inside[t] * (-0.5) * grad[t]

    first = EDGE - REACH
    body = pl.ds(EDGE, rows)
    ahead_x, behind_x = pl.ds(EDGE + 1, rows), pl.ds(EDGE - 1, rows)
    flat_rows = pl.ds(first, rows)

    def apply_first(z):
        d = depth(z)
        before, after = depth(z - 1), depth(z + 1)
        slope = 0.5 * (after - before)
        slope_after = 0.5 * (depth(z + 2) - d)
        slope_before = 0.5 * (d - depth(z - 2)) if z > 0 else 0.0
        bend = 0.5 * (slope_after - slope_before)
        sides = before + after
        if z < layers:
            place = layer_of(z)
            stiff, packed, group = stiff_ref[place], stiff_ref[layers + REACH], place
        else:
            group = jnp.where(upper, REACH - 1 - (z - layers), z - layers)
            stiff, packed = stiff_ref[layers + group], stiff_ref[layers + REACH + 1]
        turned = pltpu.roll(packed, LANES - REACH - 2 * REACH * group, 1)
        for t in range(2):
            centre = (stiff if t == 0 else turned) + (6.0 - SHIFT)
            diag[z, t] = centre
            for c in range(3):
                v = flat[t, c, flat_rows, :]
                rest = flat[t, 3 + c, flat_rows, :]
                cross = flat[t, 6 + c, flat_rows, :]
                own_part = sides if c < 2 else sides + 0.5 * bend
                w1[c, z + 1, t, body, :] = d * (centre * v + rest) - own_part * v + slope * cross

    for c in range(3):
        for t in range(2):
            w1[c, 0, t] = jnp.zeros_like(w1[c, 0, t])
            w2[c, 0, t] = jnp.zeros_like(w2[c, 0, t])
    for t in range(2):
        div1[0, t] = jnp.zeros_like(div1[0, t])
        div2[0, t] = jnp.zeros_like(div2[0, t])

    def spread(w, div, across, z):
        ahead, behind = lane_steps(w[1, z, 0, body, :], w[1, z, 1, body, :])
        for t in range(2):
            across[z, t] = ahead[t] + behind[t]
            total = w[0, z, t, ahead_x, :] - w[0, z, t, behind_x, :] + ahead[t] - behind[t]
            total += w[2, z + 1, t, body, :] - w[2, z - 1, t, body, :]
            div[z, t, body, :] = keep[t, flat_rows, :] * total

    def apply_second(z):
        ahead, behind = lane_steps(div1[z + 1, 0, body, :], div1[z + 1, 1, body, :])
        for c in range(3):
            if c != 1:
                yp, ym = lane_steps(w1[c, z + 1, 0, body, :], w1[c, z + 1, 1, body, :])
            for t in range(2):
                around = w1[c, z + 1, t, ahead_x, :] + w1[c, z + 1, t, behind_x, :]
                around += across1[z + 1, t] if c == 1 else yp[t] + ym[t]
                around += w1[c, z, t, body, :] + w1[c, z + 2, t, body, :]
                if c == 0:
                    slope = div1[z + 1, t, ahead_x, :] - div1[z + 1, t, behind_x, :]
                elif c == 1:
                    slope = ahead[t] - behind[t]
                else:
                    slope = div1[z + 2, t, body, :] - div1[z, t, body, :]
                value = diag[z, t] * w1[c, z + 1, t, body, :] - around - 0.125 * slope
                w2[c, z + 1, t, body, :] = keep[t, flat_rows, :] * value

    lo = EDGE + REACH
    mid = pl.ds(lo, local_x)
    mid_ahead, mid_behind = pl.ds(lo + 1, local_x), pl.ds(lo - 1, local_x)
    narrow = lax.broadcasted_iota(jnp.int32, (local_x, LANES), 1)
    at_last, at_first = narrow == LANES - 1, narrow == 0

    def sides_of(own, side):
        ahead = pltpu.roll(jnp.where(at_first, side, own), LANES - 1, 1)
        behind = pltpu.roll(jnp.where(at_last, side, own), 1, 1)
        return ahead, behind

    def fold(v):
        out = v[0:8]
        for k in range(8, local_x, 8):
            out += v[k : k + 8]
        return out

    def apply_third(z, sums):
        d = depth(z)
        z_out = layer_of(z)
        ahead, behind = sides_of(div2[z + 1, 0, mid, :], div2[z + 1, 1, mid, :])
        for c in range(3):
            centre = w2[c, z + 1, 0, mid, :]
            around = w2[c, z + 1, 0, mid_ahead, :] + w2[c, z + 1, 0, mid_behind, :]
            if c == 1:
                around += across2[z + 1, 0, pl.ds(REACH, local_x), :]
            else:
                yp, ym = sides_of(centre, w2[c, z + 1, 1, mid, :])
                around += yp + ym
            around += w2[c, z, 0, mid, :] + w2[c, z + 2, 0, mid, :]
            if c == 0:
                slope = div2[z + 1, 0, mid_ahead, :] - div2[z + 1, 0, mid_behind, :]
            elif c == 1:
                slope = ahead - behind
            else:
                slope = div2[z + 2, 0, mid, :] - div2[z, 0, mid, :]
            third = diag[z, 0, pl.ds(REACH, local_x), :] * centre - around - 0.125 * slope
            begin = d * flat[0, c, pl.ds(EDGE, local_x), :]
            once = w1[c, z + 1, 0, mid, :]
            factor = sign if c == 2 else None
            for ref, value in ((zero_ref, begin), (one_ref, once), (two_ref, centre), (three_ref, third)):
                ref[c, z_out] = value if factor is None else factor * value
            pairs = ((begin, begin), (begin, once), (once, once), (once, centre), (centre, centre), (centre, third))
            for k, (a, b) in enumerate(pairs):
                sums[k] = sums[k] + fold(a * b)

    zero = jnp.zeros((8, LANES), F32)
    sums = [zero] * 6
    for step in range(layers + REACH + 8):
        for stage, (count, lag) in reversed(tuple(enumerate(((REACH, 0), (REACH - 1, 2), (REACH - 2, 4), (1, 6), (0, 8))))):
            z = step - lag
            if not 0 <= z < layers + count:
                continue
            if stage == 0:
                apply_first(z)
            elif stage == 1:
                spread(w1, div1, across1, z + 1)
            elif stage == 2:
                apply_second(z)
            elif stage == 3:
                spread(w2, div2, across2, z + 1)
            else:
                apply_third(z, sums)
    spot = lax.broadcasted_iota(jnp.int32, (1, ROW), 1)
    row = tally_ref[...]
    for k in range(6):
        row = jnp.where(spot == k, jnp.sum(sums[k]), row)
    row_ref[...] = row


def powers(sizes, at, depth, beyond, mine, theirs, stiff, tally):
    layers = depth.shape[0]
    _, rows, lanes = stiff.shape
    tall = mine.shape[1]
    local_x = tall - 2 * EDGE
    field = jax.ShapeDtypeStruct((3, layers, local_x, lanes), F32)
    deep = rows + 2 * EDGE
    return pl.pallas_call(
        functools.partial(powers_kernel, sizes, layers),
        out_shape=(
            field,
            field,
            field,
            field,
            jax.ShapeDtypeStruct((1, ROW), F32),
        ),
        in_specs=[SMEM] * 3 + [VMEM] * 4,
        out_specs=(VMEM,) * 5,
        scratch_shapes=[
            pltpu.VMEM((2, 9, tall, lanes), F32),
            pltpu.VMEM((2, tall, lanes), F32),
            pltpu.VMEM((layers + REACH, 2, rows, lanes), F32),
            pltpu.VMEM((3, layers + REACH + 1, 2, deep, lanes), F32),
            pltpu.VMEM((3, layers + REACH - 1, 2, deep, lanes), F32),
            pltpu.VMEM((layers + REACH, 2, deep, lanes), F32),
            pltpu.VMEM((layers + REACH // 2, 2, deep, lanes), F32),
            pltpu.VMEM((layers + REACH, 2, rows, lanes), F32),
            pltpu.VMEM((layers + REACH // 2, 2, rows, lanes), F32),
        ],
        compiler_params=pltpu.CompilerParams(vmem_limit_bytes=20 << 20),
        cost_estimate=pl.CostEstimate(flops=100_000_000, bytes_accessed=4 << 20, transcendentals=0),
        name="powers",
    )(at, depth, beyond, mine, theirs, stiff, tally)


def step_factors(nu):
    def inner(a, b):
        total = None
        for i, u in enumerate(a):
            for j, v in enumerate(b):
                term = u * v * nu[i + j]
                total = term if total is None else total + term
        return total

    def applied(a):
        out = [SHIFT * u for u in a] + [jnp.zeros_like(nu[0])]
        for i, u in enumerate(a):
            out[i + 1] = out[i + 1] + u
        return out

    def plus(a, factor, b):
        size = max(len(a), len(b))
        out = []
        for i in range(size):
            if i >= len(b):
                out.append(a[i])
            elif i >= len(a):
                out.append(factor * b[i])
            else:
                out.append(a[i] + factor * b[i])
        return out

    one = jnp.ones_like(nu[0])
    resid, along = [one], [one]
    found = [jnp.zeros_like(one)]
    now = nu[0]
    for step in range(3):
        image = applied(along)
        alpha = now / inner(along, image)
        found = plus(found, alpha, along)
        resid = plus(resid, -alpha, image)
        if step < 2:
            new = inner(resid, resid)
            along = plus(resid, new / now, along)
            now = new
    return found, resid


def finish_kernel(
    got_ref, zero_ref, one_ref, two_ref, three_ref, field_out, resid_out, field_ref, resid_ref, sems
):
    layers = one_ref.shape[1]
    totals = jnp.sum(got_ref[...], axis=0, keepdims=True)
    values = [totals[:, k : k + 1] for k in range(8)]
    found, resid = step_factors(values[:6])
    scale = lax.rsqrt(values[6] / (EPOCHS * values[7]) + EPS)
    shape = one_ref.shape[2:]
    found = [jnp.broadcast_to(scale * v, shape) for v in found]
    resid = [jnp.broadcast_to(scale * v, shape) for v in resid]
    chunk = layers // 8
    copies = []
    for piece in range(8):
        first = piece * chunk

        def one_layer(k, carry, first=first):
            z = first + k
            for c in range(3):
                begin, once, twice = zero_ref[c, z], one_ref[c, z], two_ref[c, z]
                field_ref[c, z] = found[0] * begin + found[1] * once + found[2] * twice
                resid_ref[c, z] = resid[0] * begin + resid[1] * once + resid[2] * twice + resid[3] * three_ref[c, z]
            return carry

        lax.fori_loop(0, chunk, one_layer, 0)
        for k, (src, dst) in enumerate(((field_ref, field_out), (resid_ref, resid_out))):
            part = pl.ds(first, chunk)
            copy = pltpu.make_async_copy(src.at[:, part], dst.at[:, part], sems.at[k, piece])
            copy.start()
            copies.append(copy)
    for copy in copies:
        copy.wait()


def finish(got, zero, one, two, three):
    field = jax.ShapeDtypeStruct(one.shape, F32)
    return pl.pallas_call(
        finish_kernel,
        out_shape=(field, field),
        in_specs=[VMEM] * 5,
        out_specs=(ANY,) * 2,
        scratch_shapes=[
            pltpu.VMEM(one.shape, F32),
            pltpu.VMEM(one.shape, F32),
            pltpu.SemaphoreType.DMA((2, 8)),
        ],
        compiler_params=pltpu.CompilerParams(vmem_limit_bytes=12 << 20),
        cost_estimate=pl.CostEstimate(flops=20_000_000, bytes_accessed=4 << 20, transcendentals=0),
        name="finish",
    )(got, zero, one, two, three)


def from_below(value, axis):
    count = lax.axis_size(axis)
    return lax.ppermute(value, axis, [(i, (i + 1) % count) for i in range(count)])


def from_above(value, axis):
    count = lax.axis_size(axis)
    return lax.ppermute(value, axis, [((i + 1) % count, i) for i in range(count)])


def from_partner(value, axis):
    return lax.ppermute(value, axis, [(0, 1), (1, 0)])


def beside(left, right, width):
    lane = lax.broadcasted_iota(jnp.int32, left.shape, left.ndim - 1)
    return jnp.where(lane % (2 * width) >= width, right, left)


def per_device(
    observed,
    predicted,
    coherence_mask,
    block_count,
    block_owner,
    block_matrix_choice,
    block_patch,
    look_vector,
    interp_weights,
    depth_kernel,
    stiffness,
):
    layers, local_x, local_y = stiffness.shape
    sizes = tuple(lax.axis_size(a) for a in ("gx", "gy", "gz"))
    owners = sizes[0] * sizes[1]
    at = lax.axis_index(("gx", "gy", "gz")).astype(jnp.int32).reshape(1)
    upper = lax.axis_index("gz") == 1

    sums, tally = front(
        block_count, look_vector, block_owner[:, 0], block_patch, block_matrix_choice,
        observed, predicted, coherence_mask, interp_weights, owners, sizes[1],
    )
    sums, stiffness, depth_kernel = lax.optimization_barrier((sums, stiffness, depth_kernel))
    got = lax.all_to_all(sums, ("gy", "gx"), split_axis=0, concat_axis=0, tiled=True)
    depth_beyond = from_partner(depth_kernel, "gz")
    far = from_partner(jnp.where(upper, stiffness[:REACH], stiffness[layers - REACH :]), "gz")
    packed = pack(stiffness, far)
    side = beside(from_below(packed, "gy"), from_above(packed, "gy"), REACH)
    stiff = jnp.concatenate([stiffness, far, side])
    low, high = stiff[:, :REACH, :], stiff[:, local_x - REACH :, :]
    below = from_below(high, "gx")
    above = from_above(low, "gx")
    stiff = jnp.concatenate([below, stiff, above], axis=1)

    part, edges = place(got[:, 0], local_x, local_y)
    side = beside(from_below(edges, "gy"), from_above(edges, "gy"), EDGE)
    mine = jnp.concatenate([part, side[None]])
    mine = jnp.concatenate(
        [from_below(mine[:, local_x - EDGE :, :], "gx"), mine, from_above(mine[:, :EDGE, :], "gx")], axis=1
    )
    zero, one, two, three, row = powers(
        sizes, at, depth_kernel, depth_beyond, mine, from_partner(mine, "gz"), stiff, tally
    )
    rows = jnp.broadcast_to(row + from_partner(row, "gz"), (owners, ROW))
    rows = lax.all_to_all(rows, ("gy", "gx"), split_axis=0, concat_axis=0, tiled=True)
    return finish(rows, zero, one, two, three)


def solution(mesh):
    in_specs = (
        P(("grp", "gx", "gy", "gz"), None, None),
        P(("grp", "gx", "gy", "gz"), None, None),
        P(("grp", "gx", "gy", "gz"), None),
        P(("grp", "gx", "gy", "gz")),
        P(("grp", "gx", "gy", "gz"), None),
        P(("grp", "gx", "gy", "gz")),
        P(("grp", "gx", "gy", "gz")),
        P(),
        P(),
        P(("grp", "gz")),
        P(("grp", "gz"), "gx", "gy"),
    )
    out_specs = (P(None, ("grp", "gz"), "gx", "gy"), P(None, ("grp", "gz"), "gx", "gy"))
    return jax.shard_map(per_device, mesh=mesh, in_specs=in_specs, out_specs=out_specs, check_vma=False)
```

```python
import functools

import jax
import jax.numpy as jnp
from jax import lax
from jax.experimental import pallas as pl
from jax.experimental.pallas import tpu as pltpu
from jax.sharding import PartitionSpec as P


EPOCHS = 4
PATCH_X = 8
PATCH_Y = 16
CAP = 4
LANES = 128
EPS = 1e-06
SHIFT = 8.0
REACH = 4
EDGE = 8
ROW = 16
PIECES = 4
F32 = jnp.float32
VMEM = pl.BlockSpec(memory_space=pltpu.VMEM)
SMEM = pl.BlockSpec(memory_space=pltpu.SMEM)
ANY = pl.BlockSpec(memory_space=pl.ANY)


def column(ref, first, count, lanes):
    row = lax.broadcasted_iota(jnp.int32, (count, lanes), 0)
    out = jnp.full((count, lanes), ref[first], jnp.int32)
    for i in range(1, count):
        out = jnp.where(row == i, ref[first + i], out)
    return out


def front_kernel(
    size_y, count_hbm, look_hbm, owner_hbm, patch_hbm, choice_hbm, observed_hbm, predicted_hbm, mask_hbm, weights_hbm,
    out_ref, tally_ref,
    count_ref, look_ref, owner_ref, patch_ref, choice_ref,
    observed_ref, predicted_ref, mask_ref, weights_ref, coeffs_ref, sums_ref, used_ref, ids_ref, rank_ref, sems,
):
    blocks, _, pixels = observed_ref.shape
    tables, _, lanes = weights_ref.shape
    owners = out_ref.shape[0]

    first = [
        pltpu.make_async_copy(src, dst, sems.at[k])
        for k, (src, dst) in enumerate(
            (
                (owner_hbm, owner_ref),
                (patch_hbm, patch_ref),
                (choice_hbm, choice_ref),
                (count_hbm, count_ref),
                (look_hbm, look_ref),
                (observed_hbm, observed_ref),
                (predicted_hbm, predicted_ref),
                (mask_hbm, mask_ref),
            )
        )
    ]
    chunk = tables // PIECES
    second = []
    for piece in range(PIECES):
        part = pl.ds(piece * chunk, chunk)
        second.append(pltpu.make_async_copy(weights_hbm.at[part], weights_ref.at[part], sems.at[len(first) + piece]))
    for copy in first + second:
        copy.start()
    out_ref[...] = jnp.zeros_like(out_ref)
    for o in range(owners):
        used_ref[o] = 0
        for r in range(CAP):
            ids_ref[o * CAP + r] = 0
    for copy in first[:3]:
        copy.wait()

    def target(b):
        o = owner_ref[b]
        if size_y & (size_y - 1):
            x, y = lax.div(o, size_y), lax.rem(o, size_y)
        else:
            x, y = lax.shift_right_logical(o, size_y.bit_length() - 1), o & (size_y - 1)
        return y * (owners // size_y) + x

    for b in range(blocks):
        o = target(b)
        r = used_ref[o]
        used_ref[o] = r + 1
        rank_ref[b] = r
        owner_ref[b] = o
        ids_ref[o * CAP + r] = patch_ref[b]
    spot = lax.broadcasted_iota(jnp.int32, (1, lanes), 1)
    for o in range(owners):
        ids = jnp.zeros((1, lanes), jnp.int32)
        for r in range(CAP):
            ids = jnp.where(spot == r, ids_ref[o * CAP + r], ids)
        out_ref[o, :, 3 * CAP * lanes :] = ids.astype(F32)
    choice = jnp.concatenate([column(choice_ref, g, 8, lanes) for g in range(0, blocks, 8)] * 3, axis=0)

    for copy in first[3:]:
        copy.wait()
    group = 16
    place = lax.broadcasted_iota(jnp.int32, (group, pixels), 1)
    squares = jnp.zeros((group, pixels), F32)
    weight = jnp.zeros((group, pixels), F32)
    for g in range(0, blocks, group):
        rows = slice(g, g + group)
        inside = place < column(count_ref, g, group, pixels)
        valid = jnp.where(inside, mask_ref[rows, :].astype(F32), 0.0)
        weight += valid
        resid = []
        for e in range(EPOCHS):
            r = (predicted_ref[rows, e, :] - observed_ref[rows, e, :]) * valid
            squares += r * r
            resid.append(r)
        for c in range(3):
            total = look_ref[0, c] * resid[0]
            for e in range(1, EPOCHS):
                total += look_ref[e, c] * resid[e]
            coeffs_ref[c * blocks + g : c * blocks + g + group, :] = total.astype(jnp.bfloat16)
    spot = lax.broadcasted_iota(jnp.int32, tally_ref.shape, 1)
    tally = jnp.where(spot == 6, jnp.sum(squares), 0.0)
    tally_ref[...] = jnp.where(spot == 7, jnp.sum(weight), tally)

    coeffs = coeffs_ref[...]
    total = jnp.zeros(sums_ref.shape, F32)
    for piece in range(PIECES):
        second[piece].wait()
        for t in range(piece * chunk, (piece + 1) * chunk, 2):
            pair = jnp.concatenate([weights_ref[t], weights_ref[t + 1]], axis=1)
            product = jnp.dot(coeffs, pair, preferred_element_type=F32)
            total = jnp.where(choice == t, product[:, :lanes], total)
            total = jnp.where(choice == t + 1, product[:, lanes:], total)
    sums_ref[...] = total
    for b in range(blocks):
        o, r = owner_ref[b], rank_ref[b]
        for c in range(3):
            at = pl.multiple_of((r * 3 + c) * lanes, lanes)
            out_ref[o, :, pl.ds(at, lanes)] = sums_ref[c * blocks + b : c * blocks + b + 1, :]


def front(count, look, owner, patch, choice, observed, predicted, mask, weights, owners, size_y):
    _, pixels, cells = weights.shape
    blocks = owner.shape[0]
    return pl.pallas_call(
        functools.partial(front_kernel, size_y),
        out_shape=(
            jax.ShapeDtypeStruct((owners, 1, (3 * CAP + 1) * cells), F32),
            jax.ShapeDtypeStruct((1, ROW), F32),
        ),
        in_specs=[ANY] * 9,
        out_specs=(VMEM,) * 2,
        scratch_shapes=[
            pltpu.SMEM((blocks,), jnp.int32),
            pltpu.SMEM(look.shape, F32),
            pltpu.SMEM((blocks,), jnp.int32),
            pltpu.SMEM((blocks,), jnp.int32),
            pltpu.SMEM((blocks,), jnp.int32),
            pltpu.VMEM(observed.shape, F32),
            pltpu.VMEM(observed.shape, F32),
            pltpu.VMEM(mask.shape, jnp.int32),
            pltpu.VMEM(weights.shape, weights.dtype),
            pltpu.VMEM((3 * blocks, pixels), jnp.bfloat16),
            pltpu.VMEM((3 * blocks, cells), F32),
            pltpu.SMEM((owners,), jnp.int32),
            pltpu.SMEM((owners * CAP,), jnp.int32),
            pltpu.SMEM((blocks,), jnp.int32),
            pltpu.SemaphoreType.DMA((8 + PIECES,)),
        ],
        cost_estimate=pl.CostEstimate(flops=400_000_000, bytes_accessed=4 << 20, transcendentals=0),
        name="front",
    )(count, look, owner, patch, choice, observed, predicted, mask, weights)


def pack_kernel(own_ref, far_ref, out_ref):
    lane = lax.broadcasted_iota(jnp.int32, out_ref.shape[1:], 1)
    for k, ref in enumerate((own_ref, far_ref)):
        packed = jnp.zeros(out_ref.shape[1:], F32)
        for z in range(ref.shape[0]):
            moved = pltpu.roll(ref[z], (2 * REACH * z + REACH) % LANES, 1)
            packed = jnp.where(lane // (2 * REACH) == z, moved, packed)
        out_ref[k] = packed


def pack(own, far):
    return pl.pallas_call(
        pack_kernel,
        out_shape=jax.ShapeDtypeStruct((2,) + own.shape[1:], F32),
        in_specs=[VMEM] * 2,
        out_specs=VMEM,
        compiler_params=pltpu.CompilerParams(vmem_limit_bytes=4 << 20),
        cost_estimate=pl.CostEstimate(flops=1_000_000, bytes_accessed=1 << 18, transcendentals=0),
        name="pack",
    )(own, far)


def swap_granules(tile, size):
    count = tile.shape[0]
    lanes = tile.shape[1]
    row = lax.broadcasted_iota(jnp.int32, tile.shape, 0)
    granule = lax.broadcasted_iota(jnp.int32, tile.shape, 1) // size
    k = 1
    while k < count:
        low = (row & k) == 0
        same = low == ((granule & k) == 0)
        up = pltpu.roll(pltpu.roll(tile, count - k, 0), k * size, 1)
        down = pltpu.roll(pltpu.roll(tile, k, 0), lanes - k * size, 1)
        tile = jnp.where(same, tile, jnp.where(low, up, down))
        k *= 2
    return tile


def place_kernel(got_ref, out_ref, edge_ref):
    sources = got_ref.shape[0]
    cells = PATCH_X * PATCH_Y
    local_x, local_y = out_ref.shape[1:]
    places_x, places_y = local_x // PATCH_X, local_y // PATCH_Y
    places = places_x * places_y
    place = lax.broadcasted_iota(jnp.int32, (sources, places), 1).astype(F32)
    ids = got_ref[:, 3 * CAP * cells :]
    total = jnp.zeros((places, 3 * cells), F32)
    for r in range(CAP):
        hot = (ids[:, r : r + 1] == place).astype(F32)
        total += lax.dot_general(
            hot,
            got_ref[:, r * 3 * cells : (r + 1) * 3 * cells],
            (((0,), (0,)), ((), ())),
            precision=lax.Precision.HIGHEST,
            preferred_element_type=F32,
        )
    for c in range(3):
        for i in range(places_x):
            tile = total[i * places_y : (i + 1) * places_y, c * cells : (c + 1) * cells]
            out_ref[c, i * PATCH_X : (i + 1) * PATCH_X, :] = swap_granules(tile, PATCH_Y)
    lane = lax.broadcasted_iota(jnp.int32, edge_ref.shape, 1)
    packed = jnp.zeros(edge_ref.shape, F32)
    for c in range(3):
        moved = pltpu.roll(out_ref[c], 2 * EDGE * c + EDGE, 1)
        packed = jnp.where(lane // (2 * EDGE) == c, moved, packed)
    edge_ref[...] = packed


def place(got, local_x, local_y):
    return pl.pallas_call(
        place_kernel,
        out_shape=(
            jax.ShapeDtypeStruct((3, local_x, local_y), F32),
            jax.ShapeDtypeStruct((local_x, local_y), F32),
        ),
        in_specs=[VMEM],
        out_specs=(VMEM,) * 2,
        compiler_params=pltpu.CompilerParams(vmem_limit_bytes=8 << 20),
        cost_estimate=pl.CostEstimate(flops=40_000_000, bytes_accessed=1 << 19, transcendentals=0),
        name="place",
    )(got)


def lane_steps(own, side):
    lane = lax.broadcasted_iota(jnp.int32, own.shape, 1)
    last, first = lane == LANES - 1, lane == 0
    a0, a1 = pltpu.roll(own, LANES - 1, 1), pltpu.roll(side, LANES - 1, 1)
    b0, b1 = pltpu.roll(own, 1, 1), pltpu.roll(side, 1, 1)
    ahead = (jnp.where(last, a1, a0), jnp.where(last, a0, a1))
    behind = (jnp.where(first, b1, b0), jnp.where(first, b0, b1))
    return ahead, behind


def powers_kernel(
    layers, scalars_hbm, guide_ref, mine_ref, theirs_ref, stiff_ref,
    tally_ref, zero_ref, one_ref, two_ref, three_ref, row_ref, scalars, sem, flat, keep, diag, w1, w2, div1, div2, across1, across2,
):
    rows, local_x = stiff_ref.shape[1], one_ref.shape[2]
    tall = mine_ref.shape[1]
    copy = pltpu.make_async_copy(scalars_hbm, scalars, sem)
    copy.start()

    inside = (guide_ref[0], guide_ref[1])
    edges = mine_ref[3] + theirs_ref[3]

    def tiles(c):
        own = mine_ref[c] + theirs_ref[c]
        side = pltpu.roll(edges, LANES - EDGE - 2 * EDGE * c, 1)
        return inside[0] * own, inside[1] * side

    def down(v):
        return pltpu.roll(v, tall - 1, 0)

    def up(v):
        return pltpu.roll(v, 1, 0)

    s = [tiles(0), tiles(1), tuple(guide_ref[2] * v for v in tiles(2))]
    moved = [lane_steps(*v) for v in s]
    grad = tuple(
        inside[t] * 0.5 * (down(s[0][t]) - up(s[0][t]) + moved[1][0][t] - moved[1][1][t]) for t in range(2)
    )
    grad_moved = lane_steps(*grad)
    for t in range(2):
        around = [down(s[c][t]) + up(s[c][t]) + moved[c][0][t] + moved[c][1][t] for c in range(3)]
        keep[t] = inside[t]
        for c in range(3):
            flat[t, c] = s[c][t]
        flat[t, 3] = inside[t] * (-around[0] - 0.25 * (down(grad[t]) - up(grad[t])))
        flat[t, 4] = inside[t] * (-around[1] - 0.25 * (grad_moved[0][t] - grad_moved[1][t]))
        flat[t, 5] = inside[t] * (-around[2])
        flat[t, 6] = inside[t] * (-0.25) * (down(s[2][t]) - up(s[2][t]))
        flat[t, 7] = inside[t] * (-0.25) * (moved[2][0][t] - moved[2][1][t])
        flat[t, 8] = inside[t] * (-0.5) * grad[t]

    copy.wait()
    upper = scalars[2 * layers] > 0.5
    sign = jnp.where(upper, -1.0, 1.0).astype(F32)

    def layer_of(z):
        return jnp.where(upper, layers - 1 - z, z)

    depths = [scalars[layer_of(z)] for z in range(layers)]
    depths += [scalars[layers + layer_of(z)] for z in range(REACH + 2)]

    def depth(z):
        return depths[z] if z >= 0 else jnp.zeros((), F32)

    first = EDGE - REACH
    body = pl.ds(EDGE, rows)
    ahead_x, behind_x = pl.ds(EDGE + 1, rows), pl.ds(EDGE - 1, rows)
    flat_rows = pl.ds(first, rows)

    def apply_first(z):
        d = depth(z)
        before, after = depth(z - 1), depth(z + 1)
        slope = 0.5 * (after - before)
        slope_after = 0.5 * (depth(z + 2) - d)
        slope_before = 0.5 * (d - depth(z - 2)) if z > 0 else 0.0
        bend = 0.5 * (slope_after - slope_before)
        sides = before + after
        if z < layers:
            place = layer_of(z)
            stiff, packed, group = stiff_ref[place], stiff_ref[layers + REACH], place
        else:
            group = jnp.where(upper, REACH - 1 - (z - layers), z - layers)
            stiff, packed = stiff_ref[layers + group], stiff_ref[layers + REACH + 1]
        turned = pltpu.roll(packed, LANES - REACH - 2 * REACH * group, 1)
        for t in range(2):
            centre = (stiff if t == 0 else turned) + (6.0 - SHIFT)
            diag[z, t] = centre
            for c in range(3):
                v = flat[t, c, flat_rows, :]
                rest = flat[t, 3 + c, flat_rows, :]
                cross = flat[t, 6 + c, flat_rows, :]
                own_part = sides if c < 2 else sides + 0.5 * bend
                w1[c, z + 1, t, body, :] = d * (centre * v + rest) - own_part * v + slope * cross

    for c in range(3):
        for t in range(2):
            w1[c, 0, t] = jnp.zeros_like(w1[c, 0, t])
            w2[c, 0, t] = jnp.zeros_like(w2[c, 0, t])
    for t in range(2):
        div1[0, t] = jnp.zeros_like(div1[0, t])
        div2[0, t] = jnp.zeros_like(div2[0, t])

    def spread(w, div, across, z):
        ahead, behind = lane_steps(w[1, z, 0, body, :], w[1, z, 1, body, :])
        for t in range(2):
            across[z, t] = ahead[t] + behind[t]
            total = w[0, z, t, ahead_x, :] - w[0, z, t, behind_x, :] + ahead[t] - behind[t]
            total += w[2, z + 1, t, body, :] - w[2, z - 1, t, body, :]
            div[z, t, body, :] = keep[t, flat_rows, :] * total

    def apply_second(z):
        ahead, behind = lane_steps(div1[z + 1, 0, body, :], div1[z + 1, 1, body, :])
        for c in range(3):
            if c != 1:
                yp, ym = lane_steps(w1[c, z + 1, 0, body, :], w1[c, z + 1, 1, body, :])
            for t in range(2):
                around = w1[c, z + 1, t, ahead_x, :] + w1[c, z + 1, t, behind_x, :]
                around += across1[z + 1, t] if c == 1 else yp[t] + ym[t]
                around += w1[c, z, t, body, :] + w1[c, z + 2, t, body, :]
                if c == 0:
                    slope = div1[z + 1, t, ahead_x, :] - div1[z + 1, t, behind_x, :]
                elif c == 1:
                    slope = ahead[t] - behind[t]
                else:
                    slope = div1[z + 2, t, body, :] - div1[z, t, body, :]
                value = diag[z, t] * w1[c, z + 1, t, body, :] - around - 0.125 * slope
                w2[c, z + 1, t, body, :] = keep[t, flat_rows, :] * value

    lo = EDGE + REACH
    mid = pl.ds(lo, local_x)
    mid_ahead, mid_behind = pl.ds(lo + 1, local_x), pl.ds(lo - 1, local_x)
    narrow = lax.broadcasted_iota(jnp.int32, (local_x, LANES), 1)
    at_last, at_first = narrow == LANES - 1, narrow == 0

    def sides_of(own, side):
        ahead = pltpu.roll(jnp.where(at_first, side, own), LANES - 1, 1)
        behind = pltpu.roll(jnp.where(at_last, side, own), 1, 1)
        return ahead, behind

    def fold(v):
        out = v[0:8]
        for k in range(8, local_x, 8):
            out += v[k : k + 8]
        return out

    def apply_third(z, sums):
        d = depth(z)
        z_out = layer_of(z)
        ahead, behind = sides_of(div2[z + 1, 0, mid, :], div2[z + 1, 1, mid, :])
        for c in range(3):
            centre = w2[c, z + 1, 0, mid, :]
            around = w2[c, z + 1, 0, mid_ahead, :] + w2[c, z + 1, 0, mid_behind, :]
            if c == 1:
                around += across2[z + 1, 0, pl.ds(REACH, local_x), :]
            else:
                yp, ym = sides_of(centre, w2[c, z + 1, 1, mid, :])
                around += yp + ym
            around += w2[c, z, 0, mid, :] + w2[c, z + 2, 0, mid, :]
            if c == 0:
                slope = div2[z + 1, 0, mid_ahead, :] - div2[z + 1, 0, mid_behind, :]
            elif c == 1:
                slope = ahead - behind
            else:
                slope = div2[z + 2, 0, mid, :] - div2[z, 0, mid, :]
            third = diag[z, 0, pl.ds(REACH, local_x), :] * centre - around - 0.125 * slope
            begin = d * flat[0, c, pl.ds(EDGE, local_x), :]
            once = w1[c, z + 1, 0, mid, :]
            factor = sign if c == 2 else None
            for ref, value in ((zero_ref, begin), (one_ref, once), (two_ref, centre), (three_ref, third)):
                ref[c, z_out] = value if factor is None else factor * value
            pairs = ((begin, begin), (begin, once), (once, once), (once, centre), (centre, centre), (centre, third))
            for k, (a, b) in enumerate(pairs):
                sums[k] = sums[k] + fold(a * b)

    zero = jnp.zeros((8, LANES), F32)
    sums = [zero] * 6
    for step in range(layers + REACH + 8):
        for stage, (count, lag) in reversed(tuple(enumerate(((REACH, 0), (REACH - 1, 2), (REACH - 2, 4), (1, 6), (0, 8))))):
            z = step - lag
            if not 0 <= z < layers + count:
                continue
            if stage == 0:
                apply_first(z)
            elif stage == 1:
                spread(w1, div1, across1, z + 1)
            elif stage == 2:
                apply_second(z)
            elif stage == 3:
                spread(w2, div2, across2, z + 1)
            else:
                apply_third(z, sums)
    spot = lax.broadcasted_iota(jnp.int32, (1, ROW), 1)
    row = tally_ref[...]
    for k in range(6):
        row = jnp.where(spot == k, jnp.sum(sums[k]), row)
    row_ref[...] = row


def powers(layers, scalars, guide, mine, theirs, stiff, tally):
    _, rows, lanes = stiff.shape
    tall = mine.shape[1]
    local_x = tall - 2 * EDGE
    field = jax.ShapeDtypeStruct((3, layers, local_x, lanes), F32)
    deep = rows + 2 * EDGE
    return pl.pallas_call(
        functools.partial(powers_kernel, layers),
        out_shape=(
            field,
            field,
            field,
            field,
            jax.ShapeDtypeStruct((1, ROW), F32),
        ),
        in_specs=[ANY] + [VMEM] * 5,
        out_specs=(VMEM,) * 5,
        scratch_shapes=[
            pltpu.SMEM(scalars.shape, F32),
            pltpu.SemaphoreType.DMA,
            pltpu.VMEM((2, 9, tall, lanes), F32),
            pltpu.VMEM((2, tall, lanes), F32),
            pltpu.VMEM((layers + REACH, 2, rows, lanes), F32),
            pltpu.VMEM((3, layers + REACH + 1, 2, deep, lanes), F32),
            pltpu.VMEM((3, layers + REACH - 1, 2, deep, lanes), F32),
            pltpu.VMEM((layers + REACH, 2, deep, lanes), F32),
            pltpu.VMEM((layers + REACH // 2, 2, deep, lanes), F32),
            pltpu.VMEM((layers + REACH, 2, rows, lanes), F32),
            pltpu.VMEM((layers + REACH // 2, 2, rows, lanes), F32),
        ],
        compiler_params=pltpu.CompilerParams(vmem_limit_bytes=20 << 20),
        cost_estimate=pl.CostEstimate(flops=100_000_000, bytes_accessed=4 << 20, transcendentals=0),
        name="powers",
    )(scalars, guide, mine, theirs, stiff, tally)


def step_factors(nu):
    def inner(a, b):
        total = None
        for i, u in enumerate(a):
            for j, v in enumerate(b):
                term = u * v * nu[i + j]
                total = term if total is None else total + term
        return total

    def applied(a):
        out = [SHIFT * u for u in a] + [jnp.zeros_like(nu[0])]
        for i, u in enumerate(a):
            out[i + 1] = out[i + 1] + u
        return out

    def plus(a, factor, b):
        size = max(len(a), len(b))
        out = []
        for i in range(size):
            if i >= len(b):
                out.append(a[i])
            elif i >= len(a):
                out.append(factor * b[i])
            else:
                out.append(a[i] + factor * b[i])
        return out

    one = jnp.ones_like(nu[0])
    resid, along = [one], [one]
    found = [jnp.zeros_like(one)]
    now = nu[0]
    for step in range(3):
        image = applied(along)
        alpha = now / inner(along, image)
        found = plus(found, alpha, along)
        resid = plus(resid, -alpha, image)
        if step < 2:
            new = inner(resid, resid)
            along = plus(resid, new / now, along)
            now = new
    return found, resid


def finish_kernel(
    got_ref, zero_ref, one_ref, two_ref, three_ref, field_out, resid_out, field_ref, resid_ref, sems
):
    layers = one_ref.shape[1]
    totals = jnp.sum(got_ref[...], axis=0, keepdims=True)
    values = [totals[:, k : k + 1] for k in range(8)]
    found, resid = step_factors(values[:6])
    scale = lax.rsqrt(values[6] / (EPOCHS * values[7]) + EPS)
    shape = one_ref.shape[2:]
    found = [jnp.broadcast_to(scale * v, shape) for v in found]
    resid = [jnp.broadcast_to(scale * v, shape) for v in resid]
    chunk = layers // 8
    copies = []
    for piece in range(8):
        first = piece * chunk

        def one_layer(k, carry, first=first):
            z = first + k
            for c in range(3):
                begin, once, twice = zero_ref[c, z], one_ref[c, z], two_ref[c, z]
                field_ref[c, z] = found[0] * begin + found[1] * once + found[2] * twice
                resid_ref[c, z] = resid[0] * begin + resid[1] * once + resid[2] * twice + resid[3] * three_ref[c, z]
            return carry

        lax.fori_loop(0, chunk, one_layer, 0)
        for k, (src, dst) in enumerate(((field_ref, field_out), (resid_ref, resid_out))):
            part = pl.ds(first, chunk)
            copy = pltpu.make_async_copy(src.at[:, part], dst.at[:, part], sems.at[k, piece])
            copy.start()
            copies.append(copy)
    for copy in copies:
        copy.wait()


def finish(got, zero, one, two, three):
    field = jax.ShapeDtypeStruct(one.shape, F32)
    return pl.pallas_call(
        finish_kernel,
        out_shape=(field, field),
        in_specs=[VMEM] * 5,
        out_specs=(ANY,) * 2,
        scratch_shapes=[
            pltpu.VMEM(one.shape, F32),
            pltpu.VMEM(one.shape, F32),
            pltpu.SemaphoreType.DMA((2, 8)),
        ],
        compiler_params=pltpu.CompilerParams(vmem_limit_bytes=12 << 20),
        cost_estimate=pl.CostEstimate(flops=20_000_000, bytes_accessed=4 << 20, transcendentals=0),
        name="finish",
    )(got, zero, one, two, three)


def from_below(value, axis):
    count = lax.axis_size(axis)
    return lax.ppermute(value, axis, [(i, (i + 1) % count) for i in range(count)])


def from_above(value, axis):
    count = lax.axis_size(axis)
    return lax.ppermute(value, axis, [((i + 1) % count, i) for i in range(count)])


def from_partner(value, axis):
    return lax.ppermute(value, axis, [(0, 1), (1, 0)])


def beside(left, right, width):
    lane = lax.broadcasted_iota(jnp.int32, left.shape, left.ndim - 1)
    return jnp.where(lane % (2 * width) >= width, right, left)


def per_device(
    observed,
    predicted,
    coherence_mask,
    block_count,
    block_owner,
    block_matrix_choice,
    block_patch,
    look_vector,
    interp_weights,
    depth_kernel,
    stiffness,
):
    layers, local_x, local_y = stiffness.shape
    sizes = tuple(lax.axis_size(a) for a in ("gx", "gy", "gz"))
    owners = sizes[0] * sizes[1]
    gx, gy = lax.axis_index("gx"), lax.axis_index("gy")
    upper = lax.axis_index("gz") == 1

    sums, tally = front(
        block_count, look_vector, block_owner[:, 0], block_patch, block_matrix_choice,
        observed, predicted, coherence_mask, interp_weights, owners, sizes[1],
    )
    sums, stiffness, depth_kernel = lax.optimization_barrier((sums, stiffness, depth_kernel))
    got = lax.all_to_all(sums, ("gy", "gx"), split_axis=0, concat_axis=0, tiled=True)
    depth_beyond = from_partner(depth_kernel, "gz")
    far = from_partner(jnp.where(upper, stiffness[:REACH], stiffness[layers - REACH :]), "gz")
    packed = pack(stiffness, far)
    side = beside(from_below(packed, "gy"), from_above(packed, "gy"), REACH)
    stiff = jnp.concatenate([stiffness, far, side])
    low, high = stiff[:, :REACH, :], stiff[:, local_x - REACH :, :]
    below = from_below(high, "gx")
    above = from_above(low, "gx")
    stiff = jnp.concatenate([below, stiff, above], axis=1)

    scalars = jnp.concatenate([depth_kernel, depth_beyond, upper.astype(F32)[None]])
    shape = (local_x + 2 * EDGE, local_y)
    line, lane = (lax.broadcasted_iota(jnp.int32, shape, k) for k in range(2))
    in_x = ((line >= EDGE) | (gx > 0)) & ((line < shape[0] - EDGE) | (gx < sizes[0] - 1))
    in_y = jnp.where(lane < LANES // 2, gy < sizes[1] - 1, gy > 0)
    sign = jnp.broadcast_to(jnp.where(upper, -1.0, 1.0), shape)
    guide = jnp.stack([in_x.astype(F32), (in_x & in_y).astype(F32), sign.astype(F32)])

    part, edges = place(got[:, 0], local_x, local_y)
    side = beside(from_below(edges, "gy"), from_above(edges, "gy"), EDGE)
    mine = jnp.concatenate([part, side[None]])
    mine = jnp.concatenate(
        [from_below(mine[:, local_x - EDGE :, :], "gx"), mine, from_above(mine[:, :EDGE, :], "gx")], axis=1
    )
    zero, one, two, three, row = powers(
        layers, scalars, guide, mine, from_partner(mine, "gz"), stiff, tally
    )
    rows = jnp.broadcast_to(row + from_partner(row, "gz"), (owners, ROW))
    rows = lax.all_to_all(rows, ("gy", "gx"), split_axis=0, concat_axis=0, tiled=True)
    return finish(rows, zero, one, two, three)


def solution(mesh):
    in_specs = (
        P(("grp", "gx", "gy", "gz"), None, None),
        P(("grp", "gx", "gy", "gz"), None, None),
        P(("grp", "gx", "gy", "gz"), None),
        P(("grp", "gx", "gy", "gz")),
        P(("grp", "gx", "gy", "gz"), None),
        P(("grp", "gx", "gy", "gz")),
        P(("grp", "gx", "gy", "gz")),
        P(),
        P(),
        P(("grp", "gz")),
        P(("grp", "gz"), "gx", "gy"),
    )
    out_specs = (P(None, ("grp", "gz"), "gx", "gy"), P(None, ("grp", "gz"), "gx", "gy"))
    return jax.shard_map(per_device, mesh=mesh, in_specs=in_specs, out_specs=out_specs, check_vma=False)
```

```python
import functools

import jax
import jax.numpy as jnp
from jax import lax
from jax.experimental import pallas as pl
from jax.experimental.pallas import tpu as pltpu
from jax.sharding import PartitionSpec as P


EPOCHS = 4
PATCH_X = 8
PATCH_Y = 16
CAP = 4
LANES = 128
EPS = 1e-06
SHIFT = 8.0
REACH = 4
EDGE = 8
ROW = 16
PIECES = 4
F32 = jnp.float32
VMEM = pl.BlockSpec(memory_space=pltpu.VMEM)
SMEM = pl.BlockSpec(memory_space=pltpu.SMEM)
ANY = pl.BlockSpec(memory_space=pl.ANY)


def column(ref, first, count, lanes):
    row = lax.broadcasted_iota(jnp.int32, (count, lanes), 0)
    out = jnp.full((count, lanes), ref[first], jnp.int32)
    for i in range(1, count):
        out = jnp.where(row == i, ref[first + i], out)
    return out


def front_kernel(
    size_y, count_hbm, look_hbm, owner_hbm, patch_hbm, choice_hbm, observed_hbm, predicted_hbm, mask_hbm, weights_hbm,
    out_ref, tally_ref,
    count_ref, look_ref, owner_ref, patch_ref, choice_ref,
    observed_ref, predicted_ref, mask_ref, weights_ref, coeffs_ref, sums_ref, used_ref, ids_ref, rank_ref, sems,
):
    blocks, _, pixels = observed_ref.shape
    tables, _, lanes = weights_ref.shape
    owners = out_ref.shape[0]

    first = [
        pltpu.make_async_copy(src, dst, sems.at[k])
        for k, (src, dst) in enumerate(
            (
                (owner_hbm, owner_ref),
                (patch_hbm, patch_ref),
                (choice_hbm, choice_ref),
                (count_hbm, count_ref),
                (look_hbm, look_ref),
                (observed_hbm, observed_ref),
                (predicted_hbm, predicted_ref),
                (mask_hbm, mask_ref),
            )
        )
    ]
    chunk = tables // PIECES
    second = []
    for piece in range(PIECES):
        part = pl.ds(piece * chunk, chunk)
        second.append(pltpu.make_async_copy(weights_hbm.at[part], weights_ref.at[part], sems.at[len(first) + piece]))
    for copy in first + second:
        copy.start()
    out_ref[...] = jnp.zeros_like(out_ref)
    for o in range(owners):
        used_ref[o] = 0
        for r in range(CAP):
            ids_ref[o * CAP + r] = 0
    for copy in first[:3]:
        copy.wait()

    def target(b):
        o = owner_ref[b]
        if size_y & (size_y - 1):
            x, y = lax.div(o, size_y), lax.rem(o, size_y)
        else:
            x, y = lax.shift_right_logical(o, size_y.bit_length() - 1), o & (size_y - 1)
        return y * (owners // size_y) + x

    for b in range(blocks):
        o = target(b)
        r = used_ref[o]
        used_ref[o] = r + 1
        rank_ref[b] = r
        owner_ref[b] = o
        ids_ref[o * CAP + r] = patch_ref[b]
    spot = lax.broadcasted_iota(jnp.int32, (1, lanes), 1)
    for o in range(owners):
        ids = jnp.zeros((1, lanes), jnp.int32)
        for r in range(CAP):
            ids = jnp.where(spot == r, ids_ref[o * CAP + r], ids)
        out_ref[o, :, 3 * CAP * lanes :] = ids.astype(F32)
    choice = jnp.concatenate([column(choice_ref, g, 8, lanes) for g in range(0, blocks, 8)] * 3, axis=0)

    for copy in first[3:]:
        copy.wait()
    group = 16
    place = lax.broadcasted_iota(jnp.int32, (group, pixels), 1)
    squares = jnp.zeros((group, pixels), F32)
    weight = jnp.zeros((group, pixels), F32)
    for g in range(0, blocks, group):
        rows = slice(g, g + group)
        inside = place < column(count_ref, g, group, pixels)
        valid = jnp.where(inside, mask_ref[rows, :].astype(F32), 0.0)
        weight += valid
        resid = []
        for e in range(EPOCHS):
            r = (predicted_ref[rows, e, :] - observed_ref[rows, e, :]) * valid
            squares += r * r
            resid.append(r)
        for c in range(3):
            total = look_ref[0, c] * resid[0]
            for e in range(1, EPOCHS):
                total += look_ref[e, c] * resid[e]
            coeffs_ref[c * blocks + g : c * blocks + g + group, :] = total.astype(jnp.bfloat16)
    spot = lax.broadcasted_iota(jnp.int32, tally_ref.shape, 1)
    tally = jnp.where(spot == 6, jnp.sum(squares), 0.0)
    tally_ref[...] = jnp.where(spot == 7, jnp.sum(weight), tally)

    coeffs = coeffs_ref[...]
    total = jnp.zeros(sums_ref.shape, F32)
    for piece in range(PIECES):
        second[piece].wait()
        for t in range(piece * chunk, (piece + 1) * chunk, 2):
            pair = jnp.concatenate([weights_ref[t], weights_ref[t + 1]], axis=1)
            product = jnp.dot(coeffs, pair, preferred_element_type=F32)
            total = jnp.where(choice == t, product[:, :lanes], total)
            total = jnp.where(choice == t + 1, product[:, lanes:], total)
    sums_ref[...] = total
    for b in range(blocks):
        o, r = owner_ref[b], rank_ref[b]
        for c in range(3):
            at = pl.multiple_of((r * 3 + c) * lanes, lanes)
            out_ref[o, :, pl.ds(at, lanes)] = sums_ref[c * blocks + b : c * blocks + b + 1, :]


def front(count, look, owner, patch, choice, observed, predicted, mask, weights, owners, size_y):
    _, pixels, cells = weights.shape
    blocks = owner.shape[0]
    return pl.pallas_call(
        functools.partial(front_kernel, size_y),
        out_shape=(
            jax.ShapeDtypeStruct((owners, 1, (3 * CAP + 1) * cells), F32),
            jax.ShapeDtypeStruct((1, ROW), F32),
        ),
        in_specs=[ANY] * 9,
        out_specs=(VMEM,) * 2,
        scratch_shapes=[
            pltpu.SMEM((blocks,), jnp.int32),
            pltpu.SMEM(look.shape, F32),
            pltpu.SMEM((blocks,), jnp.int32),
            pltpu.SMEM((blocks,), jnp.int32),
            pltpu.SMEM((blocks,), jnp.int32),
            pltpu.VMEM(observed.shape, F32),
            pltpu.VMEM(observed.shape, F32),
            pltpu.VMEM(mask.shape, jnp.int32),
            pltpu.VMEM(weights.shape, weights.dtype),
            pltpu.VMEM((3 * blocks, pixels), jnp.bfloat16),
            pltpu.VMEM((3 * blocks, cells), F32),
            pltpu.SMEM((owners,), jnp.int32),
            pltpu.SMEM((owners * CAP,), jnp.int32),
            pltpu.SMEM((blocks,), jnp.int32),
            pltpu.SemaphoreType.DMA((8 + PIECES,)),
        ],
        cost_estimate=pl.CostEstimate(flops=400_000_000, bytes_accessed=4 << 20, transcendentals=0),
        name="front",
    )(count, look, owner, patch, choice, observed, predicted, mask, weights)


def pack_kernel(own_ref, far_ref, out_ref):
    lane = lax.broadcasted_iota(jnp.int32, out_ref.shape[1:], 1)
    for k, ref in enumerate((own_ref, far_ref)):
        packed = jnp.zeros(out_ref.shape[1:], F32)
        for z in range(ref.shape[0]):
            moved = pltpu.roll(ref[z], (2 * REACH * z + REACH) % LANES, 1)
            packed = jnp.where(lane // (2 * REACH) == z, moved, packed)
        out_ref[k] = packed


def pack(own, far):
    return pl.pallas_call(
        pack_kernel,
        out_shape=jax.ShapeDtypeStruct((2,) + own.shape[1:], F32),
        in_specs=[VMEM] * 2,
        out_specs=VMEM,
        compiler_params=pltpu.CompilerParams(vmem_limit_bytes=4 << 20),
        cost_estimate=pl.CostEstimate(flops=1_000_000, bytes_accessed=1 << 18, transcendentals=0),
        name="pack",
    )(own, far)


def swap_granules(tile, size):
    count = tile.shape[0]
    lanes = tile.shape[1]
    row = lax.broadcasted_iota(jnp.int32, tile.shape, 0)
    granule = lax.broadcasted_iota(jnp.int32, tile.shape, 1) // size
    k = 1
    while k < count:
        low = (row & k) == 0
        same = low == ((granule & k) == 0)
        up = pltpu.roll(pltpu.roll(tile, count - k, 0), k * size, 1)
        down = pltpu.roll(pltpu.roll(tile, k, 0), lanes - k * size, 1)
        tile = jnp.where(same, tile, jnp.where(low, up, down))
        k *= 2
    return tile


def place_kernel(got_ref, out_ref, edge_ref):
    sources = got_ref.shape[0]
    cells = PATCH_X * PATCH_Y
    local_x, local_y = out_ref.shape[1:]
    places_x, places_y = local_x // PATCH_X, local_y // PATCH_Y
    places = places_x * places_y
    place = lax.broadcasted_iota(jnp.int32, (sources, places), 1).astype(F32)
    ids = got_ref[:, 3 * CAP * cells :]
    total = jnp.zeros((places, 3 * cells), F32)
    for r in range(CAP):
        hot = (ids[:, r : r + 1] == place).astype(jnp.bfloat16)
        rest = got_ref[:, r * 3 * cells : (r + 1) * 3 * cells]
        for _ in range(3):
            piece = rest.astype(jnp.bfloat16)
            rest = rest - piece.astype(F32)
            total += lax.dot_general(hot, piece, (((0,), (0,)), ((), ())), preferred_element_type=F32)
    for c in range(3):
        for i in range(places_x):
            tile = total[i * places_y : (i + 1) * places_y, c * cells : (c + 1) * cells]
            out_ref[c, i * PATCH_X : (i + 1) * PATCH_X, :] = swap_granules(tile, PATCH_Y)
    lane = lax.broadcasted_iota(jnp.int32, edge_ref.shape, 1)
    packed = jnp.zeros(edge_ref.shape, F32)
    for c in range(3):
        moved = pltpu.roll(out_ref[c], 2 * EDGE * c + EDGE, 1)
        packed = jnp.where(lane // (2 * EDGE) == c, moved, packed)
    edge_ref[...] = packed


def place(got, local_x, local_y):
    return pl.pallas_call(
        place_kernel,
        out_shape=(
            jax.ShapeDtypeStruct((3, local_x, local_y), F32),
            jax.ShapeDtypeStruct((local_x, local_y), F32),
        ),
        in_specs=[VMEM],
        out_specs=(VMEM,) * 2,
        compiler_params=pltpu.CompilerParams(vmem_limit_bytes=8 << 20),
        cost_estimate=pl.CostEstimate(flops=40_000_000, bytes_accessed=1 << 19, transcendentals=0),
        name="place",
    )(got)


def lane_steps(own, side):
    lane = lax.broadcasted_iota(jnp.int32, own.shape, 1)
    last, first = lane == LANES - 1, lane == 0
    a0, a1 = pltpu.roll(own, LANES - 1, 1), pltpu.roll(side, LANES - 1, 1)
    b0, b1 = pltpu.roll(own, 1, 1), pltpu.roll(side, 1, 1)
    ahead = (jnp.where(last, a1, a0), jnp.where(last, a0, a1))
    behind = (jnp.where(first, b1, b0), jnp.where(first, b0, b1))
    return ahead, behind


def powers_kernel(
    layers, scalars_hbm, guide_ref, mine_ref, stiff_ref,
    tally_ref, zero_ref, one_ref, two_ref, three_ref, row_ref, scalars, sem, flat, keep, diag, w1, w2, div1, div2, across1, across2,
):
    rows, local_x = stiff_ref.shape[1], one_ref.shape[2]
    tall = mine_ref.shape[1]
    copy = pltpu.make_async_copy(scalars_hbm, scalars, sem)
    copy.start()

    inside = (guide_ref[0], guide_ref[1])
    edges = mine_ref[3]

    def tiles(c):
        own = mine_ref[c]
        side = pltpu.roll(edges, LANES - EDGE - 2 * EDGE * c, 1)
        return inside[0] * own, inside[1] * side

    def down(v):
        return pltpu.roll(v, tall - 1, 0)

    def up(v):
        return pltpu.roll(v, 1, 0)

    s = [tiles(0), tiles(1), tuple(guide_ref[2] * v for v in tiles(2))]
    moved = [lane_steps(*v) for v in s]
    grad = tuple(
        inside[t] * 0.5 * (down(s[0][t]) - up(s[0][t]) + moved[1][0][t] - moved[1][1][t]) for t in range(2)
    )
    grad_moved = lane_steps(*grad)
    for t in range(2):
        around = [down(s[c][t]) + up(s[c][t]) + moved[c][0][t] + moved[c][1][t] for c in range(3)]
        keep[t] = inside[t]
        for c in range(3):
            flat[t, c] = s[c][t]
        flat[t, 3] = inside[t] * (-around[0] - 0.25 * (down(grad[t]) - up(grad[t])))
        flat[t, 4] = inside[t] * (-around[1] - 0.25 * (grad_moved[0][t] - grad_moved[1][t]))
        flat[t, 5] = inside[t] * (-around[2])
        flat[t, 6] = inside[t] * (-0.25) * (down(s[2][t]) - up(s[2][t]))
        flat[t, 7] = inside[t] * (-0.25) * (moved[2][0][t] - moved[2][1][t])
        flat[t, 8] = inside[t] * (-0.5) * grad[t]

    copy.wait()
    upper = scalars[2 * layers] > 0.5
    sign = jnp.where(upper, -1.0, 1.0).astype(F32)

    def layer_of(z):
        return jnp.where(upper, layers - 1 - z, z)

    depths = [scalars[layer_of(z)] for z in range(layers)]
    depths += [scalars[layers + layer_of(z)] for z in range(REACH + 2)]

    def depth(z):
        return depths[z] if z >= 0 else jnp.zeros((), F32)

    first = EDGE - REACH
    body = pl.ds(EDGE, rows)
    ahead_x, behind_x = pl.ds(EDGE + 1, rows), pl.ds(EDGE - 1, rows)
    flat_rows = pl.ds(first, rows)

    def apply_first(z):
        d = depth(z)
        before, after = depth(z - 1), depth(z + 1)
        slope = 0.5 * (after - before)
        slope_after = 0.5 * (depth(z + 2) - d)
        slope_before = 0.5 * (d - depth(z - 2)) if z > 0 else 0.0
        bend = 0.5 * (slope_after - slope_before)
        sides = before + after
        if z < layers:
            place = layer_of(z)
            stiff, packed, group = stiff_ref[place], stiff_ref[layers + REACH], place
        else:
            group = jnp.where(upper, REACH - 1 - (z - layers), z - layers)
            stiff, packed = stiff_ref[layers + group], stiff_ref[layers + REACH + 1]
        turned = pltpu.roll(packed, LANES - REACH - 2 * REACH * group, 1)
        for t in range(2):
            centre = (stiff if t == 0 else turned) + (6.0 - SHIFT)
            diag[z, t] = centre
            for c in range(3):
                v = flat[t, c, flat_rows, :]
                rest = flat[t, 3 + c, flat_rows, :]
                cross = flat[t, 6 + c, flat_rows, :]
                own_part = sides if c < 2 else sides + 0.5 * bend
                w1[c, z + 1, t, body, :] = d * (centre * v + rest) - own_part * v + slope * cross

    for c in range(3):
        for t in range(2):
            w1[c, 0, t] = jnp.zeros_like(w1[c, 0, t])
            w2[c, 0, t] = jnp.zeros_like(w2[c, 0, t])
    for t in range(2):
        div1[0, t] = jnp.zeros_like(div1[0, t])
        div2[0, t] = jnp.zeros_like(div2[0, t])

    def spread(w, div, across, z):
        ahead, behind = lane_steps(w[1, z, 0, body, :], w[1, z, 1, body, :])
        for t in range(2):
            across[z, t] = ahead[t] + behind[t]
            total = w[0, z, t, ahead_x, :] - w[0, z, t, behind_x, :] + ahead[t] - behind[t]
            total += w[2, z + 1, t, body, :] - w[2, z - 1, t, body, :]
            div[z, t, body, :] = keep[t, flat_rows, :] * total

    def apply_second(z):
        ahead, behind = lane_steps(div1[z + 1, 0, body, :], div1[z + 1, 1, body, :])
        for c in range(3):
            if c != 1:
                yp, ym = lane_steps(w1[c, z + 1, 0, body, :], w1[c, z + 1, 1, body, :])
            for t in range(2):
                around = w1[c, z + 1, t, ahead_x, :] + w1[c, z + 1, t, behind_x, :]
                around += across1[z + 1, t] if c == 1 else yp[t] + ym[t]
                around += w1[c, z, t, body, :] + w1[c, z + 2, t, body, :]
                if c == 0:
                    slope = div1[z + 1, t, ahead_x, :] - div1[z + 1, t, behind_x, :]
                elif c == 1:
                    slope = ahead[t] - behind[t]
                else:
                    slope = div1[z + 2, t, body, :] - div1[z, t, body, :]
                value = diag[z, t] * w1[c, z + 1, t, body, :] - around - 0.125 * slope
                w2[c, z + 1, t, body, :] = keep[t, flat_rows, :] * value

    lo = EDGE + REACH
    mid = pl.ds(lo, local_x)
    mid_ahead, mid_behind = pl.ds(lo + 1, local_x), pl.ds(lo - 1, local_x)
    narrow = lax.broadcasted_iota(jnp.int32, (local_x, LANES), 1)
    at_last, at_first = narrow == LANES - 1, narrow == 0

    def sides_of(own, side):
        ahead = pltpu.roll(jnp.where(at_first, side, own), LANES - 1, 1)
        behind = pltpu.roll(jnp.where(at_last, side, own), 1, 1)
        return ahead, behind

    def fold(v):
        out = v[0:8]
        for k in range(8, local_x, 8):
            out += v[k : k + 8]
        return out

    def apply_third(z, sums):
        d = depth(z)
        z_out = layer_of(z)
        ahead, behind = sides_of(div2[z + 1, 0, mid, :], div2[z + 1, 1, mid, :])
        for c in range(3):
            centre = w2[c, z + 1, 0, mid, :]
            around = w2[c, z + 1, 0, mid_ahead, :] + w2[c, z + 1, 0, mid_behind, :]
            if c == 1:
                around += across2[z + 1, 0, pl.ds(REACH, local_x), :]
            else:
                yp, ym = sides_of(centre, w2[c, z + 1, 1, mid, :])
                around += yp + ym
            around += w2[c, z, 0, mid, :] + w2[c, z + 2, 0, mid, :]
            if c == 0:
                slope = div2[z + 1, 0, mid_ahead, :] - div2[z + 1, 0, mid_behind, :]
            elif c == 1:
                slope = ahead - behind
            else:
                slope = div2[z + 2, 0, mid, :] - div2[z, 0, mid, :]
            third = diag[z, 0, pl.ds(REACH, local_x), :] * centre - around - 0.125 * slope
            begin = d * flat[0, c, pl.ds(EDGE, local_x), :]
            once = w1[c, z + 1, 0, mid, :]
            factor = sign if c == 2 else None
            for ref, value in ((zero_ref, begin), (one_ref, once), (two_ref, centre), (three_ref, third)):
                ref[c, z_out] = value if factor is None else factor * value
            pairs = ((begin, begin), (begin, once), (once, once), (once, centre), (centre, centre), (centre, third))
            for k, (a, b) in enumerate(pairs):
                sums[k] = sums[k] + fold(a * b)

    zero = jnp.zeros((8, LANES), F32)
    sums = [zero] * 6
    for step in range(layers + REACH + 8):
        for stage, (count, lag) in reversed(tuple(enumerate(((REACH, 0), (REACH - 1, 2), (REACH - 2, 4), (1, 6), (0, 8))))):
            z = step - lag
            if not 0 <= z < layers + count:
                continue
            if stage == 0:
                apply_first(z)
            elif stage == 1:
                spread(w1, div1, across1, z + 1)
            elif stage == 2:
                apply_second(z)
            elif stage == 3:
                spread(w2, div2, across2, z + 1)
            else:
                apply_third(z, sums)
    spot = lax.broadcasted_iota(jnp.int32, (1, ROW), 1)
    row = tally_ref[...]
    for k in range(6):
        row = jnp.where(spot == k, jnp.sum(sums[k]), row)
    row_ref[...] = row


def powers(layers, scalars, guide, mine, stiff, tally):
    _, rows, lanes = stiff.shape
    tall = mine.shape[1]
    local_x = tall - 2 * EDGE
    field = jax.ShapeDtypeStruct((3, layers, local_x, lanes), F32)
    deep = rows + 2 * EDGE
    return pl.pallas_call(
        functools.partial(powers_kernel, layers),
        out_shape=(
            field,
            field,
            field,
            field,
            jax.ShapeDtypeStruct((1, ROW), F32),
        ),
        in_specs=[ANY] + [VMEM] * 4,
        out_specs=(VMEM,) * 5,
        scratch_shapes=[
            pltpu.SMEM(scalars.shape, F32),
            pltpu.SemaphoreType.DMA,
            pltpu.VMEM((2, 9, tall, lanes), F32),
            pltpu.VMEM((2, tall, lanes), F32),
            pltpu.VMEM((layers + REACH, 2, rows, lanes), F32),
            pltpu.VMEM((3, layers + REACH + 1, 2, deep, lanes), F32),
            pltpu.VMEM((3, layers + REACH - 1, 2, deep, lanes), F32),
            pltpu.VMEM((layers + REACH, 2, deep, lanes), F32),
            pltpu.VMEM((layers + REACH // 2, 2, deep, lanes), F32),
            pltpu.VMEM((layers + REACH, 2, rows, lanes), F32),
            pltpu.VMEM((layers + REACH // 2, 2, rows, lanes), F32),
        ],
        compiler_params=pltpu.CompilerParams(vmem_limit_bytes=20 << 20),
        cost_estimate=pl.CostEstimate(flops=100_000_000, bytes_accessed=4 << 20, transcendentals=0),
        name="powers",
    )(scalars, guide, mine, stiff, tally)


def step_factors(nu):
    def inner(a, b):
        total = None
        for i, u in enumerate(a):
            for j, v in enumerate(b):
                term = u * v * nu[i + j]
                total = term if total is None else total + term
        return total

    def applied(a):
        out = [SHIFT * u for u in a] + [jnp.zeros_like(nu[0])]
        for i, u in enumerate(a):
            out[i + 1] = out[i + 1] + u
        return out

    def plus(a, factor, b):
        size = max(len(a), len(b))
        out = []
        for i in range(size):
            if i >= len(b):
                out.append(a[i])
            elif i >= len(a):
                out.append(factor * b[i])
            else:
                out.append(a[i] + factor * b[i])
        return out

    one = jnp.ones_like(nu[0])
    resid, along = [one], [one]
    found = [jnp.zeros_like(one)]
    now = nu[0]
    for step in range(3):
        image = applied(along)
        alpha = now / inner(along, image)
        found = plus(found, alpha, along)
        resid = plus(resid, -alpha, image)
        if step < 2:
            new = inner(resid, resid)
            along = plus(resid, new / now, along)
            now = new
    return found, resid


def finish_kernel(
    got_ref, zero_ref, one_ref, two_ref, three_ref, field_out, resid_out, field_ref, resid_ref, sems
):
    layers = one_ref.shape[1]
    totals = jnp.sum(got_ref[...], axis=0, keepdims=True)
    values = [totals[:, k : k + 1] for k in range(8)]
    found, resid = step_factors(values[:6])
    scale = lax.rsqrt(values[6] / (EPOCHS * values[7]) + EPS)
    shape = one_ref.shape[2:]
    found = [jnp.broadcast_to(scale * v, shape) for v in found]
    resid = [jnp.broadcast_to(scale * v, shape) for v in resid]
    chunk = layers // 8
    copies = []
    for piece in range(8):
        first = piece * chunk

        def one_layer(k, carry, first=first):
            z = first + k
            for c in range(3):
                begin, once, twice = zero_ref[c, z], one_ref[c, z], two_ref[c, z]
                field_ref[c, z] = found[0] * begin + found[1] * once + found[2] * twice
                resid_ref[c, z] = resid[0] * begin + resid[1] * once + resid[2] * twice + resid[3] * three_ref[c, z]
            return carry

        lax.fori_loop(0, chunk, one_layer, 0)
        for k, (src, dst) in enumerate(((field_ref, field_out), (resid_ref, resid_out))):
            part = pl.ds(first, chunk)
            copy = pltpu.make_async_copy(src.at[:, part], dst.at[:, part], sems.at[k, piece])
            copy.start()
            copies.append(copy)
    for copy in copies:
        copy.wait()


def finish(got, zero, one, two, three):
    field = jax.ShapeDtypeStruct(one.shape, F32)
    return pl.pallas_call(
        finish_kernel,
        out_shape=(field, field),
        in_specs=[VMEM] * 5,
        out_specs=(ANY,) * 2,
        scratch_shapes=[
            pltpu.VMEM(one.shape, F32),
            pltpu.VMEM(one.shape, F32),
            pltpu.SemaphoreType.DMA((2, 8)),
        ],
        compiler_params=pltpu.CompilerParams(vmem_limit_bytes=12 << 20),
        cost_estimate=pl.CostEstimate(flops=20_000_000, bytes_accessed=4 << 20, transcendentals=0),
        name="finish",
    )(got, zero, one, two, three)


def from_below(value, axis):
    count = lax.axis_size(axis)
    return lax.ppermute(value, axis, [(i, (i + 1) % count) for i in range(count)])


def from_above(value, axis):
    count = lax.axis_size(axis)
    return lax.ppermute(value, axis, [((i + 1) % count, i) for i in range(count)])


def from_partner(value, axis):
    return lax.ppermute(value, axis, [(0, 1), (1, 0)])


def beside(left, right, width):
    lane = lax.broadcasted_iota(jnp.int32, left.shape, left.ndim - 1)
    return jnp.where(lane % (2 * width) >= width, right, left)


def per_device(
    observed,
    predicted,
    coherence_mask,
    block_count,
    block_owner,
    block_matrix_choice,
    block_patch,
    look_vector,
    interp_weights,
    depth_kernel,
    stiffness,
):
    layers, local_x, local_y = stiffness.shape
    sizes = tuple(lax.axis_size(a) for a in ("gx", "gy", "gz"))
    owners = sizes[0] * sizes[1]
    gx, gy = lax.axis_index("gx"), lax.axis_index("gy")
    upper = lax.axis_index("gz") == 1

    sums, tally = front(
        block_count, look_vector, block_owner[:, 0], block_patch, block_matrix_choice,
        observed, predicted, coherence_mask, interp_weights, owners, sizes[1],
    )
    sums, stiffness, depth_kernel = lax.optimization_barrier((sums, stiffness, depth_kernel))
    got = lax.all_to_all(sums, ("gy", "gx"), split_axis=0, concat_axis=0, tiled=True)
    depth_beyond = from_partner(depth_kernel, "gz")
    far = from_partner(jnp.where(upper, stiffness[:REACH], stiffness[layers - REACH :]), "gz")
    packed = pack(stiffness, far)
    side = beside(from_below(packed, "gy"), from_above(packed, "gy"), REACH)
    stiff = jnp.concatenate([stiffness, far, side])
    low, high = stiff[:, :REACH, :], stiff[:, local_x - REACH :, :]
    below = from_below(high, "gx")
    above = from_above(low, "gx")
    stiff = jnp.concatenate([below, stiff, above], axis=1)

    scalars = jnp.concatenate([depth_kernel, depth_beyond, upper.astype(F32)[None]])
    shape = (local_x + 2 * EDGE, local_y)
    line, lane = (lax.broadcasted_iota(jnp.int32, shape, k) for k in range(2))
    in_x = ((line >= EDGE) | (gx > 0)) & ((line < shape[0] - EDGE) | (gx < sizes[0] - 1))
    in_y = jnp.where(lane < LANES // 2, gy < sizes[1] - 1, gy > 0)
    sign = jnp.broadcast_to(jnp.where(upper, -1.0, 1.0), shape)
    guide = jnp.stack([in_x.astype(F32), (in_x & in_y).astype(F32), sign.astype(F32)])

    part, edges = place(got[:, 0], local_x, local_y)
    part = jnp.concatenate([part, edges[None]])
    part = part + from_partner(part, "gz")
    part, edges = part[:3], part[3]
    side = beside(from_below(edges, "gy"), from_above(edges, "gy"), EDGE)
    mine = jnp.concatenate([part, side[None]])
    mine = jnp.concatenate(
        [from_below(mine[:, local_x - EDGE :, :], "gx"), mine, from_above(mine[:, :EDGE, :], "gx")], axis=1
    )
    zero, one, two, three, row = powers(
        layers, scalars, guide, mine, stiff, tally
    )
    rows = jnp.broadcast_to(row + from_partner(row, "gz"), (owners, ROW))
    rows = lax.all_to_all(rows, ("gy", "gx"), split_axis=0, concat_axis=0, tiled=True)
    return finish(rows, zero, one, two, three)


def solution(mesh):
    in_specs = (
        P(("grp", "gx", "gy", "gz"), None, None),
        P(("grp", "gx", "gy", "gz"), None, None),
        P(("grp", "gx", "gy", "gz"), None),
        P(("grp", "gx", "gy", "gz")),
        P(("grp", "gx", "gy", "gz"), None),
        P(("grp", "gx", "gy", "gz")),
        P(("grp", "gx", "gy", "gz")),
        P(),
        P(),
        P(("grp", "gz")),
        P(("grp", "gz"), "gx", "gy"),
    )
    out_specs = (P(None, ("grp", "gz"), "gx", "gy"), P(None, ("grp", "gz"), "gx", "gy"))
    return jax.shard_map(per_device, mesh=mesh, in_specs=in_specs, out_specs=out_specs, check_vma=False)
```
